128 devices in a mesh: patch: 128 (over y, z, x, core).
Axes of the slice: x: 4, y: 4, z: 4, core: 2. Of those that a mesh axis runs over, the one named last changes fastest.
Arguments:
- positions: float32 [3, 262144], P(None, 'patch'), may hold values from -6 to 6
- densities: float32 [3, 262144], P(None, 'patch'), may hold values from -6 to 6
- near_src: int32 [2048, 8], P('patch'), may hold values from 0 to 2047, as said below
- near_count: int32 [2048], P('patch'), may hold values from 1 to 8
- far_slot: int32 [2048, 32], P('patch'), may hold values from 0 to 511
- far_class: int32 [2048, 32], P('patch'), may hold values from 0 to 188
- far_count: int32 [2048], P('patch'), may hold values from 1 to 32
- requests: int32 [128, 128, 4], P('patch'), may hold values from 0 to 15, as said below
- up_basis: bfloat16 [2048, 144, 384], P('patch'), may hold values from -0.3125 to 0.3125
- transfer_table: bfloat16 [189, 20736], replicated, may hold values from -0.5 to 0.5
- down_basis: bfloat16 [2048, 144, 9, 128], P('patch'), may hold values from -0.09375 to 0.09375
Outputs:
- shape_grad: float32 [3, 262144], P(None, 'patch')
The draws below stay inside these ranges and needn't reach their ends.
Inputs may be any that keep to these rules, and one draw needn't show every extreme that they name: `near_src`: the source leaf of each near-field block is held by the device of its target leaf or by the device just before or after it along patch. `requests`: each row names 4 different leaves of the source device, by their index on that device.
All inputs are finite; a program needn't handle non-finite values.
Results may differ from the reference program's by a relative error of at most 0.0042.
Values may be sent and summed in bfloat16 or wider, within the bound.
A program may use at most 192 MiB of HBM per device.

```python
import math
import jax
import jax.numpy as jnp
from jax import lax

P_SIZE = 128
RANK = 48
LEAF_DEV = 16
NEAR = 8
FAR = 32
CLASSES = 189
CAP = 4
LEAVES = 2048
NODES = 262144
SLOTS = 512
N_PATCH = 128


def draw_near_src(key, part):
    leaves = jnp.arange(LEAVES, dtype=jnp.int32)
    owner = leaves // LEAF_DEV
    last_dev = LEAVES // LEAF_DEV - 1
    span = jnp.where((owner == 0) | (owner == last_dev), 2 * LEAF_DEV, 3 * LEAF_DEV)
    lowest = jnp.where(owner == 0, 0, (owner - 1) * LEAF_DEV)
    raw = jax.random.randint(jax.random.fold_in(key, 11), (LEAVES, NEAR), 0, 1 << 30)
    return (lowest[:, None] + raw % span[:, None]).astype(jnp.int32)


def draw_near_count(key, part):
    first, second, third = jax.random.split(jax.random.fold_in(key, 12), 3)
    ndev = LEAVES // LEAF_DEV
    level = jax.random.randint(first, (ndev,), max(1, NEAR // 4), NEAR + 1)
    raw = jax.random.randint(second, (LEAVES,), 0, 1 << 30)
    count = 1 + raw % jnp.repeat(level, LEAF_DEV)
    chosen = jax.random.randint(third, (), 0, ndev)
    leaves = jnp.arange(LEAVES, dtype=jnp.int32)
    return jnp.where(leaves == chosen * LEAF_DEV, NEAR, count).astype(jnp.int32)


def draw_requests(key, part):
    ndev = LEAVES // LEAF_DEV
    scores = jax.random.randint(jax.random.fold_in(key, 13), (ndev, ndev, LEAF_DEV), 0, 1 << 20)
    scores = scores * LEAF_DEV + jnp.arange(LEAF_DEV, dtype=jnp.int32)
    order = jnp.argsort(scores, axis=-1, stable=True)
    return order[:, :, :CAP].astype(jnp.int32)


def with_ends(entries, own_key, least, top_value):
    longest = entries.shape.index(max(entries.shape))
    spots = []
    for shift in (0, 1):
        where = [jax.random.randint(jax.random.fold_in(own_key, axis), (), 0, length) for axis, length in enumerate(entries.shape)]
        where[longest] = (where[longest] + shift) % entries.shape[longest]
        spots.append(tuple(where))
    return entries.at[spots[0]].set(least).at[spots[1]].set(top_value)


def steps_of(stream_key, shape, cuts, low, high):
    def one(position, blocks):
        draws = jax.random.uniform(jax.random.fold_in(jax.random.fold_in(stream_key, 6), position), (blocks,), jnp.float32, low / len(cuts), high / len(cuts))
        return jnp.repeat(jnp.exp(draws), shape[position] // blocks).reshape((-1,) + (1,) * (len(shape) - position - 1))

    factor_of = one(*cuts[0])
    for cut in cuts[1:]:
        factor_of = factor_of * one(*cut)
    return factor_of


def gaussian(own_key, extent, spread, most, pieces=(), kind=jnp.bfloat16):
    gain = steps_of(own_key, extent, pieces, -0.22, 0.18) if pieces else 1.0
    entries = jax.random.normal(own_key, extent, jnp.float32) * spread * gain
    return jnp.minimum(jnp.maximum(entries, -most), most).astype(kind)


def setup_inputs(seed: int = 0) -> dict:
    splits = jax.random.split(jax.random.key(seed), 12)
    positions = gaussian(splits[0], (3, NODES), 1.0, 6.0, ((1, 128),), jnp.float32)
    densities = gaussian(splits[1], (3, NODES), 1.0, 6.0, ((1, 128),), jnp.float32)
    near_src = draw_near_src(jax.random.fold_in(splits[11], 71), 0)
    near_count = draw_near_count(jax.random.fold_in(splits[11], 71), 0)
    far_slot = with_ends(jax.random.randint(splits[4], (LEAVES, FAR), 0, SLOTS), jax.random.fold_in(splits[4], 1), 0, SLOTS - 1).astype(jnp.int32)
    far_class = with_ends(jax.random.randint(splits[5], (LEAVES, FAR), 0, CLASSES), jax.random.fold_in(splits[5], 1), 0, CLASSES - 1).astype(jnp.int32)
    far_count = with_ends(jax.random.randint(splits[6], (LEAVES,), 1, FAR + 1), jax.random.fold_in(splits[6], 1), 1, FAR).astype(jnp.int32)
    requests = draw_requests(jax.random.fold_in(splits[11], 71), 0)
    up_basis = gaussian(splits[8], (LEAVES, 3 * RANK, 3 * P_SIZE), (3 * P_SIZE) ** -0.5, 0.3125, ((0, 128),))
    transfer_table = gaussian(splits[9], (CLASSES, 9 * RANK * RANK), (3 * RANK) ** -0.5, 0.5)
    down_basis = gaussian(splits[10], (LEAVES, 3 * RANK, 9, P_SIZE), (3 * RANK * FAR) ** -0.5, 0.09375, ((0, 128),))
    return dict(positions=positions, densities=densities, near_src=near_src, near_count=near_count, far_slot=far_slot, far_class=far_class, far_count=far_count, requests=requests, up_basis=up_basis, transfer_table=transfer_table, down_basis=down_basis)


KERNEL = 1.0 / (8.0 * math.pi)
BLOB = 0.25

def pair_terms(target, source):
    xt = target[:, :3]
    ft = target[:, 3:]
    xs = source[:, :3]
    fs = source[:, 3:]
    sep = xt[:, :, :, None] - xs[:, :, None, :]
    rho_sq = lax.optimization_barrier(jnp.sum(sep * sep, axis=1)) + BLOB
    inv_one = lax.rsqrt(rho_sq)
    inv_three = inv_one / rho_sq
    inv_five = inv_three / rho_sq
    fa = ft[:, :, :, None]
    fb = fs[:, :, None, :]
    prod_ab = lax.optimization_barrier(jnp.sum(fa * fb, axis=1))
    prod_ar = lax.optimization_barrier(jnp.sum(fa * sep, axis=1))
    prod_br = lax.optimization_barrier(jnp.sum(fb * sep, axis=1))
    first = (fa * prod_br[:, None] + fb * prod_ar[:, None] - prod_ab[:, None] * sep) * inv_three[:, None]
    second = 3.0 * (prod_ar * prod_br * inv_five)[:, None] * sep
    return (first - second) * KERNEL

def reference(positions, densities, near_src, near_count, far_slot, far_class, far_count, requests, up_basis, transfer_table, down_basis):
    stacked = jnp.concatenate([positions, densities], 0).reshape(6, LEAVES, P_SIZE).transpose(1, 0, 2)
    blocks = jnp.arange(N_PATCH, dtype=jnp.int32)

    def slot_body(slot, grad):
        source = near_src[:, slot]
        live = (slot < near_count).astype(jnp.float32)

        def one_block(block):
            start = (block * LEAF_DEV).astype(jnp.int32)
            target = lax.dynamic_slice_in_dim(stacked, start, LEAF_DEV, 0)
            src_ids = lax.dynamic_slice_in_dim(source, start, LEAF_DEV, 0)
            weight = lax.dynamic_slice_in_dim(live, start, LEAF_DEV, 0)
            terms = pair_terms(target, stacked[src_ids]) * weight[:, None, None, None]
            return (lax.optimization_barrier(jnp.sum(terms, axis=3)), lax.optimization_barrier(jnp.sum(terms, axis=2)))
        tgt_sum, src_sum = lax.map(one_block, blocks)
        grad = grad + tgt_sum.reshape(LEAVES, 3, P_SIZE)
        return grad.at[source].add(-src_sum.reshape(LEAVES, 3, P_SIZE))
    near = lax.fori_loop(0, NEAR, slot_body, jnp.zeros((LEAVES, 3, P_SIZE), jnp.float32))
    dens_leaf = stacked[:, 3:]
    dens_round = lax.optimization_barrier(dens_leaf.reshape(LEAVES, 3 * P_SIZE).astype(jnp.bfloat16))
    dens_flat = dens_round.astype(jnp.float32)

    def upward(block):
        start = (block * LEAF_DEV).astype(jnp.int32)
        basis = lax.dynamic_slice_in_dim(up_basis, start, LEAF_DEV, 0).astype(jnp.float32)
        dens_b = lax.dynamic_slice_in_dim(dens_flat, start, LEAF_DEV, 0)
        return jnp.einsum('lrq,lq->lr', basis, dens_b, precision=lax.Precision.HIGHEST).astype(jnp.bfloat16)
    moments = lax.map(upward, blocks).reshape(LEAVES, 3 * RANK)
    moments = lax.optimization_barrier(moments).astype(jnp.float32)
    dev_of = jnp.arange(LEAVES, dtype=jnp.int32) // LEAF_DEV
    peer = far_slot // CAP
    place = far_slot % CAP
    source_ids = peer * LEAF_DEV + requests[dev_of[:, None], peer, place]

    def far_block(block):
        start = (block * LEAF_DEV).astype(jnp.int32)
        ids = lax.dynamic_slice_in_dim(source_ids, start, LEAF_DEV, 0)
        classes = lax.dynamic_slice_in_dim(far_class, start, LEAF_DEV, 0)
        counts = lax.dynamic_slice_in_dim(far_count, start, LEAF_DEV, 0)

        def far_step(slot, expansion):
            src = moments[ids[:, slot]]
            oper = transfer_table[classes[:, slot]].reshape(LEAF_DEV, 3 * RANK, 3 * RANK).astype(jnp.float32)
            live = (slot < counts).astype(jnp.float32)
            return expansion + live[:, None] * jnp.einsum('lij,lj->li', oper, src, precision=lax.Precision.HIGHEST)
        expansion = lax.fori_loop(0, FAR, far_step, jnp.zeros((LEAF_DEV, 3 * RANK), jnp.float32))
        expansion = lax.optimization_barrier(expansion.astype(jnp.bfloat16)).astype(jnp.float32)
        basis = lax.dynamic_slice_in_dim(down_basis, start, LEAF_DEV, 0).astype(jnp.float32)
        field = jnp.einsum('lr,lrqp->lqp', expansion, basis, precision=lax.Precision.HIGHEST)
        dens_b = lax.dynamic_slice_in_dim(dens_leaf, start, LEAF_DEV, 0)
        return jnp.einsum('lcp,lckp->lkp', dens_b, field.reshape(LEAF_DEV, 3, 3, P_SIZE), precision=lax.Precision.HIGHEST)
    far = lax.map(far_block, blocks).reshape(LEAVES, 3, P_SIZE)
    return (near + far).transpose(1, 0, 2).reshape(3, NODES)
```

```python
import math

import jax
import jax.numpy as jnp
import numpy as np
from jax import lax
from jax.experimental import pallas as pl
from jax.experimental.pallas import tpu as pltpu
from jax.sharding import PartitionSpec as P

KERNEL = 1.0 / (8.0 * math.pi)
BLOB = 0.25
PITCH = 9
F32 = jnp.float32
BF16 = jnp.bfloat16


def with_halo(x, sides, width):
    for axis, dim in sides:
        peers, length = (lax.axis_size(axis), x.shape[dim])
        up = [(i, (i + 1) % peers) for i in range(peers - 1)]
        down = [(j, i) for i, j in up]
        last = lax.slice_in_dim(x, length - width, length, axis=dim)
        first = lax.slice_in_dim(x, 0, width, axis=dim)
        before = lax.ppermute(last, axis, up)
        after = lax.ppermute(first, axis, down)
        x = jnp.concatenate([before, x, after], axis=dim)
    return x


def passed_along(x, axis, by):
    peers = lax.axis_size(axis)
    pairs = [(i, i + by) for i in range(peers) if 0 <= i + by < peers]
    return lax.ppermute(x, axis, pairs)


def near_kernel(idx_ref, cnt_ref, win_ref, tgt_ref, src_ref, cols, racc, sacc):
    leaves = tgt_ref.shape[0]
    tiles = racc.shape[1] // 8
    sacc[...] = jnp.zeros_like(sacc)

    def leaf_step(leaf, _):
        turned = jnp.transpose(win_ref[leaves + leaf], (1, 0))
        for k in range(6):
            cols[k] = jnp.broadcast_to(turned[:, k : k + 1], cols.shape[1:])
        racc[...] = jnp.zeros_like(racc)

        def slot_step(slot, _):
            other = idx_ref[leaf * 8 + slot]
            source = win_ref[other]
            rows = [jnp.broadcast_to(source[k : k + 1], (8, 128)) for k in range(6)]
            xs, fs = rows[:3], rows[3:]
            down = [jnp.zeros((8, 128), F32) for _ in range(3)]
            for tile in range(tiles):
                part = pl.ds(8 * tile, 8)
                fa = [cols[3 + k, part] for k in range(3)]
                sep = [cols[k, part] - xs[k] for k in range(3)]
                rho = (sep[0] * sep[0] + sep[1] * sep[1]) + (sep[2] * sep[2] + BLOB)
                inv = lax.rsqrt(rho)
                inv_two = inv * inv
                inv_three = inv_two * inv
                ab = fa[0] * fs[0] + fa[1] * fs[1] + fa[2] * fs[2]
                ar = fa[0] * sep[0] + fa[1] * sep[1] + fa[2] * sep[2]
                br = fs[0] * sep[0] + fs[1] * sep[1] + fs[2] * sep[2]
                on_b = ar * inv_three
                on_a = br * inv_three
                on_r = ab * inv_three + (on_b * br) * (inv_two * 3.0)
                for k in range(3):
                    term = fa[k] * on_a + fs[k] * on_b - on_r * sep[k]
                    racc[k, part] += term
                    down[k] = down[k] + term
            for k in range(3):
                sacc[other, k] -= down[k]
            return 0

        lax.fori_loop(0, cnt_ref[leaf], slot_step, 0)
        for k in range(3):
            turned = jnp.transpose(racc[k], (1, 0))
            tgt_ref[leaf, k : k + 1] = jnp.sum(turned, axis=0, keepdims=True) * KERNEL
        return 0

    lax.fori_loop(0, leaves, leaf_step, 0)

    def out_step(leaf, _):
        for k in range(3):
            src_ref[leaf, k : k + 1] = jnp.sum(sacc[leaf, k], axis=0, keepdims=True) * KERNEL
        return 0

    lax.fori_loop(0, src_ref.shape[0], out_step, 0)


def near_call(index, count, window):
    leaves = count.shape[0]
    smem = pl.BlockSpec(memory_space=pltpu.SMEM)
    vmem = pl.BlockSpec(memory_space=pltpu.VMEM)
    return pl.pallas_call(
        near_kernel,
        name="near",
        out_shape=(
            jax.ShapeDtypeStruct((leaves, 3, 128), F32),
            jax.ShapeDtypeStruct((3 * leaves, 3, 128), F32),
        ),
        in_specs=[smem, smem, vmem],
        out_specs=(vmem, vmem),
        scratch_shapes=[
            pltpu.VMEM((6, 128, 128), F32),
            pltpu.VMEM((3, 128, 128), F32),
            pltpu.VMEM((3 * leaves, 3, 8, 128), F32),
        ],
        compiler_params=pltpu.CompilerParams(vmem_limit_bytes=16 << 20),
        cost_estimate=pl.CostEstimate(flops=10**8, bytes_accessed=10**6, transcendentals=10**6),
    )(index, count, window)


def far_kernel(
    slot_ref,
    class_ref,
    cnt_ref,
    mom_ref,
    sel_ref,
    seg_ref,
    rep_ref,
    dens_ref,
    table_hbm,
    basis_hbm,
    out_ref,
    table,
    wide,
    basis,
    pattern,
    sums,
    splat,
    sems,
):
    leaves = out_ref.shape[0]
    classes = table_hbm.shape[0]
    chunks = table_hbm.shape[1] // 128
    get_table = pltpu.make_async_copy(table_hbm, table, sems.at[0])
    get_basis = pltpu.make_async_copy(basis_hbm, basis, sems.at[1])
    get_table.start()
    get_basis.start()
    for v in range(9):
        part = sel_ref[:, 128 * v : 128 * v + 128]
        pattern[v] = jnp.dot(mom_ref[...], part, preferred_element_type=F32)
    get_table.wait()

    def widen(block, _):
        def piece(step, _):
            for sub in range(9):
                chunk = step * 9 + sub
                lanes = pl.ds(pl.multiple_of(chunk * 128, 128), 128)
                rows = pl.ds(pl.multiple_of(block * 8, 8), 8)
                wide[pl.ds((block * chunks + chunk) * PITCH, 8)] = table[rows, lanes].astype(F32)
            return 0

        lax.fori_loop(0, chunks // 9, piece, 0)
        return 0

    full = classes // 8
    lax.fori_loop(0, full, widen, 0)

    def tail(step, _):
        for sub in range(9):
            chunk = step * 9 + sub
            lanes = pl.ds(pl.multiple_of(chunk * 128, 128), 128)
            wide[pl.ds((full * chunks + chunk) * PITCH, classes - 8 * full)] = table[
                8 * full :, lanes
            ].astype(F32)
        return 0

    lax.fori_loop(0, chunks // 9, tail, 0)

    def leaf_step(leaf, _):
        def slot_step(slot, acc):
            kind = class_ref[leaf * 32 + slot]
            place = slot_ref[leaf * 32 + slot]
            base = (kind // 8) * (chunks * PITCH) + kind % 8
            new = []
            for v in range(9):
                p = jnp.broadcast_to(pattern[v, pl.ds(place, 1), :], (8, 128))
                for g in range(3):
                    t = wide[pl.ds(base + (72 * g + v) * PITCH, 8, stride=9 * PITCH), :]
                    new.append(acc[3 * v + g] + p * t)
            return tuple(new)

        zero = jnp.zeros((8, 128), F32)
        acc = lax.fori_loop(0, cnt_ref[leaf], slot_step, (zero,) * 27)
        for v in range(9):
            for g in range(3):
                rows = pl.ds(pl.multiple_of(leaf * 24 + 8 * g, 8), 8)
                sums[rows, pl.ds(128 * v, 128)] = acc[3 * v + g]
        return 0

    lax.fori_loop(0, leaves, leaf_step, 0)
    total = sums[...]
    high = total.astype(BF16)
    low = (total - high.astype(F32)).astype(BF16)
    expansion = jnp.dot(high, seg_ref[...], preferred_element_type=F32) + jnp.dot(
        low, seg_ref[...], preferred_element_type=F32
    )
    expansion = expansion.astype(BF16)
    for w in range(8):
        part = rep_ref[:, 128 * w : 128 * w + 128]
        splat[w] = jnp.dot(expansion, part, preferred_element_type=F32)
    get_basis.wait()

    def down_step(leaf, _):
        def group(u, acc):
            acc = list(acc)
            for w in range(8):
                x = jnp.broadcast_to(splat[w, pl.ds(leaf * 24 + u, 1), :], (8, 128))
                d = basis[leaf, u * 8 + w].astype(F32)
                top, last = acc[w % 2]
                acc[w % 2] = (top + x * d[:8], last + x[:1] * d[8:])
            return tuple(acc)

        zero = (jnp.zeros((8, 128), F32), jnp.zeros((1, 128), F32))
        acc = lax.fori_loop(0, 18, group, (zero, zero))
        top = acc[0][0] + acc[1][0]
        last = acc[0][1] + acc[1][1]
        f = dens_ref[leaf]
        out_ref[leaf] = (
            f[0:1] * top[0:3]
            + f[1:2] * top[3:6]
            + f[2:3] * jnp.concatenate([top[6:8], last], axis=0)
        )
        return 0

    lax.fori_loop(0, leaves, down_step, 0)


def far_consts(width):
    flat = np.arange(9 * 128)
    sel = (flat[None, :] % width == np.arange(width)[:, None]).astype(np.float32)
    seg = (flat[:, None] // width == np.arange(128)[None, :]).astype(np.float32)
    rep = (np.arange(1024)[None, :] // 128 == np.arange(128)[:, None]).astype(np.float32)
    return [jnp.asarray(m, BF16) for m in (sel, seg, rep)]


def far_call(slots, kinds, count, moments, dens, table, basis):
    leaves = count.shape[0]
    width = basis.shape[1]
    classes = table.shape[0]
    chunks = table.shape[1] // 128
    blocks = -(-classes // 8)
    sel, seg, rep = far_consts(width)
    smem = pl.BlockSpec(memory_space=pltpu.SMEM)
    vmem = pl.BlockSpec(memory_space=pltpu.VMEM)
    hbm = pl.BlockSpec(memory_space=pltpu.HBM)
    return pl.pallas_call(
        far_kernel,
        name="far",
        out_shape=jax.ShapeDtypeStruct((leaves, 3, 128), F32),
        in_specs=[smem] * 3 + [vmem] * 5 + [hbm, hbm],
        out_specs=vmem,
        scratch_shapes=[
            pltpu.VMEM(table.shape, BF16),
            pltpu.VMEM(((blocks * chunks + 54) * PITCH, 128), F32),
            pltpu.VMEM(basis.shape, BF16),
            pltpu.VMEM((9, moments.shape[0], 128), F32),
            pltpu.VMEM((leaves * 24, 1152), F32),
            pltpu.VMEM((8, leaves * 24, 128), F32),
            pltpu.SemaphoreType.DMA((2,)),
        ],
        compiler_params=pltpu.CompilerParams(vmem_limit_bytes=56 << 20),
        cost_estimate=pl.CostEstimate(flops=10**8, bytes_accessed=2 * 10**7, transcendentals=0),
    )(slots, kinds, count, moments, sel, seg, rep, dens, table, basis)


def per_device(
    positions,
    densities,
    near_src,
    near_count,
    far_slot,
    far_class,
    far_count,
    requests,
    up_basis,
    transfer_table,
    down_basis,
):
    leaf_num = near_count.shape[0]
    per_leaf = positions.shape[1] // leaf_num
    width = up_basis.shape[1]
    device = lax.axis_index("patch")
    stacked = jnp.concatenate([positions, densities], 0)
    window = with_halo(stacked, (("patch", 1),), stacked.shape[1])
    window = window.reshape(6, 3 * leaf_num, per_leaf).transpose(1, 0, 2)
    window = jnp.pad(window, ((0, 0), (0, 2), (0, 0)))
    local = stacked.reshape(6, leaf_num, per_leaf).transpose(1, 0, 2)
    offset = (device - 1) * leaf_num
    tgt_sum, src_part = near_call((near_src - offset).reshape(-1), near_count, window)
    near = tgt_sum + src_part[leaf_num : 2 * leaf_num]
    for step_by, piece in ((-1, src_part[:leaf_num]), (1, src_part[2 * leaf_num :])):
        near = near + passed_along(piece, "patch", step_by)
    dens_leaf = local[:, 3:]
    dens_round = dens_leaf.reshape(leaf_num, 3 * per_leaf).astype(BF16)
    moments = jnp.einsum("lrq,lq->lr", up_basis, dens_round, preferred_element_type=F32).astype(BF16)
    asked = lax.all_to_all(requests[0], "patch", split_axis=0, concat_axis=0, tiled=True)
    replies = moments[asked].reshape(asked.shape[0], asked.shape[1] * width)
    table = lax.all_to_all(replies, "patch", split_axis=0, concat_axis=0, tiled=True).reshape(
        -1, width
    )
    far = far_call(
        far_slot.reshape(-1),
        far_class.reshape(-1),
        far_count,
        table,
        dens_leaf,
        transfer_table,
        down_basis,
    )
    return (near + far).transpose(1, 0, 2).reshape(3, leaf_num * per_leaf)


def solution(mesh):
    placed = (
        P(None, "patch"),
        P(None, "patch"),
        P("patch", None),
        P("patch"),
        P("patch", None),
        P("patch", None),
        P("patch"),
        P("patch", None, None),
        P("patch", None, None),
        P(),
        P("patch", None, None, None),
    )
    return jax.shard_map(
        per_device, mesh=mesh, in_specs=placed, out_specs=P(None, "patch"), check_vma=False
    )
```

```python
import functools
import math

import jax
import jax.numpy as jnp
import numpy as np
from jax import lax
from jax.experimental import pallas as pl
from jax.experimental.pallas import tpu as pltpu
from jax.sharding import PartitionSpec as P

KERNEL = 1.0 / (8.0 * math.pi)
BLOB = 0.25
PITCH = 9
SIDE = 4
F32 = jnp.float32
BF16 = jnp.bfloat16
MESH = pl.DeviceIdType.MESH
SMEM = pl.BlockSpec(memory_space=pltpu.SMEM)
VMEM = pl.BlockSpec(memory_space=pltpu.VMEM)
HBM = pl.BlockSpec(memory_space=pltpu.HBM)


def exchange_kernel(
    count, pos_ref, den_ref, up_hbm, wpos_ref, wden_ref, mom_ref, up, up_sem, own_sem, halo_send, halo_recv,
    send_sem, recv_sem, fwd_send, fwd_recv
):
    leaves, width = up.shape[0], up.shape[1]
    chips = SIDE * SIDE * SIDE
    plane = SIDE * SIDE
    me = lax.axis_index("patch")
    core = me % 2
    chip = me // 2
    y, z, x = chip // plane, (chip // SIDE) % SIDE, chip % SIDE
    partner = me + 1 - 2 * core
    other = (me + 2 * core - 1 + count) % count
    before = (me + count - 1) % count
    after = (me + 1) % count

    def peer(k):
        ty = (y + k // plane) % SIDE
        tz = (z + (k // SIDE) % SIDE) % SIDE
        tx = (x + k % SIDE) % SIDE
        return ((ty * SIDE + tz) * SIDE + tx) * 2 + core

    get_up = pltpu.make_async_copy(up_hbm, up, up_sem)
    get_up.start()
    barrier = pltpu.get_barrier_semaphore()

    def greet(k, _):
        pl.semaphore_signal(barrier, inc=1, device_id=(peer(k),), device_id_type=MESH)
        return 0

    pl.semaphore_signal(barrier, inc=1, device_id=(partner,), device_id_type=MESH)
    pl.semaphore_signal(barrier, inc=1, device_id=(other,), device_id_type=MESH)
    lax.fori_loop(1, chips, greet, 0)

    own = []
    for i, (src, dst) in enumerate(((pos_ref, wpos_ref), (den_ref, wden_ref))):
        dst[pl.ds(leaves, leaves)] = src[...]

    rounded = jnp.concatenate([den_ref[:, c, :] for c in range(3)], axis=1)
    row = lax.broadcasted_iota(jnp.int32, rounded.shape, 0)
    get_up.wait()
    total = jnp.zeros((leaves, width), F32)
    for leaf in range(leaves):
        only = jnp.where(row == leaf, rounded, 0.0).astype(BF16)
        total = total + lax.dot_general(
            only, up[leaf], (((1,), (1,)), ((), ())), preferred_element_type=F32
        )
    pad = jnp.zeros((leaves, mom_ref.shape[-1] - width), F32)
    mom_ref[core, y, z * SIDE + x] = jnp.concatenate([total, pad], axis=1).astype(BF16)

    pl.semaphore_wait(barrier, chips + 1)
    halos = []
    for i, (src, dst) in enumerate(((pos_ref, wpos_ref), (den_ref, wden_ref))):
        for j, (target, at) in enumerate(((before, 2 * leaves), (after, 0))):
            halos.append(
                pltpu.make_async_remote_copy(
                    src_ref=src,
                    dst_ref=dst.at[pl.ds(at, leaves)],
                    send_sem=halo_send.at[2 * i + j],
                    recv_sem=halo_recv.at[2 * i + j],
                    device_id=(target,),
                    device_id_type=MESH,
                )
            )
    for copy in halos:
        copy.start()
    mine = mom_ref.at[core, y, z * SIDE + x]

    def send(k, _):
        pltpu.make_async_remote_copy(
            src_ref=mine,
            dst_ref=mine,
            send_sem=send_sem,
            recv_sem=recv_sem.at[k // plane],
            device_id=(peer(k),),
            device_id_type=MESH,
        ).start()
        return 0

    lax.fori_loop(1, chips, send, 0)
    forwards = []
    for group in range(SIDE):
        from_y = (y + SIDE - group) % SIDE
        got = mom_ref.at[core, from_y]
        part = mom_ref.at[core, from_y, pl.ds(0, plane - 1)] if group == 0 else got
        pltpu.make_async_copy(part, part, recv_sem.at[group]).wait()
        forwards.append(
            pltpu.make_async_remote_copy(
                src_ref=got,
                dst_ref=got,
                send_sem=fwd_send.at[group],
                recv_sem=fwd_recv.at[group],
                device_id=(partner,),
                device_id_type=MESH,
            )
        )
        forwards[-1].start()
    for copy in halos + forwards:
        copy.wait()
    sent = mom_ref.at[core, pl.ds(0, SIDE - 1)]
    pltpu.make_async_copy(sent, sent, send_sem).wait()
    sent = mom_ref.at[core, 0, pl.ds(0, plane - 1)]
    pltpu.make_async_copy(sent, sent, send_sem).wait()


def exchange_call(count, pos, den, up):
    leaves, rows, lanes = pos.shape
    return pl.pallas_call(
        functools.partial(exchange_kernel, count),
        name="exchange",
        out_shape=(
            jax.ShapeDtypeStruct((3 * leaves, rows, lanes), F32),
            jax.ShapeDtypeStruct((3 * leaves, rows, lanes), F32),
            jax.ShapeDtypeStruct((2, SIDE, SIDE * SIDE, leaves, 256), BF16),
        ),
        in_specs=[VMEM, VMEM, HBM],
        out_specs=(VMEM, VMEM, VMEM),
        scratch_shapes=[
            pltpu.VMEM(up.shape, BF16),
            pltpu.SemaphoreType.DMA,
            pltpu.SemaphoreType.DMA((2,)),
            pltpu.SemaphoreType.DMA((4,)),
            pltpu.SemaphoreType.DMA((4,)),
            pltpu.SemaphoreType.DMA,
            pltpu.SemaphoreType.DMA((SIDE,)),
            pltpu.SemaphoreType.DMA((SIDE,)),
            pltpu.SemaphoreType.DMA((SIDE,)),
        ],
        compiler_params=pltpu.CompilerParams(
            collective_id=0, has_side_effects=True, vmem_limit_bytes=24 << 20
        ),
    )(pos, den, up)


def near_blocks(near_ref, cnt_ref, wpos_ref, wden_ref, tgt_ref, bef_ref, aft_ref, cols, racc, sacc):
    leaves = tgt_ref.shape[0]
    shift = (lax.axis_index("patch") - 1) * leaves
    tiles = 128 // 8
    sacc[...] = jnp.zeros_like(sacc)

    def spread(pair, _):
        for sub in range(2):
            leaf = pair * 2 + sub
            rows = jnp.concatenate(
                [wpos_ref[leaves + leaf], wden_ref[leaves + leaf], jnp.zeros((2, 128), F32)], axis=0
            )
            turned = jnp.transpose(rows, (1, 0))
            for k in range(6):
                cols[leaf, k] = jnp.broadcast_to(turned[:, k : k + 1], (128, 128))
        return 0

    lax.fori_loop(0, leaves // 2, spread, 0)

    def leaf_step(leaf, _):
        racc[leaf] = jnp.zeros_like(racc[leaf])

        def slot_step(slot, _):
            other = near_ref[slot, leaf] - shift
            xs3, fs3 = wpos_ref[other], wden_ref[other]
            xs = [jnp.broadcast_to(xs3[k : k + 1], (8, 128)) for k in range(3)]
            fs = [jnp.broadcast_to(fs3[k : k + 1], (8, 128)) for k in range(3)]
            down = [jnp.zeros((8, 128), F32) for _ in range(3)]
            for tile in range(tiles):
                part = pl.ds(8 * tile, 8)
                fa = [cols[leaf, 3 + k, part] for k in range(3)]
                sep = [cols[leaf, k, part] - xs[k] for k in range(3)]
                rho = (sep[0] * sep[0] + sep[1] * sep[1]) + (sep[2] * sep[2] + BLOB)
                inv = lax.rsqrt(rho)
                inv_two = inv * inv
                inv_three = inv_two * inv
                ab = fa[0] * fs[0] + fa[1] * fs[1] + fa[2] * fs[2]
                ar = fa[0] * sep[0] + fa[1] * sep[1] + fa[2] * sep[2]
                br = fs[0] * sep[0] + fs[1] * sep[1] + fs[2] * sep[2]
                on_b = ar * inv_three
                on_a = br * inv_three
                on_r = ab * inv_three + (on_b * br) * (inv_two * 3.0)
                for k in range(3):
                    term = fa[k] * on_a + fs[k] * on_b - on_r * sep[k]
                    racc[leaf, k, part] += term
                    down[k] = down[k] + term
            for k in range(3):
                sacc[other, k] -= down[k]
            return 0

        lax.fori_loop(0, cnt_ref[leaf], slot_step, 0)
        return 0

    lax.fori_loop(0, leaves, leaf_step, 0)

    def gather(pair, _):
        for sub in range(2):
            leaf = pair * 2 + sub
            for k in range(3):
                turned = jnp.transpose(racc[leaf, k], (1, 0))
                folded = turned[0:8]
                for tile in range(1, tiles):
                    folded = folded + turned[8 * tile : 8 * tile + 8]
                folded = folded + sacc[leaves + leaf, k]
                row = pl.ds(k, 1)
                tgt_ref[leaf, row] = jnp.sum(folded, axis=0, keepdims=True) * KERNEL
                bef_ref[leaf, row] = jnp.sum(sacc[leaf, k], axis=0, keepdims=True) * KERNEL
                aft_ref[leaf, row] = (
                    jnp.sum(sacc[2 * leaves + leaf, k], axis=0, keepdims=True) * KERNEL
                )
        return 0

    lax.fori_loop(0, leaves // 2, gather, 0)


def middle_kernel(
    near_ref, cnt_ref, slot_ref, class_ref, fcnt_ref, req_ref, wpos_ref, wden_ref, mom_ref, sel_ref, seg_ref, table_hbm,
    tgt_ref, bef_ref, aft_ref, exp_ref, cols, racc, sacc, table, wide, pattern, sums, place, base, sem
):
    leaves = tgt_ref.shape[0]
    classes = table_hbm.shape[0]
    chunks = table_hbm.shape[1] // 128
    get_table = pltpu.make_async_copy(table_hbm, table, sem)
    get_table.start()

    def lookup(leaf, _):
        for slot in range(32):
            v = slot_ref[leaf, slot]
            kind = class_ref[leaf, slot]
            who = v >> 2
            which = req_ref[v & 3, who]
            place[leaf * 32 + slot] = ((who & 1) * (SIDE * SIDE * SIDE) + (who >> 1)) * leaves + which
            base[leaf * 32 + slot] = (kind >> 3) * (chunks * PITCH) + (kind & 7)
        return 0

    lax.fori_loop(0, leaves, lookup, 0)
    near_blocks(near_ref, cnt_ref, wpos_ref, wden_ref, tgt_ref, bef_ref, aft_ref, cols, racc, sacc)

    def spread(step, _):
        rows = pl.ds(pl.multiple_of(step * 128, 128), 128)
        for v in range(9):
            part = sel_ref[:, 128 * v : 128 * v + 128]
            pattern[v, rows] = jnp.dot(mom_ref[rows], part, preferred_element_type=F32)
        return 0

    lax.fori_loop(0, mom_ref.shape[0] // 128, spread, 0)
    get_table.wait()

    def widen(block, _):
        rows = pl.ds(pl.multiple_of(block * 8, 8), 8)
        at = block * (chunks * PITCH)
        for chunk in range(chunks):
            wide[pl.ds(at + chunk * PITCH, 8)] = table[rows, 128 * chunk : 128 * chunk + 128].astype(F32)
        return 0

    full = classes // 8
    rest = classes - 8 * full
    lax.fori_loop(0, full, widen, 0)
    if rest:
        at = full * chunks * PITCH
        for chunk in range(chunks):
            wide[at + chunk * PITCH : at + chunk * PITCH + rest] = table[
                8 * full :, 128 * chunk : 128 * chunk + 128
            ].astype(F32)

    def leaf_step(leaf, _):
        def slot_step(slot, carry):
            at, start, acc = carry
            new = []
            for v in range(9):
                p = jnp.broadcast_to(pattern[v, pl.ds(at, 1), :], (8, 128))
                for g in range(3):
                    t = wide[pl.ds(start + (72 * g + v) * PITCH, 8, stride=9 * PITCH), :]
                    new.append(acc[3 * v + g] + p * t)
            index = jnp.minimum(leaf * 32 + slot + 1, leaves * 32 - 1)
            return place[index], base[index], tuple(new)

        zero = jnp.zeros((8, 128), F32)
        first = leaf * 32
        _, _, acc = lax.fori_loop(0, fcnt_ref[leaf], slot_step, (place[first], base[first], (zero,) * 27))
        for v in range(9):
            for g in range(3):
                rows = pl.ds(pl.multiple_of(leaf * 24 + 8 * g, 8), 8)
                sums[v, rows] = acc[3 * v + g]
        return 0

    lax.fori_loop(0, leaves, leaf_step, 0)
    result = jnp.zeros((leaves * 24, seg_ref.shape[1]), F32)
    for v in range(9):
        total = sums[v]
        high = total.astype(BF16)
        low = (total - high.astype(F32)).astype(BF16)
        part = seg_ref[128 * v : 128 * v + 128]
        result = result + jnp.dot(high, part, preferred_element_type=F32)
        result = result + jnp.dot(low, part, preferred_element_type=F32)
    group = lax.broadcasted_iota(jnp.int32, (24, seg_ref.shape[1]), 0)
    lane = lax.broadcasted_iota(jnp.int32, (24, seg_ref.shape[1]), 1)
    keep = group == (lane >> 3)
    rows = []
    for leaf in range(leaves):
        mine = jnp.where(keep, result[24 * leaf : 24 * leaf + 24], 0.0)
        rows.append(jnp.sum(mine, axis=0, keepdims=True))
    out = jnp.concatenate(rows, axis=0).astype(BF16)
    exp_ref[...] = out[:, : exp_ref.shape[1]]


def middle_consts(width):
    flat = np.arange(9 * 128)
    sel = (flat[None, :] % width == np.arange(256)[:, None]).astype(np.float32)
    seg = (flat[:, None] // width == np.arange(256)[None, :] % 8).astype(np.float32)
    return [jnp.asarray(m, BF16) for m in (sel, seg)]


def middle_call(near, cnt, slots, kinds, fcnt, requests, wpos, wden, mom, table, width):
    leaves = cnt.shape[0]
    classes = table.shape[0]
    chunks = table.shape[1] // 128
    blocks = -(-classes // 8)
    sel, seg = middle_consts(width)
    grad = jax.ShapeDtypeStruct((leaves, 3, 128), F32)
    return pl.pallas_call(
        middle_kernel,
        name="middle",
        out_shape=(grad, grad, grad, jax.ShapeDtypeStruct((leaves, width), BF16)),
        in_specs=[SMEM] * 6 + [VMEM] * 5 + [HBM],
        out_specs=(VMEM,) * 4,
        scratch_shapes=[
            pltpu.VMEM((leaves, 6, 128, 128), F32),
            pltpu.VMEM((leaves, 3, 128, 128), F32),
            pltpu.VMEM((3 * leaves, 3, 8, 128), F32),
            pltpu.VMEM(table.shape, BF16),
            pltpu.VMEM(((blocks * chunks + 54) * PITCH, 128), F32),
            pltpu.VMEM((9, mom.shape[0], 128), F32),
            pltpu.VMEM((9, leaves * 24, 128), F32),
            pltpu.SMEM((leaves * 32,), jnp.int32),
            pltpu.SMEM((leaves * 32,), jnp.int32),
            pltpu.SemaphoreType.DMA,
        ],
        compiler_params=pltpu.CompilerParams(vmem_limit_bytes=60 << 20),
        cost_estimate=pl.CostEstimate(flops=10**8, bytes_accessed=10**7, transcendentals=10**6),
    )(near, cnt, slots, kinds, fcnt, requests, wpos, wden, mom, sel, seg, table)


def final_kernel(
    count, exp_ref, den_ref, tgt_ref, bef_ref, aft_ref, basis_hbm, out_ref, basis, got, sem, send_sem, recv_sem
):
    leaves, parts = basis.shape[0], basis.shape[1]
    me = lax.axis_index("patch")
    before = (me + count - 1) % count
    after = (me + 1) % count
    half = leaves // 2
    gets = []
    for i in range(2):
        part = pl.ds(half * i, half)
        gets.append(pltpu.make_async_copy(basis_hbm.at[part], basis.at[part], sem.at[i]))
        gets[-1].start()
    barrier = pltpu.get_barrier_semaphore()
    for target in (before, after):
        pl.semaphore_signal(barrier, inc=1, device_id=(target,), device_id_type=MESH)
    pl.semaphore_wait(barrier, 2)
    copies = []
    for i, (src, target) in enumerate(((bef_ref, before), (aft_ref, after))):
        copies.append(
            pltpu.make_async_remote_copy(
                src_ref=src,
                dst_ref=got.at[i],
                send_sem=send_sem.at[i],
                recv_sem=recv_sem.at[i],
                device_id=(target,),
                device_id_type=MESH,
            )
        )
        copies[-1].start()
    expansion = exp_ref[...]
    row = lax.broadcasted_iota(jnp.int32, expansion.shape, 0)
    field = [jnp.zeros((leaves, 128), F32) for _ in range(parts)]
    for leaf in range(leaves):
        if leaf % half == 0:
            gets[leaf // half].wait()
        only = jnp.where(row == leaf, expansion, jnp.zeros_like(expansion))
        for q in range(parts):
            field[q] = field[q] + jnp.dot(only, basis[leaf, q], preferred_element_type=F32)
    far = []
    for k in range(3):
        part = den_ref[:, 0, :] * field[k]
        for c in range(1, 3):
            part = part + den_ref[:, c, :] * field[3 * c + k]
        far.append(part)
    for copy in copies:
        copy.wait()
    for k in range(3):
        out_ref[:, k, :] = far[k] + (tgt_ref[:, k, :] + (got[0, :, k, :] + got[1, :, k, :]))


def final_call(count, expansion, den, tgt, bef, aft, basis):
    leaves = den.shape[0]
    return pl.pallas_call(
        functools.partial(final_kernel, count),
        name="final",
        out_shape=jax.ShapeDtypeStruct(den.shape, F32),
        in_specs=[VMEM] * 5 + [HBM],
        out_specs=VMEM,
        scratch_shapes=[
            pltpu.VMEM(basis.shape, BF16),
            pltpu.VMEM((2,) + den.shape, F32),
            pltpu.SemaphoreType.DMA((2,)),
            pltpu.SemaphoreType.DMA((2,)),
            pltpu.SemaphoreType.DMA((2,)),
        ],
        compiler_params=pltpu.CompilerParams(
            collective_id=1, has_side_effects=True, vmem_limit_bytes=24 << 20
        ),
    )(expansion, den, tgt, bef, aft, basis)


def per_device(
    count,
    positions,
    densities,
    near_src,
    near_count,
    far_slot,
    far_class,
    far_count,
    requests,
    up_basis,
    transfer_table,
    down_basis,
):
    leaves = near_count.shape[0]
    width = up_basis.shape[1]

    def by_leaf(a):
        return a.reshape(3, leaves, -1).transpose(1, 0, 2)

    pos, den = by_leaf(positions), by_leaf(densities)
    wpos, wden, mom = exchange_call(count, pos, den, up_basis)
    tgt, bef, aft, expansion = middle_call(
        near_src.T,
        near_count,
        far_slot,
        far_class,
        far_count,
        requests[0].T,
        wpos,
        wden,
        mom.reshape(-1, mom.shape[-1]),
        transfer_table,
        width,
    )
    out = final_call(count, expansion, den, tgt, bef, aft, down_basis.transpose(0, 2, 1, 3))
    return out.transpose(1, 0, 2).reshape(3, -1)


def solution(mesh):
    placed = (
        P(None, "patch"),
        P(None, "patch"),
        P("patch", None),
        P("patch"),
        P("patch", None),
        P("patch", None),
        P("patch"),
        P("patch", None, None),
        P("patch", None, None),
        P(),
        P("patch", None, None, None),
    )
    return jax.shard_map(
        functools.partial(per_device, mesh.shape["patch"]),
        mesh=mesh,
        in_specs=placed,
        out_specs=P(None, "patch"),
        check_vma=False,
    )
```

```python
import functools
import math

import jax
import jax.numpy as jnp
import numpy as np
from jax import lax
from jax.experimental import pallas as pl
from jax.experimental.pallas import tpu as pltpu
from jax.sharding import PartitionSpec as P

KERNEL = 1.0 / (8.0 * math.pi)
BLOB = 0.25
PITCH = 9
SIDE = 4
F32 = jnp.float32
BF16 = jnp.bfloat16
MESH = pl.DeviceIdType.MESH
SMEM = pl.BlockSpec(memory_space=pltpu.SMEM)
VMEM = pl.BlockSpec(memory_space=pltpu.VMEM)
HBM = pl.BlockSpec(memory_space=pltpu.HBM)
MIB = 1 << 20
LIMIT = 8 * MIB


def in_hbm(*arrays):
    return [pltpu.with_memory_space_constraint(a, pltpu.HBM) for a in arrays]

EARLY = 4


def pair_block(leaf, source_x, source_f, cols, racc):
    xs = [jnp.broadcast_to(source_x[k : k + 1], (8, 128)) for k in range(3)]
    fs = [jnp.broadcast_to(source_f[k : k + 1], (8, 128)) for k in range(3)]
    down = [jnp.zeros((8, 128), F32) for _ in range(3)]
    for tile in range(16):
        part = pl.ds(8 * tile, 8)
        fa = [cols[leaf, 3 + k, part] for k in range(3)]
        sep = [cols[leaf, k, part] - xs[k] for k in range(3)]
        rho = (sep[0] * sep[0] + sep[1] * sep[1]) + (sep[2] * sep[2] + BLOB)
        inv = lax.rsqrt(rho)
        inv_two = inv * inv
        inv_three = inv_two * inv
        ab = fa[0] * fs[0] + fa[1] * fs[1] + fa[2] * fs[2]
        ar = fa[0] * sep[0] + fa[1] * sep[1] + fa[2] * sep[2]
        br = fs[0] * sep[0] + fs[1] * sep[1] + fs[2] * sep[2]
        on_b = ar * inv_three
        on_a = br * inv_three
        on_r = ab * inv_three + (on_b * br) * (inv_two * 3.0)
        for k in range(3):
            term = fa[k] * on_a + fs[k] * on_b - on_r * sep[k]
            racc[leaf, k, part] += term
            down[k] = down[k] + term
    return down


def exchange_kernel(
    count, near_ref, cnt_ref, pos_ref, den_ref, up_hbm, wpos_ref, wden_ref, mom_ref, cols, racc, early_ref, up, own, theirs,
    up_sem, pair_send, pair_recv, halo_send, halo_recv, send_sem, recv_sem
):
    leaves, width = up.shape[0], up.shape[1]
    plane = SIDE * SIDE
    chips = plane * SIDE
    me = lax.axis_index("patch")
    core = me % 2
    chip = me // 2
    y, z, x = chip // plane, (chip // SIDE) % SIDE, chip % SIDE
    partner = me + 1 - 2 * core
    other_side = (me + 2 * core - 1 + count) % count
    before = (me + count - 1) % count
    after = (me + 1) % count
    at_y = [((y + k) % SIDE) * (2 * plane) + core for k in range(SIDE)]
    at_z = [((z + k) % SIDE) * (2 * SIDE) for k in range(SIDE)]
    at_x = [((x + k) % SIDE) * 2 for k in range(SIDE)]
    steps = [(a, b, c) for a in range(SIDE) for b in range(SIDE) for c in range(SIDE)][1:]
    steps.sort(key=lambda s: -sum(min(v, SIDE - v) for v in s))
    peers = [at_y[a] + at_z[b] + at_x[c] for a, b, c in steps]

    get_up = pltpu.make_async_copy(up_hbm, up, up_sem)
    get_up.start()
    barrier = pltpu.get_barrier_semaphore()
    for target in [partner] + peers + [other_side]:
        pl.semaphore_signal(barrier, inc=1, device_id=(target,), device_id_type=MESH)

    wpos_ref[pl.ds(leaves, leaves)] = pos_ref[...]
    wden_ref[pl.ds(leaves, leaves)] = den_ref[...]
    rounded = jnp.concatenate([den_ref[:, c, :] for c in range(3)], axis=1)
    row = lax.broadcasted_iota(jnp.int32, rounded.shape, 0)

    def spread(pair, _):
        for sub in range(2):
            leaf = pair * 2 + sub
            rows = jnp.concatenate([pos_ref[leaf], den_ref[leaf], jnp.zeros((2, 128), F32)], axis=0)
            turned = jnp.transpose(rows, (1, 0))
            for k in range(6):
                cols[leaf, k] = jnp.broadcast_to(turned[:, k : k + 1], (128, 128))
        return 0

    get_up.wait()
    total = jnp.zeros((leaves, width), F32)
    for leaf in range(leaves):
        only = jnp.where(row == leaf, rounded, 0.0).astype(BF16)
        total = total + lax.dot_general(
            only, up[leaf], (((1,), (1,)), ((), ())), preferred_element_type=F32
        )
    main = total[:, :128]
    tail = jnp.concatenate([total[:, 128:]] * (128 // (width - 128)), axis=1)
    lane = lax.broadcasted_iota(jnp.int32, tail.shape, 1)
    leaf_of = lax.broadcasted_iota(jnp.int32, tail.shape, 0)
    per_row = 128 // (width - 128)
    tail = jnp.where(lane // (width - 128) == leaf_of % per_row, tail, 0.0)
    ends = [
        jnp.sum(tail[i * per_row : (i + 1) * per_row], axis=0, keepdims=True)
        for i in range(leaves // per_row)
    ]
    fill = jnp.zeros((8 - len(ends), 128), F32)
    own[...] = jnp.concatenate([main] + ends + [fill], axis=0).astype(BF16)
    lax.fori_loop(0, leaves // 2, spread, 0)
    racc[...] = jnp.zeros_like(racc)

    pl.semaphore_wait(barrier, chips + 1)
    to_partner = pltpu.make_async_remote_copy(
        src_ref=own,
        dst_ref=theirs,
        send_sem=pair_send,
        recv_sem=pair_recv,
        device_id=(partner,),
        device_id_type=MESH,
    )
    to_partner.start()
    halos = []
    for i, (src, dst) in enumerate(((pos_ref, wpos_ref), (den_ref, wden_ref))):
        for j, (target, at) in enumerate(((before, 2 * leaves), (after, 0))):
            halos.append(
                pltpu.make_async_remote_copy(
                    src_ref=src,
                    dst_ref=dst.at[pl.ds(at, leaves)],
                    send_sem=halo_send.at[2 * i + j],
                    recv_sem=halo_recv.at[2 * i + j],
                    device_id=(target,),
                    device_id_type=MESH,
                )
            )
    for copy in halos:
        copy.start()
    to_partner.wait_recv()
    mine, his = own[...].astype(F32), theirs[...].astype(F32)
    first = jnp.where(core == 0, mine, his)
    second = jnp.where(core == 0, his, mine)
    main_rows = leaves
    mom_ref[chip] = jnp.concatenate(
        [
            first[:main_rows],
            second[:main_rows],
            first[main_rows : main_rows + 2],
            second[main_rows : main_rows + 2],
            jnp.zeros((4, 128), F32),
        ],
        axis=0,
    ).astype(BF16)
    block = mom_ref.at[chip]
    for target in peers:
        pltpu.make_async_remote_copy(
            src_ref=block,
            dst_ref=block,
            send_sem=send_sem,
            recv_sem=recv_sem,
            device_id=(target,),
            device_id_type=MESH,
        ).start()
    for copy in halos:
        copy.wait()

    shift = (me - 1) * leaves

    def early(leaf, _):
        for slot in range(EARLY):
            source = jnp.clip(near_ref[slot, leaf] - shift, 0, 3 * leaves - 1)
            live = jnp.where(slot < cnt_ref[leaf], 1.0, 0.0)
            down = pair_block(leaf, wpos_ref[source], wden_ref[source] * live, cols, racc)
            early_ref[leaf, slot] = jnp.concatenate(
                [jnp.sum(d, axis=0, keepdims=True) for d in down], axis=0
            )
        return 0

    lax.fori_loop(0, leaves, early, 0)
    to_partner.wait_send()
    moved = mom_ref.at[pl.ds(0, chips - 1)]
    pltpu.make_async_copy(moved, moved, send_sem).wait()
    pltpu.make_async_copy(moved, moved, recv_sem).wait()


def exchange_call(count, near, cnt, pos, den, up):
    leaves, rows, lanes = pos.shape
    window = jax.ShapeDtypeStruct((3 * leaves, rows, lanes), F32)
    return pl.pallas_call(
        functools.partial(exchange_kernel, count),
        name="exchange",
        out_shape=(
            window,
            window,
            jax.ShapeDtypeStruct((count // 2, 40, 128), BF16),
            jax.ShapeDtypeStruct((leaves, 6, 128, 128), F32),
            jax.ShapeDtypeStruct((leaves, 3, 128, 128), F32),
            jax.ShapeDtypeStruct((leaves, EARLY, 3, 128), F32),
        ),
        in_specs=[SMEM, SMEM, VMEM, VMEM, HBM],
        out_specs=(VMEM,) * 6,
        scratch_shapes=[
            pltpu.VMEM(up.shape, BF16),
            pltpu.VMEM((24, 128), BF16),
            pltpu.VMEM((24, 128), BF16),
            pltpu.SemaphoreType.DMA,
            pltpu.SemaphoreType.DMA,
            pltpu.SemaphoreType.DMA,
            pltpu.SemaphoreType.DMA((4,)),
            pltpu.SemaphoreType.DMA((4,)),
            pltpu.SemaphoreType.DMA,
            pltpu.SemaphoreType.DMA,
        ],
        compiler_params=pltpu.CompilerParams(
            collective_id=0, has_side_effects=True, vmem_limit_bytes=LIMIT
        ),
    )(*in_hbm(near, cnt, pos, den, up))


def near_kernel(near_ref, cnt_ref, wpos_ref, wden_ref, cols, before_acc, early_ref, tgt_ref, bef_ref, aft_ref, racc, sacc):
    leaves = tgt_ref.shape[0]
    shift = (lax.axis_index("patch") - 1) * leaves
    sacc[...] = jnp.zeros_like(sacc)

    def leaf_step(leaf, _):
        racc[leaf] = jnp.zeros_like(racc[leaf])
        for slot in range(EARLY):
            other = near_ref[slot, leaf] - shift
            sacc[other, :, 0, :] += early_ref[leaf, slot]

        def slot_step(slot, _):
            other = near_ref[slot, leaf] - shift
            down = pair_block(leaf, wpos_ref[other], wden_ref[other], cols, racc)
            for k in range(3):
                sacc[other, k] += down[k]
            return 0

        lax.fori_loop(EARLY, cnt_ref[leaf], slot_step, 0)
        return 0

    lax.fori_loop(0, leaves, leaf_step, 0)

    def gather(pair, _):
        for sub in range(2):
            leaf = pair * 2 + sub
            for k in range(3):
                turned = jnp.transpose(racc[leaf, k] + before_acc[leaf, k], (1, 0))
                folded = turned[0:8]
                for tile in range(1, 16):
                    folded = folded + turned[8 * tile : 8 * tile + 8]
                folded = folded - sacc[leaves + leaf, k]
                row = pl.ds(k, 1)
                tgt_ref[leaf, row] = jnp.sum(folded, axis=0, keepdims=True) * KERNEL
                bef_ref[leaf, row] = jnp.sum(sacc[leaf, k], axis=0, keepdims=True) * -KERNEL
                aft_ref[leaf, row] = (
                    jnp.sum(sacc[2 * leaves + leaf, k], axis=0, keepdims=True) * -KERNEL
                )
        return 0

    lax.fori_loop(0, leaves // 2, gather, 0)


def near_call(near, cnt, wpos, wden, cols, racc, early):
    leaves = cnt.shape[0]
    grad = jax.ShapeDtypeStruct((leaves, 3, 128), F32)
    return pl.pallas_call(
        near_kernel,
        name="near",
        out_shape=(grad, grad, grad),
        in_specs=[SMEM] * 2 + [VMEM] * 5,
        out_specs=(VMEM,) * 3,
        scratch_shapes=[
            pltpu.VMEM((leaves, 3, 128, 128), F32),
            pltpu.VMEM((3 * leaves, 3, 8, 128), F32),
        ],
        compiler_params=pltpu.CompilerParams(vmem_limit_bytes=LIMIT),
        cost_estimate=pl.CostEstimate(flops=10**8, bytes_accessed=10**7, transcendentals=10**6),
    )(*in_hbm(near, cnt), wpos, wden, cols, racc, early)


def back_kernel(count, bef_ref, aft_ref, mom_ref, sel_ref, table, got, wide, pattern, send_sem, recv_sem):
    classes = table.shape[0]
    chunks = table.shape[1] // 128
    me = lax.axis_index("patch")
    before = (me + count - 1) % count
    after = (me + 1) % count
    barrier = pltpu.get_barrier_semaphore()
    for target in (before, after):
        pl.semaphore_signal(barrier, inc=1, device_id=(target,), device_id_type=MESH)
    pl.semaphore_wait(barrier, 2)
    copies = []
    for i, (src, target) in enumerate(((bef_ref, before), (aft_ref, after))):
        copies.append(
            pltpu.make_async_remote_copy(
                src_ref=src,
                dst_ref=got.at[i],
                send_sem=send_sem.at[i],
                recv_sem=recv_sem.at[i],
                device_id=(target,),
                device_id_type=MESH,
            )
        )
        copies[-1].start()
    lane = lax.broadcasted_iota(jnp.int32, (8, 128), 1)
    mine = lane // 16 == lax.broadcasted_iota(jnp.int32, (8, 128), 0)

    def spread(step, _):
        lefts, rights = [], []
        for sub in range(8):
            block = mom_ref[step * 8 + sub]
            lefts.append(block[:32])
            ends = block[32:40].astype(F32)
            for i in range(4):
                rights.append(jnp.where(mine, jnp.broadcast_to(ends[i : i + 1], (8, 128)), 0.0))
        lhs = jnp.concatenate(
            [jnp.concatenate(lefts, axis=0), jnp.concatenate(rights, axis=0).astype(BF16)], axis=1
        )
        rows = pl.ds(pl.multiple_of(step * 256, 256), 256)
        for v in range(0, 9, 2):
            some = min(2, 9 - v)
            out = jnp.dot(lhs, sel_ref[:, 128 * v : 128 * (v + some)], preferred_element_type=F32)
            for i in range(some):
                pattern[v + i, rows] = out[:, 128 * i : 128 * i + 128]
        return 0

    lax.fori_loop(0, mom_ref.shape[0] // 8, spread, 0)

    def widen(block, _):
        rows = pl.ds(pl.multiple_of(block * 8, 8), 8)
        at = block * (chunks * PITCH)
        for chunk in range(chunks):
            wide[pl.ds(at + chunk * PITCH, 8)] = table[rows, 128 * chunk : 128 * chunk + 128].astype(F32)
        return 0

    full = classes // 8
    rest = classes - 8 * full
    lax.fori_loop(0, full, widen, 0)
    if rest:
        at = full * chunks * PITCH
        for chunk in range(chunks):
            wide[at + chunk * PITCH : at + chunk * PITCH + rest] = table[
                8 * full :, 128 * chunk : 128 * chunk + 128
            ].astype(F32)
    for copy in copies:
        copy.wait()


def back_call(count, bef, aft, mom, table, width):
    leaves = bef.shape[0]
    chunks = table.shape[1] // 128
    blocks = -(-table.shape[0] // 8)
    sel, _ = constants(width)
    return pl.pallas_call(
        functools.partial(back_kernel, count),
        name="back",
        out_shape=(
            jax.ShapeDtypeStruct((2,) + bef.shape, F32),
            jax.ShapeDtypeStruct(((blocks * chunks + 54) * PITCH, 128), F32),
            jax.ShapeDtypeStruct((9, count * leaves, 128), F32),
        ),
        in_specs=[VMEM] * 5,
        out_specs=(VMEM,) * 3,
        scratch_shapes=[
            pltpu.SemaphoreType.DMA((2,)),
            pltpu.SemaphoreType.DMA((2,)),
        ],
        compiler_params=pltpu.CompilerParams(
            collective_id=1, has_side_effects=True, vmem_limit_bytes=LIMIT
        ),
    )(bef, aft, mom, sel, table)


def far_kernel(
    slot_ref, class_ref, fcnt_ref, req_ref, wide, pattern, seg_ref, basis, den_ref, tgt_ref, got, out_ref, sums
):
    leaves, parts = basis.shape[0], basis.shape[1]
    width = basis.shape[2]
    block_rows = width * width // 128 * PITCH

    def leaf_step(leaf, _):
        def fetch(slot):
            v = slot_ref[leaf, slot]
            kind = class_ref[leaf, slot]
            who = v >> 2
            return who * leaves + req_ref[v & 3, who], (kind >> 3) * block_rows + (kind & 7)

        def slot_step(slot, carry):
            at, start, acc = carry
            following = fetch(jnp.minimum(slot + 1, 31))
            new = []
            for v in range(9):
                p = jnp.broadcast_to(pattern[v, pl.ds(at, 1), :], (8, 128))
                for g in range(3):
                    t = wide[pl.ds(start + (72 * g + v) * PITCH, 8, stride=9 * PITCH), :]
                    new.append(acc[3 * v + g] + p * t)
            return following[0], following[1], tuple(new)

        zero = jnp.zeros((8, 128), F32)
        at, start = fetch(0)
        _, _, acc = lax.fori_loop(0, fcnt_ref[leaf], slot_step, (at, start, (zero,) * 27))
        for v in range(9):
            for g in range(3):
                rows = pl.ds(pl.multiple_of(leaf * 24 + 8 * g, 8), 8)
                sums[v, rows] = acc[3 * v + g]
        return 0

    lax.fori_loop(0, leaves, leaf_step, 0)
    result = jnp.zeros((leaves * 24, seg_ref.shape[1]), F32)
    for v in range(9):
        total = sums[v]
        high = total.astype(BF16)
        low = (total - high.astype(F32)).astype(BF16)
        part = seg_ref[128 * v : 128 * v + 128]
        result = result + jnp.dot(high, part, preferred_element_type=F32)
        result = result + jnp.dot(low, part, preferred_element_type=F32)
    group = lax.broadcasted_iota(jnp.int32, (24, seg_ref.shape[1]), 0)
    lane = lax.broadcasted_iota(jnp.int32, (24, seg_ref.shape[1]), 1)
    keep = group == (lane >> 3)
    rows = []
    for leaf in range(leaves):
        mine = jnp.where(keep, result[24 * leaf : 24 * leaf + 24], 0.0)
        rows.append(jnp.sum(mine, axis=0, keepdims=True))
    expansion = jnp.concatenate(rows, axis=0)[:, :width].astype(BF16)
    row = lax.broadcasted_iota(jnp.int32, expansion.shape, 0)
    field = [jnp.zeros((leaves, 128), F32) for _ in range(parts)]
    for leaf in range(leaves):
        only = jnp.where(row == leaf, expansion, jnp.zeros_like(expansion))
        for q in range(parts):
            field[q] = field[q] + jnp.dot(only, basis[leaf, q], preferred_element_type=F32)
    for k in range(3):
        far = den_ref[:, 0, :] * field[k]
        for c in range(1, 3):
            far = far + den_ref[:, c, :] * field[3 * c + k]
        out_ref[:, k, :] = far + (tgt_ref[:, k, :] + (got[0, :, k, :] + got[1, :, k, :]))


def constants(width):
    flat = np.arange(9 * 128)
    sel = np.zeros((256, 9 * 128), np.float32)
    place = flat % width
    sel[:128] = place[None, :] == np.arange(128)[:, None]
    sel[128:] = (place[None, :] >= 128) & ((place[None, :] - 128) == np.arange(128)[:, None] % (width - 128))
    seg = (flat[:, None] // width == np.arange(256)[None, :] % 8).astype(np.float32)
    return [jnp.asarray(m, BF16) for m in (sel, seg)]


def far_call(slots, kinds, fcnt, requests, wide, pattern, basis, den, tgt, got):
    leaves = den.shape[0]
    _, seg = constants(basis.shape[2])
    return pl.pallas_call(
        far_kernel,
        name="far",
        out_shape=jax.ShapeDtypeStruct(den.shape, F32),
        in_specs=[SMEM] * 4 + [VMEM] * 7,
        out_specs=VMEM,
        scratch_shapes=[pltpu.VMEM((9, leaves * 24, 128), F32)],
        compiler_params=pltpu.CompilerParams(vmem_limit_bytes=LIMIT),
        cost_estimate=pl.CostEstimate(flops=10**8, bytes_accessed=10**7, transcendentals=0),
    )(slots, kinds, fcnt, requests, wide, pattern, seg, basis, den, tgt, got)


def per_device(
    count,
    positions,
    densities,
    near_src,
    near_count,
    far_slot,
    far_class,
    far_count,
    requests,
    up_basis,
    transfer_table,
    down_basis,
):
    leaves = near_count.shape[0]
    width = up_basis.shape[1]

    def by_leaf(a):
        return a.reshape(3, leaves, -1).transpose(1, 0, 2)

    pos, den = by_leaf(positions), by_leaf(densities)
    near = near_src.T
    wpos, wden, mom, cols, racc, early = exchange_call(count, near, near_count, pos, den, up_basis)
    tgt, bef, aft = near_call(near, near_count, wpos, wden, cols, racc, early)
    got, wide, pattern = back_call(count, bef, aft, mom, transfer_table, width)
    out = far_call(
        far_slot,
        far_class,
        far_count,
        requests[0].T,
        wide,
        pattern,
        down_basis.transpose(0, 2, 1, 3),
        den,
        tgt,
        got,
    )
    return out.transpose(1, 0, 2).reshape(3, -1)


def solution(mesh):
    placed = (
        P(None, "patch"),
        P(None, "patch"),
        P("patch", None),
        P("patch"),
        P("patch", None),
        P("patch", None),
        P("patch"),
        P("patch", None, None),
        P("patch", None, None),
        P(),
        P("patch", None, None, None),
    )
    return jax.shard_map(
        functools.partial(per_device, mesh.shape["patch"]),
        mesh=mesh,
        in_specs=placed,
        out_specs=P(None, "patch"),
        check_vma=False,
    )
```

```python
import functools
import math

import jax
import jax.numpy as jnp
import numpy as np
from jax import lax
from jax.experimental import pallas as pl
from jax.experimental.pallas import tpu as pltpu
from jax.sharding import PartitionSpec as P

KERNEL = 1.0 / (8.0 * math.pi)
BLOB = 0.25
SIDE = 4
F32 = jnp.float32
BF16 = jnp.bfloat16
MESH = pl.DeviceIdType.MESH
SMEM = pl.BlockSpec(memory_space=pltpu.SMEM)
VMEM = pl.BlockSpec(memory_space=pltpu.VMEM)
HBM = pl.BlockSpec(memory_space=pltpu.HBM)
MIB = 1 << 20
LIMIT = 8 * MIB


def in_hbm(*arrays):
    return [pltpu.with_memory_space_constraint(a, pltpu.HBM) for a in arrays]

UNROLL = 2
EARLY = 4


def pair_block(leaf, source_x, source_f, cols, racc):
    xs = [jnp.broadcast_to(source_x[k : k + 1], (8, 128)) for k in range(3)]
    fs = [jnp.broadcast_to(source_f[k : k + 1], (8, 128)) for k in range(3)]
    down = [jnp.zeros((8, 128), F32) for _ in range(3)]
    for tile in range(16):
        part = pl.ds(8 * tile, 8)
        fa = [cols[leaf, 3 + k, part] for k in range(3)]
        sep = [cols[leaf, k, part] - xs[k] for k in range(3)]
        rho = (sep[0] * sep[0] + sep[1] * sep[1]) + (sep[2] * sep[2] + BLOB)
        inv = lax.rsqrt(rho)
        inv_two = inv * inv
        inv_three = inv_two * inv
        ab = fa[0] * fs[0] + fa[1] * fs[1] + fa[2] * fs[2]
        ar = fa[0] * sep[0] + fa[1] * sep[1] + fa[2] * sep[2]
        br = fs[0] * sep[0] + fs[1] * sep[1] + fs[2] * sep[2]
        on_b = ar * inv_three
        on_a = br * inv_three
        on_r = ab * inv_three + (on_b * br) * (inv_two * 3.0)
        for k in range(3):
            term = fa[k] * on_a + fs[k] * on_b - on_r * sep[k]
            racc[leaf, k, part] += term
            down[k] = down[k] + term
    return down


def exchange_kernel(
    count, near_ref, cnt_ref, pos_ref, den_ref, up_hbm, wpos_ref, wden_ref, mom_ref, cols, racc, early_ref, up, own, theirs,
    up_sem, pair_send, pair_recv, halo_send, halo_recv, send_sem, recv_sem
):
    leaves, width = up.shape[0], up.shape[1]
    plane = SIDE * SIDE
    chips = plane * SIDE
    me = lax.axis_index("patch")
    core = me % 2
    chip = me // 2
    y, z, x = chip // plane, (chip // SIDE) % SIDE, chip % SIDE
    partner = me + 1 - 2 * core
    other_side = (me + 2 * core - 1 + count) % count
    before = (me + count - 1) % count
    after = (me + 1) % count
    at_y = [((y + k) % SIDE) * (2 * plane) + core for k in range(SIDE)]
    at_z = [((z + k) % SIDE) * (2 * SIDE) for k in range(SIDE)]
    at_x = [((x + k) % SIDE) * 2 for k in range(SIDE)]
    steps = [(a, b, c) for a in range(SIDE) for b in range(SIDE) for c in range(SIDE)][1:]
    steps.sort(key=lambda s: -sum(min(v, SIDE - v) for v in s))
    peers = [at_y[a] + at_z[b] + at_x[c] for a, b, c in steps]

    get_up = pltpu.make_async_copy(up_hbm, up, up_sem)
    get_up.start()
    barrier = pltpu.get_barrier_semaphore()
    for target in [partner] + peers + [other_side]:
        pl.semaphore_signal(barrier, inc=1, device_id=(target,), device_id_type=MESH)

    wpos_ref[pl.ds(leaves, leaves)] = pos_ref[...]
    wden_ref[pl.ds(leaves, leaves)] = den_ref[...]
    rounded = jnp.concatenate([den_ref[:, c, :] for c in range(3)], axis=1)
    row = lax.broadcasted_iota(jnp.int32, rounded.shape, 0)

    def spread(pair, _):
        for sub in range(2):
            leaf = pair * 2 + sub
            rows = jnp.concatenate([pos_ref[leaf], den_ref[leaf], jnp.zeros((2, 128), F32)], axis=0)
            turned = jnp.transpose(rows, (1, 0))
            for k in range(6):
                cols[leaf, k] = jnp.broadcast_to(turned[:, k : k + 1], (128, 128))
        return 0

    get_up.wait()
    total = jnp.zeros((leaves, width), F32)
    for leaf in range(leaves):
        only = jnp.where(row == leaf, rounded, 0.0).astype(BF16)
        total = total + lax.dot_general(
            only, up[leaf], (((1,), (1,)), ((), ())), preferred_element_type=F32
        )
    main = total[:, :128]
    tail = jnp.concatenate([total[:, 128:]] * (128 // (width - 128)), axis=1)
    lane = lax.broadcasted_iota(jnp.int32, tail.shape, 1)
    leaf_of = lax.broadcasted_iota(jnp.int32, tail.shape, 0)
    per_row = 128 // (width - 128)
    tail = jnp.where(lane // (width - 128) == leaf_of % per_row, tail, 0.0)
    ends = [
        jnp.sum(tail[i * per_row : (i + 1) * per_row], axis=0, keepdims=True)
        for i in range(leaves // per_row)
    ]
    fill = jnp.zeros((8 - len(ends), 128), F32)
    own[...] = jnp.concatenate([main] + ends + [fill], axis=0).astype(BF16)
    pl.semaphore_wait(barrier, chips + 1)
    to_partner = pltpu.make_async_remote_copy(
        src_ref=own,
        dst_ref=theirs,
        send_sem=pair_send,
        recv_sem=pair_recv,
        device_id=(partner,),
        device_id_type=MESH,
    )
    to_partner.start()
    halos = []
    for i, (src, dst) in enumerate(((pos_ref, wpos_ref), (den_ref, wden_ref))):
        for j, (target, at) in enumerate(((before, 2 * leaves), (after, 0))):
            halos.append(
                pltpu.make_async_remote_copy(
                    src_ref=src,
                    dst_ref=dst.at[pl.ds(at, leaves)],
                    send_sem=halo_send.at[2 * i + j],
                    recv_sem=halo_recv.at[2 * i + j],
                    device_id=(target,),
                    device_id_type=MESH,
                )
            )
    for copy in halos:
        copy.start()
    to_partner.wait_recv()
    mine, his = own[...].astype(F32), theirs[...].astype(F32)
    first = jnp.where(core == 0, mine, his)
    second = jnp.where(core == 0, his, mine)
    main_rows = leaves
    mom_ref[chip] = jnp.concatenate(
        [
            first[:main_rows],
            second[:main_rows],
            first[main_rows : main_rows + 2],
            second[main_rows : main_rows + 2],
            jnp.zeros((4, 128), F32),
        ],
        axis=0,
    ).astype(BF16)
    block = mom_ref.at[chip]
    for target in peers:
        pltpu.make_async_remote_copy(
            src_ref=block,
            dst_ref=block,
            send_sem=send_sem,
            recv_sem=recv_sem,
            device_id=(target,),
            device_id_type=MESH,
        ).start()
    lax.fori_loop(0, leaves // 2, spread, 0)
    racc[...] = jnp.zeros_like(racc)
    for copy in halos:
        copy.wait()

    shift = (me - 1) * leaves

    def early(leaf, _):
        for slot in range(EARLY):
            source = jnp.clip(near_ref[slot, leaf] - shift, 0, 3 * leaves - 1)
            live = jnp.where(slot < cnt_ref[leaf], 1.0, 0.0)
            down = pair_block(leaf, wpos_ref[source], wden_ref[source] * live, cols, racc)
            early_ref[leaf, slot] = jnp.concatenate(
                [jnp.sum(d, axis=0, keepdims=True) for d in down], axis=0
            )
        return 0

    lax.fori_loop(0, leaves, early, 0)
    to_partner.wait_send()
    moved = mom_ref.at[pl.ds(0, chips - 1)]
    pltpu.make_async_copy(moved, moved, send_sem).wait()
    pltpu.make_async_copy(moved, moved, recv_sem).wait()


def exchange_call(count, near, cnt, pos, den, up):
    leaves, rows, lanes = pos.shape
    window = jax.ShapeDtypeStruct((3 * leaves, rows, lanes), F32)
    return pl.pallas_call(
        functools.partial(exchange_kernel, count),
        name="exchange",
        out_shape=(
            window,
            window,
            jax.ShapeDtypeStruct((count // 2, 40, 128), BF16),
            jax.ShapeDtypeStruct((leaves, 6, 128, 128), F32),
            jax.ShapeDtypeStruct((leaves, 3, 128, 128), F32),
            jax.ShapeDtypeStruct((leaves, EARLY, 3, 128), F32),
        ),
        in_specs=[SMEM, SMEM, VMEM, VMEM, HBM],
        out_specs=(VMEM,) * 6,
        scratch_shapes=[
            pltpu.VMEM(up.shape, BF16),
            pltpu.VMEM((24, 128), BF16),
            pltpu.VMEM((24, 128), BF16),
            pltpu.SemaphoreType.DMA,
            pltpu.SemaphoreType.DMA,
            pltpu.SemaphoreType.DMA,
            pltpu.SemaphoreType.DMA((4,)),
            pltpu.SemaphoreType.DMA((4,)),
            pltpu.SemaphoreType.DMA,
            pltpu.SemaphoreType.DMA,
        ],
        compiler_params=pltpu.CompilerParams(
            collective_id=0, has_side_effects=True, vmem_limit_bytes=LIMIT
        ),
    )(*in_hbm(near, cnt, pos, den, up))


def near_kernel(near_ref, cnt_ref, wpos_ref, wden_ref, cols, before_acc, early_ref, tgt_ref, bef_ref, aft_ref, racc, sacc):
    leaves = tgt_ref.shape[0]
    shift = (lax.axis_index("patch") - 1) * leaves
    sacc[...] = jnp.zeros_like(sacc)

    def leaf_step(leaf, _):
        racc[leaf] = jnp.zeros_like(racc[leaf])
        for slot in range(EARLY):
            other = near_ref[slot, leaf] - shift
            sacc[other, :, 0, :] += early_ref[leaf, slot]

        def slot_step(slot, _):
            other = near_ref[slot, leaf] - shift
            down = pair_block(leaf, wpos_ref[other], wden_ref[other], cols, racc)
            for k in range(3):
                sacc[other, k] += down[k]
            return 0

        lax.fori_loop(EARLY, cnt_ref[leaf], slot_step, 0)
        return 0

    lax.fori_loop(0, leaves, leaf_step, 0)

    def gather(pair, _):
        for sub in range(2):
            leaf = pair * 2 + sub
            for k in range(3):
                turned = jnp.transpose(racc[leaf, k] + before_acc[leaf, k], (1, 0))
                folded = turned[0:8]
                for tile in range(1, 16):
                    folded = folded + turned[8 * tile : 8 * tile + 8]
                folded = folded - sacc[leaves + leaf, k]
                row = pl.ds(k, 1)
                tgt_ref[leaf, row] = jnp.sum(folded, axis=0, keepdims=True) * KERNEL
                bef_ref[leaf, row] = jnp.sum(sacc[leaf, k], axis=0, keepdims=True) * -KERNEL
                aft_ref[leaf, row] = (
                    jnp.sum(sacc[2 * leaves + leaf, k], axis=0, keepdims=True) * -KERNEL
                )
        return 0

    lax.fori_loop(0, leaves // 2, gather, 0)


def near_call(near, cnt, wpos, wden, cols, racc, early):
    leaves = cnt.shape[0]
    grad = jax.ShapeDtypeStruct((leaves, 3, 128), F32)
    return pl.pallas_call(
        near_kernel,
        name="near",
        out_shape=(grad, grad, grad),
        in_specs=[SMEM] * 2 + [VMEM] * 5,
        out_specs=(VMEM,) * 3,
        scratch_shapes=[
            pltpu.VMEM((leaves, 3, 128, 128), F32),
            pltpu.VMEM((3 * leaves, 3, 8, 128), F32),
        ],
        compiler_params=pltpu.CompilerParams(vmem_limit_bytes=LIMIT),
        cost_estimate=pl.CostEstimate(flops=10**8, bytes_accessed=10**7, transcendentals=10**6),
    )(*in_hbm(near, cnt), wpos, wden, cols, racc, early)


def class_pitch(chunks):
    return chunks + 1 + chunks % 2


def back_kernel(count, bef_ref, aft_ref, mom_ref, sel_ref, table, got, wide, pattern, send_sem, recv_sem):
    classes = table.shape[0]
    chunks = table.shape[1] // 128
    me = lax.axis_index("patch")
    before = (me + count - 1) % count
    after = (me + 1) % count
    barrier = pltpu.get_barrier_semaphore()
    for target in (before, after):
        pl.semaphore_signal(barrier, inc=1, device_id=(target,), device_id_type=MESH)
    pl.semaphore_wait(barrier, 2)
    copies = []
    for i, (src, target) in enumerate(((bef_ref, before), (aft_ref, after))):
        copies.append(
            pltpu.make_async_remote_copy(
                src_ref=src,
                dst_ref=got.at[i],
                send_sem=send_sem.at[i],
                recv_sem=recv_sem.at[i],
                device_id=(target,),
                device_id_type=MESH,
            )
        )
        copies[-1].start()
    lane = lax.broadcasted_iota(jnp.int32, (8, 128), 1)
    mine = lane // 16 == lax.broadcasted_iota(jnp.int32, (8, 128), 0)

    def spread(step, _):
        lefts, rights = [], []
        for sub in range(8):
            block = mom_ref[step * 8 + sub]
            lefts.append(block[:32])
            ends = block[32:40].astype(F32)
            for i in range(4):
                rights.append(jnp.where(mine, jnp.broadcast_to(ends[i : i + 1], (8, 128)), 0.0))
        lhs = jnp.concatenate(
            [jnp.concatenate(lefts, axis=0), jnp.concatenate(rights, axis=0).astype(BF16)], axis=1
        )
        rows = pl.ds(pl.multiple_of(step * 256, 256), 256)
        for v in range(0, 9, 2):
            some = min(2, 9 - v)
            out = jnp.dot(lhs, sel_ref[:, 128 * v : 128 * (v + some)], preferred_element_type=F32)
            for i in range(some):
                pattern[v + i, rows] = out[:, 128 * i : 128 * i + 128]
        return 0

    lax.fori_loop(0, mom_ref.shape[0] // 8, spread, 0)

    pitch = class_pitch(chunks)

    def widen(block, _):
        rows = pl.ds(pl.multiple_of(block * 8, 8), 8)
        at = block * (8 * pitch)
        for chunk in range(chunks):
            to = chunk % 9 * (chunks // 9) + chunk // 9
            wide[pl.ds(at + to, 8, stride=pitch), :] = table[rows, 128 * chunk : 128 * chunk + 128].astype(F32)
        return 0

    full = classes // 8
    rest = classes - 8 * full
    lax.fori_loop(0, full, widen, 0)
    if rest:
        at = full * 8 * pitch
        for chunk in range(chunks):
            to = chunk % 9 * (chunks // 9) + chunk // 9
            wide[pl.ds(at + to, rest, stride=pitch), :] = table[
                8 * full :, 128 * chunk : 128 * chunk + 128
            ].astype(F32)
    pattern[:, mom_ref.shape[0] * 32 :] = jnp.zeros((9, 8, 128), F32)
    for copy in copies:
        copy.wait()


def back_call(count, bef, aft, mom, table, width):
    leaves = bef.shape[0]
    chunks = table.shape[1] // 128
    rows = table.shape[0] * class_pitch(chunks) + 8
    sel, _ = constants(width)
    return pl.pallas_call(
        functools.partial(back_kernel, count),
        name="back",
        out_shape=(
            jax.ShapeDtypeStruct((2,) + bef.shape, F32),
            jax.ShapeDtypeStruct((rows + -rows % 8, 128), F32),
            jax.ShapeDtypeStruct((9, count * leaves + 8, 128), F32),
        ),
        in_specs=[VMEM] * 5,
        out_specs=(VMEM,) * 3,
        scratch_shapes=[
            pltpu.SemaphoreType.DMA((2,)),
            pltpu.SemaphoreType.DMA((2,)),
        ],
        compiler_params=pltpu.CompilerParams(
            collective_id=1, has_side_effects=True, vmem_limit_bytes=LIMIT
        ),
    )(bef, aft, mom, sel, table)


def far_kernel(
    slot_ref, class_ref, fcnt_ref, req_ref, wide, pattern, seg_ref, basis, den_ref, tgt_ref, got, out_ref, sums, weight, down
):
    leaves, parts = basis.shape[0], basis.shape[1]
    width = basis.shape[2]
    pitch = class_pitch(width * width // 128)
    tall = width // 8
    nothing = pattern.shape[1] - 8
    slots = slot_ref.shape[1]

    def leaf_step(leaf, _):
        live = fcnt_ref[leaf]

        def fetch(slot):
            at = jnp.minimum(slot, slots - 1)
            v = slot_ref[leaf, at]
            who = v >> 2
            place = who * leaves + req_ref[v & 3, who]
            return jnp.where(slot < live, place, nothing), class_ref[leaf, at] * pitch

        def slot_step(step, carry):
            now, acc = carry
            following = tuple(fetch(UNROLL * (step + 1) + i) for i in range(UNROLL))
            new = []
            for v in range(9):
                p = [jnp.broadcast_to(pattern[v, pl.ds(a[0], 1), :], (8, 128)) for a in now]
                for g in range(3):
                    t = [wide[pl.ds(a[1] + tall * v + 8 * g, 8), :] for a in now]
                    terms = [x * y for x, y in zip(p, t)]
                    while len(terms) > 1:
                        terms = [x + y for x, y in zip(terms[::2], terms[1::2])]
                    new.append(acc[3 * v + g] + terms[0])
            return following, tuple(new)

        zero = jnp.zeros((8, 128), F32)
        first = tuple(fetch(i) for i in range(UNROLL))
        _, acc = lax.fori_loop(0, (live + UNROLL - 1) // UNROLL, slot_step, (first, (zero,) * 27))
        for v in range(9):
            for g in range(3):
                rows = pl.ds(pl.multiple_of(leaf * 24 + 8 * g, 8), 8)
                sums[v, rows] = acc[3 * v + g]
        return 0

    lax.fori_loop(0, leaves, leaf_step, 0)
    result = jnp.zeros((leaves * 24, seg_ref.shape[1]), F32)
    for v in range(9):
        total = sums[v]
        high = total.astype(BF16)
        low = (total - high.astype(F32)).astype(BF16)
        both = jnp.concatenate([high, low], axis=1)
        part = seg_ref[256 * v : 256 * v + 256]
        result = result + jnp.dot(both, part, preferred_element_type=F32)
    group = lax.broadcasted_iota(jnp.int32, (24, seg_ref.shape[1]), 0)
    lane = lax.broadcasted_iota(jnp.int32, (24, seg_ref.shape[1]), 1)
    keep = group == (lane >> 3)
    rows = []
    for leaf in range(leaves):
        mine = jnp.where(keep, result[24 * leaf : 24 * leaf + 24], 0.0)
        rows.append(jnp.sum(mine, axis=0, keepdims=True))
    expansion = jnp.concatenate(rows, axis=0)[:, :width].astype(BF16).astype(F32)
    square = (width, width)
    diagonal = lax.broadcasted_iota(jnp.int32, square, 0) == lax.broadcasted_iota(jnp.int32, square, 1)
    ones = jnp.ones((width, 128), BF16)
    for leaf in range(leaves):
        only = jnp.where(diagonal, jnp.broadcast_to(expansion[leaf : leaf + 1], square), 0.0)
        weight[leaf] = jnp.dot(only.astype(BF16), ones, preferred_element_type=F32)

    def down_step(leaf, _):
        for q in range(parts):
            part = [jnp.zeros((8, 128), F32) for _ in range(2)]
            for r in range(width // 16):
                d = basis[leaf, q, 16 * r : 16 * r + 16].astype(F32)
                for i in range(2):
                    part[i] = part[i] + d[8 * i : 8 * i + 8] * weight[leaf, 16 * r + 8 * i : 16 * r + 8 * i + 8]
            down[q, pl.ds(leaf, 1)] = jnp.sum(part[0] + part[1], axis=0, keepdims=True)
        return 0

    lax.fori_loop(0, leaves, down_step, 0)
    field = [down[q] for q in range(parts)]
    for k in range(3):
        far = den_ref[:, 0, :] * field[k]
        for c in range(1, 3):
            far = far + den_ref[:, c, :] * field[3 * c + k]
        out_ref[:, k, :] = far + (tgt_ref[:, k, :] + (got[0, :, k, :] + got[1, :, k, :]))


def constants(width):
    flat = np.arange(9 * 128)
    sel = np.zeros((256, 9 * 128), np.float32)
    place = flat % width
    sel[:128] = place[None, :] == np.arange(128)[:, None]
    sel[128:] = (place[None, :] >= 128) & ((place[None, :] - 128) == np.arange(128)[:, None] % (width - 128))
    seg = (flat[:, None] // width == np.arange(256)[None, :] % 8).astype(np.float32)
    seg = np.repeat(seg.reshape(9, 1, 128, 256), 2, axis=1).reshape(-1, 256)
    return [jnp.asarray(m, BF16) for m in (sel, seg)]


def far_call(slots, kinds, fcnt, requests, wide, pattern, basis, den, tgt, got):
    leaves = den.shape[0]
    _, seg = constants(basis.shape[2])
    return pl.pallas_call(
        far_kernel,
        name="far",
        out_shape=jax.ShapeDtypeStruct(den.shape, F32),
        in_specs=[SMEM] * 4 + [VMEM] * 7,
        out_specs=VMEM,
        scratch_shapes=[
            pltpu.VMEM((9, leaves * 24, 128), F32),
            pltpu.VMEM((leaves, basis.shape[2], 128), F32),
            pltpu.VMEM((basis.shape[1], leaves, 128), F32),
        ],
        compiler_params=pltpu.CompilerParams(vmem_limit_bytes=LIMIT),
        cost_estimate=pl.CostEstimate(flops=10**8, bytes_accessed=10**7, transcendentals=0),
    )(slots, kinds, fcnt, requests, wide, pattern, seg, basis, den, tgt, got)


def per_device(
    count,
    positions,
    densities,
    near_src,
    near_count,
    far_slot,
    far_class,
    far_count,
    requests,
    up_basis,
    transfer_table,
    down_basis,
):
    leaves = near_count.shape[0]
    width = up_basis.shape[1]

    def by_leaf(a):
        return a.reshape(3, leaves, -1).transpose(1, 0, 2)

    pos, den = by_leaf(positions), by_leaf(densities)
    near = near_src.T
    wpos, wden, mom, cols, racc, early = exchange_call(count, near, near_count, pos, den, up_basis)
    tgt, bef, aft = near_call(near, near_count, wpos, wden, cols, racc, early)
    got, wide, pattern = back_call(count, bef, aft, mom, transfer_table, width)
    out = far_call(
        far_slot,
        far_class,
        far_count,
        requests[0].T,
        wide,
        pattern,
        down_basis.transpose(0, 2, 1, 3),
        den,
        tgt,
        got,
    )
    return out.transpose(1, 0, 2).reshape(3, -1)


def solution(mesh):
    placed = (
        P(None, "patch"),
        P(None, "patch"),
        P("patch", None),
        P("patch"),
        P("patch", None),
        P("patch", None),
        P("patch"),
        P("patch", None, None),
        P("patch", None, None),
        P(),
        P("patch", None, None, None),
    )
    return jax.shard_map(
        functools.partial(per_device, mesh.shape["patch"]),
        mesh=mesh,
        in_specs=placed,
        out_specs=P(None, "patch"),
        check_vma=False,
    )
```

```python
import functools
import math

import jax
import jax.numpy as jnp
import numpy as np
from jax import lax
from jax.experimental import pallas as pl
from jax.experimental.pallas import tpu as pltpu
from jax.sharding import PartitionSpec as P

KERNEL = 1.0 / (8.0 * math.pi)
BLOB = 0.25
SIDE = 4
F32 = jnp.float32
BF16 = jnp.bfloat16
MESH = pl.DeviceIdType.MESH
SMEM = pl.BlockSpec(memory_space=pltpu.SMEM)
VMEM = pl.BlockSpec(memory_space=pltpu.VMEM)
HBM = pl.BlockSpec(memory_space=pltpu.HBM)
MIB = 1 << 20
LIMIT = 8 * MIB


def in_hbm(*arrays):
    return [pltpu.with_memory_space_constraint(a, pltpu.HBM) for a in arrays]

UNROLL = 3
EARLY = 4


PARTS = ((0, 0), (0, 1), (0, 2), (1, 0), (1, 1), (2, 0))
DEEP = 24
APART = DEEP + 1
SCALE = KERNEL / (3.0 * math.sqrt(3.0))


def three_parts(a):
    first = a.astype(BF16).astype(F32)
    second = (a - first).astype(BF16).astype(F32)
    return first, second, (a - first - second).astype(BF16).astype(F32)


def dot3(a, b):
    return a[0] * b[0] + a[1] * b[1] + a[2] * b[2]


def target_rows(pos, den, left):
    leaves = pos[0].shape[0]

    def put(n, row, value):
        left[n, pl.ds(row, leaves, stride=APART), :] = value

    for n, values in enumerate((pos, den)):
        for c in range(3):
            parts = three_parts(values[c])
            for p, (a, _) in enumerate(PARTS):
                put(n, 6 * c + p, parts[a])
    squares = three_parts(dot3(pos, pos) * (1.0 / 3.0))
    mixed = three_parts(dot3(den, pos))
    for i in range(3):
        put(0, 18 + i, jnp.ones_like(pos[0]))
        put(0, 21 + i, squares[i])
        put(1, 18 + i, mixed[i])
        put(1, 21 + i, jnp.zeros_like(pos[0]))


def source_rows(pos, den, right):
    leaves = pos[0].shape[0]

    def put(n, row, value):
        right[n, pl.ds(row, leaves, stride=APART), :] = value

    for c in range(3):
        x, f = three_parts(pos[c]), three_parts(den[c])
        scaled = three_parts(pos[c] * (-2.0 / 3.0))
        for p, (_, b) in enumerate(PARTS):
            put(0, 6 * c + p, scaled[b])
            put(1, 6 * c + p, f[b])
            put(2, 6 * c + p, f[b])
            put(3, 6 * c + p, -x[b])
    one, zero = jnp.ones_like(pos[0]), jnp.zeros_like(pos[0])
    squares = three_parts((dot3(pos, pos) + BLOB) * (1.0 / 3.0))
    mixed = three_parts(dot3(den, pos))
    for i in range(3):
        put(0, 18 + i, squares[i])
        put(0, 21 + i, one)
        put(1, 18 + i, -mixed[i])
        put(1, 21 + i, zero)
        put(2, 18 + i, zero)
        put(2, 21 + i, zero)
        put(3, 18 + i, one)
        put(3, 21 + i, zero)


def pair_products(leaf, other, lhs, right):
    rows = pl.ds(other * APART, DEEP)
    out = []
    for n in range(2):
        rhs = jnp.concatenate([right[2 * n, rows, :], right[2 * n + 1, rows, :]], axis=1).astype(BF16)
        out.append(jnp.dot(lhs[leaf, n], rhs, preferred_element_type=F32))
    return jnp.concatenate(out, axis=1)


def pair_block(leaf, other, wpos_ref, wden_ref, products, cols, racc):
    xs = [jnp.broadcast_to(wpos_ref[k, pl.ds(other, 1), :], (8, 128)) for k in range(3)]
    fs = [jnp.broadcast_to(wden_ref[k, pl.ds(other, 1), :], (8, 128)) for k in range(3)]
    down = [jnp.zeros((8, 128), F32) for _ in range(3)]
    for tile in range(16):
        part = pl.ds(8 * tile, 8)
        rho, br, ab, ar = [products[8 * tile : 8 * tile + 8, 128 * n : 128 * n + 128] for n in range(4)]
        fa = [cols[leaf, 3 + k, part] for k in range(3)]
        sep = [cols[leaf, k, part] - xs[k] for k in range(3)]
        inv = lax.rsqrt(rho)
        inv_two = inv * inv
        inv_three = inv_two * inv
        on_b = ar * inv_three
        on_a = br * inv_three
        on_r = ab * inv_three + (on_b * br) * inv_two
        for k in range(3):
            term = fa[k] * on_a + fs[k] * on_b - on_r * sep[k]
            racc[leaf, k, part] += term
            down[k] = down[k] + term
    return down


def exchange_kernel(
    count, near_ref, cnt_ref, pos_ref, den_ref, up_hbm, sum_ref, wpos_ref, wden_ref, mom_ref, cols, racc, early_ref, lhs, right,
    left, mine_x, mine_f, ahead, up, own, theirs, up_sem, pair_send, pair_recv, halo_send, halo_recv, send_sem, recv_sem
):
    leaves, width = up.shape[0], up.shape[1]
    plane = SIDE * SIDE
    chips = plane * SIDE
    me = lax.axis_index("patch")
    core = me % 2
    chip = me // 2
    y, z, x = chip // plane, (chip // SIDE) % SIDE, chip % SIDE
    partner = me + 1 - 2 * core
    other_side = (me + 2 * core - 1 + count) % count
    before = (me + count - 1) % count
    after = (me + 1) % count
    at_y = [((y + k) % SIDE) * (2 * plane) + core for k in range(SIDE)]
    at_z = [((z + k) % SIDE) * (2 * SIDE) for k in range(SIDE)]
    at_x = [((x + k) % SIDE) * 2 for k in range(SIDE)]
    steps = [(a, b, c) for a in range(SIDE) for b in range(SIDE) for c in range(SIDE)][1:]
    steps.sort(key=lambda s: -sum(min(v, SIDE - v) for v in s))
    peers = [at_y[a] + at_z[b] + at_x[c] for a, b, c in steps]

    get_up = pltpu.make_async_copy(up_hbm, up, up_sem)
    get_up.start()
    barrier = pltpu.get_barrier_semaphore()
    for target in [partner] + peers + [other_side]:
        pl.semaphore_signal(barrier, inc=1, device_id=(target,), device_id_type=MESH)

    for c in range(3):
        for src, mid, dst in ((pos_ref, mine_x, wpos_ref), (den_ref, mine_f, wden_ref)):
            mid[c] = src[:, c, :]
            dst[c, pl.ds(leaves, leaves)] = mid[c]
            dst[c, pl.ds(3 * leaves, 8)] = jnp.zeros((8, 128), F32)
    rounded = jnp.concatenate([mine_f[c] for c in range(3)], axis=1)
    row = lax.broadcasted_iota(jnp.int32, rounded.shape, 0)

    def spread(step, _):
        for sub in range(4):
            leaf = step * 4 + sub
            for n in range(2):
                turned = jnp.transpose(left[n, pl.ds(leaf * APART, DEEP), :], (1, 0)).astype(BF16)
                lhs[leaf, n] = turned
                spreads = jnp.dot(turned, sum_ref[...], preferred_element_type=F32)
                for k in range(3):
                    cols[leaf, 3 * n + k] = spreads[:, 128 * k : 128 * k + 128]
        return 0

    get_up.wait()
    total = jnp.zeros((leaves, width), F32)
    for leaf in range(leaves):
        only = jnp.where(row == leaf, rounded, 0.0).astype(BF16)
        total = total + lax.dot_general(
            only, up[leaf], (((1,), (1,)), ((), ())), preferred_element_type=F32
        )
    main = total[:, :128]
    tail = jnp.concatenate([total[:, 128:]] * (128 // (width - 128)), axis=1)
    lane = lax.broadcasted_iota(jnp.int32, tail.shape, 1)
    leaf_of = lax.broadcasted_iota(jnp.int32, tail.shape, 0)
    per_row = 128 // (width - 128)
    tail = jnp.where(lane // (width - 128) == leaf_of % per_row, tail, 0.0)
    ends = [
        jnp.sum(tail[i * per_row : (i + 1) * per_row], axis=0, keepdims=True)
        for i in range(leaves // per_row)
    ]
    fill = jnp.zeros((8 - len(ends), 128), F32)
    own[...] = jnp.concatenate([main] + ends + [fill], axis=0).astype(BF16)
    pl.semaphore_wait(barrier, chips + 1)
    to_partner = pltpu.make_async_remote_copy(
        src_ref=own,
        dst_ref=theirs,
        send_sem=pair_send,
        recv_sem=pair_recv,
        device_id=(partner,),
        device_id_type=MESH,
    )
    to_partner.start()
    halos = []
    for i, (src, dst) in enumerate(((mine_x, wpos_ref), (mine_f, wden_ref))):
        for j, (target, at) in enumerate(((before, 2 * leaves), (after, 0))):
            halos.append(
                pltpu.make_async_remote_copy(
                    src_ref=src,
                    dst_ref=dst.at[:, pl.ds(at, leaves)],
                    send_sem=halo_send.at[2 * i + j],
                    recv_sem=halo_recv.at[2 * i + j],
                    device_id=(target,),
                    device_id_type=MESH,
                )
            )
    for copy in halos:
        copy.start()
    to_partner.wait_recv()
    mine, his = own[...].astype(F32), theirs[...].astype(F32)
    first = jnp.where(core == 0, mine, his)
    second = jnp.where(core == 0, his, mine)
    main_rows = leaves
    mom_ref[chip] = jnp.concatenate(
        [
            first[:main_rows],
            second[:main_rows],
            first[main_rows : main_rows + 2],
            second[main_rows : main_rows + 2],
            jnp.zeros((4, 128), F32),
        ],
        axis=0,
    ).astype(BF16)
    block = mom_ref.at[chip]
    for target in peers:
        pltpu.make_async_remote_copy(
            src_ref=block,
            dst_ref=block,
            send_sem=send_sem,
            recv_sem=recv_sem,
            device_id=(target,),
            device_id_type=MESH,
        ).start()
    target_rows([mine_x[c] for c in range(3)], [mine_f[c] for c in range(3)], left)
    lax.fori_loop(0, leaves // 4, spread, 0)
    racc[...] = jnp.zeros_like(racc)
    for copy in halos:
        copy.wait()
    source_rows([wpos_ref[c] for c in range(3)], [wden_ref[c] for c in range(3)], right)

    shift = (me - 1) * leaves

    def source_of(leaf, slot):
        source = jnp.clip(near_ref[slot, leaf] - shift, 0, 3 * leaves - 1)
        return jnp.where(slot < cnt_ref[leaf], source, 3 * leaves)

    def early(leaf, _):
        sources = [source_of(leaf, slot) for slot in range(EARLY)]
        for slot, source in enumerate(sources):
            products = ahead if slot == 0 else pair_products(leaf, source, lhs, right)
            down = pair_block(leaf, source, wpos_ref, wden_ref, products, cols, racc)
            early_ref[leaf, slot] = jnp.concatenate(
                [jnp.sum(d, axis=0, keepdims=True) for d in down], axis=0
            )
        following = jnp.minimum(leaf + 1, leaves - 1)
        ahead[...] = pair_products(following, source_of(following, 0), lhs, right)
        return 0

    ahead[...] = pair_products(0, source_of(0, 0), lhs, right)
    lax.fori_loop(0, leaves, early, 0)
    to_partner.wait_send()
    moved = mom_ref.at[pl.ds(0, chips - 1)]
    pltpu.make_async_copy(moved, moved, send_sem).wait()
    pltpu.make_async_copy(moved, moved, recv_sem).wait()


def exchange_call(count, near, cnt, pos, den, up):
    sums = np.zeros((DEEP, 3 * 128), np.float32)
    for c in range(3):
        for p in (0, 3, 5):
            sums[6 * c + p, 128 * c : 128 * c + 128] = 1.0
    leaves, rows, lanes = pos.shape
    window = jax.ShapeDtypeStruct((rows, 3 * leaves + 8, lanes), F32)
    return pl.pallas_call(
        functools.partial(exchange_kernel, count),
        name="exchange",
        out_shape=(
            window,
            window,
            jax.ShapeDtypeStruct((count // 2, 40, 128), BF16),
            jax.ShapeDtypeStruct((leaves, 6, 128, 128), F32),
            jax.ShapeDtypeStruct((leaves, 3, 128, 128), F32),
            jax.ShapeDtypeStruct((leaves, EARLY, 3, 128), F32),
            jax.ShapeDtypeStruct((leaves, 2, 128, DEEP), BF16),
            jax.ShapeDtypeStruct((4, (3 * leaves + 8) * APART, 128), F32),
        ),
        in_specs=[SMEM, SMEM, VMEM, VMEM, HBM, VMEM],
        out_specs=(VMEM,) * 8,
        scratch_shapes=[
            pltpu.VMEM((2, leaves * APART, 128), F32),
            pltpu.VMEM((3, leaves, 128), F32),
            pltpu.VMEM((3, leaves, 128), F32),
            pltpu.VMEM((128, 512), F32),
            pltpu.VMEM(up.shape, BF16),
            pltpu.VMEM((24, 128), BF16),
            pltpu.VMEM((24, 128), BF16),
            pltpu.SemaphoreType.DMA,
            pltpu.SemaphoreType.DMA,
            pltpu.SemaphoreType.DMA,
            pltpu.SemaphoreType.DMA((4,)),
            pltpu.SemaphoreType.DMA((4,)),
            pltpu.SemaphoreType.DMA,
            pltpu.SemaphoreType.DMA,
        ],
        compiler_params=pltpu.CompilerParams(
            collective_id=0, has_side_effects=True, vmem_limit_bytes=LIMIT
        ),
    )(*in_hbm(near, cnt, pos, den, up, jnp.asarray(sums, BF16)))


def near_kernel(
    near_ref, cnt_ref, wpos_ref, wden_ref, cols, before_acc, early_ref, lhs, right, tgt_ref, bef_ref, aft_ref, racc, sacc,
    ahead, whose, which
):
    leaves = tgt_ref.shape[0]
    shift = (lax.axis_index("patch") - 1) * leaves
    sacc[...] = jnp.zeros_like(sacc)

    racc[...] = jnp.zeros_like(racc)

    def leaf_step(leaf, made):
        for slot in range(EARLY):
            other = near_ref[slot, leaf] - shift
            sacc[other, :, 0, :] += early_ref[leaf, slot]

        def note(slot, made):
            whose[made] = leaf
            which[made] = near_ref[slot, leaf] - shift
            return made + 1

        return lax.fori_loop(EARLY, cnt_ref[leaf], note, made)

    made = lax.fori_loop(0, leaves, leaf_step, 0)
    for i in range(3):
        whose[made + i] = 0
        which[made + i] = 3 * leaves

    def block(leaf, other, products):
        down = pair_block(leaf, other, wpos_ref, wden_ref, products, cols, racc)
        for k in range(3):
            sacc[other, k] += down[k]

    def two_blocks(pair, _):
        at = 2 * pair
        second = pair_products(whose[at + 1], which[at + 1], lhs, right)
        block(whose[at], which[at], ahead)
        third = pair_products(whose[at + 2], which[at + 2], lhs, right)
        block(whose[at + 1], which[at + 1], second)
        ahead[...] = third
        return 0

    ahead[...] = pair_products(whose[0], which[0], lhs, right)
    lax.fori_loop(0, (made + 1) // 2, two_blocks, 0)

    def gather(pair, _):
        for sub in range(2):
            leaf = pair * 2 + sub
            for k in range(3):
                turned = jnp.transpose(racc[leaf, k] + before_acc[leaf, k], (1, 0))
                folded = turned[0:8]
                for tile in range(1, 16):
                    folded = folded + turned[8 * tile : 8 * tile + 8]
                folded = folded - sacc[leaves + leaf, k]
                row = pl.ds(k, 1)
                tgt_ref[leaf, row] = jnp.sum(folded, axis=0, keepdims=True) * SCALE
                bef_ref[leaf, row] = jnp.sum(sacc[leaf, k], axis=0, keepdims=True) * -SCALE
                aft_ref[leaf, row] = (
                    jnp.sum(sacc[2 * leaves + leaf, k], axis=0, keepdims=True) * -SCALE
                )
        return 0

    lax.fori_loop(0, leaves // 2, gather, 0)


def near_call(near, cnt, wpos, wden, cols, racc, early, lhs, right):
    leaves = cnt.shape[0]
    grad = jax.ShapeDtypeStruct((leaves, 3, 128), F32)
    return pl.pallas_call(
        near_kernel,
        name="near",
        out_shape=(grad, grad, grad),
        in_specs=[SMEM] * 2 + [VMEM] * 7,
        out_specs=(VMEM,) * 3,
        scratch_shapes=[
            pltpu.VMEM((leaves, 3, 128, 128), F32),
            pltpu.VMEM((3 * leaves + 8, 3, 8, 128), F32),
            pltpu.VMEM((128, 512), F32),
            pltpu.SMEM((leaves * 8 + 8,), jnp.int32),
            pltpu.SMEM((leaves * 8 + 8,), jnp.int32),
        ],
        compiler_params=pltpu.CompilerParams(vmem_limit_bytes=LIMIT),
        cost_estimate=pl.CostEstimate(flops=10**8, bytes_accessed=10**7, transcendentals=10**6),
    )(*in_hbm(near, cnt), wpos, wden, cols, racc, early, lhs, right)


def class_pitch(chunks):
    return chunks + 1 + chunks % 2


def back_kernel(count, bef_ref, aft_ref, mom_ref, sel_ref, table, got, wide, pattern, send_sem, recv_sem):
    classes = table.shape[0]
    chunks = table.shape[1] // 128
    me = lax.axis_index("patch")
    before = (me + count - 1) % count
    after = (me + 1) % count
    barrier = pltpu.get_barrier_semaphore()
    for target in (before, after):
        pl.semaphore_signal(barrier, inc=1, device_id=(target,), device_id_type=MESH)
    pl.semaphore_wait(barrier, 2)
    copies = []
    for i, (src, target) in enumerate(((bef_ref, before), (aft_ref, after))):
        copies.append(
            pltpu.make_async_remote_copy(
                src_ref=src,
                dst_ref=got.at[i],
                send_sem=send_sem.at[i],
                recv_sem=recv_sem.at[i],
                device_id=(target,),
                device_id_type=MESH,
            )
        )
        copies[-1].start()
    lane = lax.broadcasted_iota(jnp.int32, (8, 128), 1)
    mine = lane // 16 == lax.broadcasted_iota(jnp.int32, (8, 128), 0)

    def spread(step, _):
        lefts, rights = [], []
        for sub in range(8):
            block = mom_ref[step * 8 + sub]
            lefts.append(block[:32])
            ends = block[32:40].astype(F32)
            for i in range(4):
                rights.append(jnp.where(mine, jnp.broadcast_to(ends[i : i + 1], (8, 128)), 0.0))
        lhs = jnp.concatenate(
            [jnp.concatenate(lefts, axis=0), jnp.concatenate(rights, axis=0).astype(BF16)], axis=1
        )
        rows = pl.ds(pl.multiple_of(step * 256, 256), 256)
        for v in range(0, 9, 2):
            some = min(2, 9 - v)
            out = jnp.dot(lhs, sel_ref[:, 128 * v : 128 * (v + some)], preferred_element_type=F32)
            for i in range(some):
                pattern[v + i, rows] = out[:, 128 * i : 128 * i + 128]
        return 0

    lax.fori_loop(0, mom_ref.shape[0] // 8, spread, 0)

    pitch = class_pitch(chunks)

    def widen(block, _):
        rows = pl.ds(pl.multiple_of(block * 8, 8), 8)
        at = block * (8 * pitch)
        for chunk in range(chunks):
            to = chunk % 9 * (chunks // 9) + chunk // 9
            wide[pl.ds(at + to, 8, stride=pitch), :] = table[rows, 128 * chunk : 128 * chunk + 128].astype(F32)
        return 0

    full = classes // 8
    rest = classes - 8 * full
    lax.fori_loop(0, full, widen, 0)
    if rest:
        at = full * 8 * pitch
        for chunk in range(chunks):
            to = chunk % 9 * (chunks // 9) + chunk // 9
            wide[pl.ds(at + to, rest, stride=pitch), :] = table[
                8 * full :, 128 * chunk : 128 * chunk + 128
            ].astype(F32)
    pattern[:, mom_ref.shape[0] * 32 :] = jnp.zeros((9, 8, 128), F32)
    for copy in copies:
        copy.wait()


def back_call(count, bef, aft, mom, table, width):
    leaves = bef.shape[0]
    chunks = table.shape[1] // 128
    rows = table.shape[0] * class_pitch(chunks) + 8
    sel, _ = constants(width)
    return pl.pallas_call(
        functools.partial(back_kernel, count),
        name="back",
        out_shape=(
            jax.ShapeDtypeStruct((2,) + bef.shape, F32),
            jax.ShapeDtypeStruct((rows + -rows % 8, 128), F32),
            jax.ShapeDtypeStruct((9, count * leaves + 8, 128), F32),
        ),
        in_specs=[VMEM] * 5,
        out_specs=(VMEM,) * 3,
        scratch_shapes=[
            pltpu.SemaphoreType.DMA((2,)),
            pltpu.SemaphoreType.DMA((2,)),
        ],
        compiler_params=pltpu.CompilerParams(
            collective_id=1, has_side_effects=True, vmem_limit_bytes=LIMIT
        ),
    )(bef, aft, mom, sel, table)


def far_kernel(
    slot_ref, class_ref, fcnt_ref, req_ref, wide, pattern, seg_ref, basis, den_ref, tgt_ref, got, out_ref, sums, weight, down
):
    leaves, parts = basis.shape[0], basis.shape[1]
    width = basis.shape[2]
    pitch = class_pitch(width * width // 128)
    tall = width // 8
    nothing = pattern.shape[1] - 8
    slots = slot_ref.shape[1]

    def leaf_step(leaf, _):
        live = fcnt_ref[leaf]

        def fetch(slot):
            at = jnp.minimum(slot, slots - 1)
            v = slot_ref[leaf, at]
            who = v >> 2
            place = who * leaves + req_ref[v & 3, who]
            return jnp.where(slot < live, place, nothing), class_ref[leaf, at] * pitch

        def slot_step(step, carry):
            now, acc = carry
            following = tuple(fetch(UNROLL * (step + 1) + i) for i in range(UNROLL))
            new = []
            for v in range(9):
                p = [jnp.broadcast_to(pattern[v, pl.ds(a[0], 1), :], (8, 128)) for a in now]
                for g in range(3):
                    t = [wide[pl.ds(a[1] + tall * v + 8 * g, 8), :] for a in now]
                    total = acc[3 * v + g]
                    for x, y in zip(p, t):
                        total = total + x * y
                    new.append(total)
            return following, tuple(new)

        zero = jnp.zeros((8, 128), F32)
        first = tuple(fetch(i) for i in range(UNROLL))
        _, acc = lax.fori_loop(0, (live + UNROLL - 1) // UNROLL, slot_step, (first, (zero,) * 27))
        for v in range(9):
            for g in range(3):
                rows = pl.ds(pl.multiple_of(leaf * 24 + 8 * g, 8), 8)
                sums[v, rows] = acc[3 * v + g]
        return 0

    lax.fori_loop(0, leaves, leaf_step, 0)
    result = jnp.zeros((leaves * 24, seg_ref.shape[1]), F32)
    for v in range(9):
        total = sums[v]
        high = total.astype(BF16)
        low = (total - high.astype(F32)).astype(BF16)
        both = jnp.concatenate([high, low], axis=1)
        part = seg_ref[256 * v : 256 * v + 256]
        result = result + jnp.dot(both, part, preferred_element_type=F32)
    group = lax.broadcasted_iota(jnp.int32, (24, seg_ref.shape[1]), 0)
    lane = lax.broadcasted_iota(jnp.int32, (24, seg_ref.shape[1]), 1)
    keep = group == (lane >> 3)
    rows = []
    for leaf in range(leaves):
        mine = jnp.where(keep, result[24 * leaf : 24 * leaf + 24], 0.0)
        rows.append(jnp.sum(mine, axis=0, keepdims=True))
    expansion = jnp.concatenate(rows, axis=0)[:, :width].astype(BF16).astype(F32)
    square = (width, width)
    diagonal = lax.broadcasted_iota(jnp.int32, square, 0) == lax.broadcasted_iota(jnp.int32, square, 1)
    ones = jnp.ones((width, 128), BF16)
    for leaf in range(leaves):
        only = jnp.where(diagonal, jnp.broadcast_to(expansion[leaf : leaf + 1], square), 0.0)
        weight[leaf] = jnp.dot(only.astype(BF16), ones, preferred_element_type=F32)

    def down_step(leaf, _):
        for q in range(parts):
            part = [jnp.zeros((8, 128), F32) for _ in range(2)]
            for r in range(width // 16):
                d = basis[leaf, q, 16 * r : 16 * r + 16].astype(F32)
                for i in range(2):
                    part[i] = part[i] + d[8 * i : 8 * i + 8] * weight[leaf, 16 * r + 8 * i : 16 * r + 8 * i + 8]
            down[q, pl.ds(leaf, 1)] = jnp.sum(part[0] + part[1], axis=0, keepdims=True)
        return 0

    lax.fori_loop(0, leaves, down_step, 0)
    field = [down[q] for q in range(parts)]
    for k in range(3):
        far = den_ref[:, 0, :] * field[k]
        for c in range(1, 3):
            far = far + den_ref[:, c, :] * field[3 * c + k]
        out_ref[:, k, :] = far + (tgt_ref[:, k, :] + (got[0, :, k, :] + got[1, :, k, :]))


def constants(width):
    flat = np.arange(9 * 128)
    sel = np.zeros((256, 9 * 128), np.float32)
    place = flat % width
    sel[:128] = place[None, :] == np.arange(128)[:, None]
    sel[128:] = (place[None, :] >= 128) & ((place[None, :] - 128) == np.arange(128)[:, None] % (width - 128))
    seg = (flat[:, None] // width == np.arange(256)[None, :] % 8).astype(np.float32)
    seg = np.repeat(seg.reshape(9, 1, 128, 256), 2, axis=1).reshape(-1, 256)
    return [jnp.asarray(m, BF16) for m in (sel, seg)]


def far_call(slots, kinds, fcnt, requests, wide, pattern, basis, den, tgt, got):
    leaves = den.shape[0]
    _, seg = constants(basis.shape[2])
    return pl.pallas_call(
        far_kernel,
        name="far",
        out_shape=jax.ShapeDtypeStruct(den.shape, F32),
        in_specs=[SMEM] * 4 + [VMEM] * 7,
        out_specs=VMEM,
        scratch_shapes=[
            pltpu.VMEM((9, leaves * 24, 128), F32),
            pltpu.VMEM((leaves, basis.shape[2], 128), F32),
            pltpu.VMEM((basis.shape[1], leaves, 128), F32),
        ],
        compiler_params=pltpu.CompilerParams(vmem_limit_bytes=LIMIT),
        cost_estimate=pl.CostEstimate(flops=10**8, bytes_accessed=10**7, transcendentals=0),
    )(slots, kinds, fcnt, requests, wide, pattern, seg, basis, den, tgt, got)


def per_device(
    count,
    positions,
    densities,
    near_src,
    near_count,
    far_slot,
    far_class,
    far_count,
    requests,
    up_basis,
    transfer_table,
    down_basis,
):
    leaves = near_count.shape[0]
    width = up_basis.shape[1]

    def by_leaf(a):
        return a.reshape(3, leaves, -1).transpose(1, 0, 2)

    pos, den = by_leaf(positions), by_leaf(densities)
    near = near_src.T
    wpos, wden, mom, cols, racc, early, lhs, right = exchange_call(count, near, near_count, pos, den, up_basis)
    tgt, bef, aft = near_call(near, near_count, wpos, wden, cols, racc, early, lhs, right)
    got, wide, pattern = back_call(count, bef, aft, mom, transfer_table, width)
    out = far_call(
        far_slot,
        far_class,
        far_count,
        requests[0].T,
        wide,
        pattern,
        down_basis.transpose(0, 2, 1, 3),
        den,
        tgt,
        got,
    )
    return out.transpose(1, 0, 2).reshape(3, -1)


def solution(mesh):
    placed = (
        P(None, "patch"),
        P(None, "patch"),
        P("patch", None),
        P("patch"),
        P("patch", None),
        P("patch", None),
        P("patch"),
        P("patch", None, None),
        P("patch", None, None),
        P(),
        P("patch", None, None, None),
    )
    return jax.shard_map(
        functools.partial(per_device, mesh.shape["patch"]),
        mesh=mesh,
        in_specs=placed,
        out_specs=P(None, "patch"),
        check_vma=False,
    )
```

```python
import functools
import math

import jax
import jax.numpy as jnp
import numpy as np
from jax import lax
from jax.experimental import pallas as pl
from jax.experimental.pallas import tpu as pltpu
from jax.sharding import PartitionSpec as P

KERNEL = 1.0 / (8.0 * math.pi)
BLOB = 0.25
SIDE = 4
F32 = jnp.float32
BF16 = jnp.bfloat16
MESH = pl.DeviceIdType.MESH
SMEM = pl.BlockSpec(memory_space=pltpu.SMEM)
VMEM = pl.BlockSpec(memory_space=pltpu.VMEM)
HBM = pl.BlockSpec(memory_space=pltpu.HBM)
MIB = 1 << 20
LIMIT = 6 * MIB


def in_hbm(*arrays):
    return [pltpu.with_memory_space_constraint(a, pltpu.HBM) for a in arrays]

UNROLL = 3
EARLY = 3


def class_pitch(chunks):
    return chunks + 1 + chunks % 2


def widen_table(table, wide):
    classes = table.shape[0]
    chunks = table.shape[1] // 128
    pitch = class_pitch(chunks)

    def widen(block, _):
        rows = pl.ds(pl.multiple_of(block * 8, 8), 8)
        at = block * (8 * pitch)
        for chunk in range(chunks):
            to = chunk % 9 * (chunks // 9) + chunk // 9
            wide[pl.ds(at + to, 8, stride=pitch), :] = table[rows, 128 * chunk : 128 * chunk + 128].astype(F32)
        return 0

    full = classes // 8
    rest = classes - 8 * full
    lax.fori_loop(0, full, widen, 0)
    if rest:
        at = full * 8 * pitch
        for chunk in range(chunks):
            to = chunk % 9 * (chunks // 9) + chunk // 9
            wide[pl.ds(at + to, rest, stride=pitch), :] = table[
                8 * full :, 128 * chunk : 128 * chunk + 128
            ].astype(F32)


def pair_block(leaf, source_x, source_f, cols, racc):
    xs = [jnp.broadcast_to(source_x[k : k + 1], (8, 128)) for k in range(3)]
    fs = [jnp.broadcast_to(source_f[k : k + 1], (8, 128)) for k in range(3)]
    down = [jnp.zeros((8, 128), F32) for _ in range(3)]
    for tile in range(16):
        part = pl.ds(8 * tile, 8)
        fa = [cols[leaf, 3 + k, part] for k in range(3)]
        sep = [cols[leaf, k, part] - xs[k] for k in range(3)]
        rho = (sep[0] * sep[0] + sep[1] * sep[1]) + (sep[2] * sep[2] + BLOB)
        inv = lax.rsqrt(rho)
        inv_two = inv * inv
        inv_three = inv_two * inv
        ab = fa[0] * fs[0] + fa[1] * fs[1] + fa[2] * fs[2]
        ar = fa[0] * sep[0] + fa[1] * sep[1] + fa[2] * sep[2]
        br = fs[0] * sep[0] + fs[1] * sep[1] + fs[2] * sep[2]
        on_b = ar * inv_three
        on_a = br * inv_three
        on_r = ab * inv_three + (on_b * br) * (inv_two * 3.0)
        for k in range(3):
            term = fa[k] * on_a + fs[k] * on_b - on_r * sep[k]
            racc[leaf, k, part] += term
            down[k] = down[k] + term
    return down


def exchange_kernel(
    count, near_ref, cnt_ref, pos_ref, den_ref, up_hbm, table_hbm, wpos_ref, wden_ref, mom_ref, cols, racc, early_ref, wide,
    table, up, own, theirs, up_sem, table_sem, pair_send, pair_recv, halo_send, halo_recv, send_sem, recv_sem
):
    leaves, width = up.shape[0], up.shape[1]
    plane = SIDE * SIDE
    chips = plane * SIDE
    me = lax.axis_index("patch")
    core = me % 2
    chip = me // 2
    y, z, x = chip // plane, (chip // SIDE) % SIDE, chip % SIDE
    partner = me + 1 - 2 * core
    other_side = (me + 2 * core - 1 + count) % count
    before = (me + count - 1) % count
    after = (me + 1) % count
    at_y = [((y + k) % SIDE) * (2 * plane) + core for k in range(SIDE)]
    at_z = [((z + k) % SIDE) * (2 * SIDE) for k in range(SIDE)]
    at_x = [((x + k) % SIDE) * 2 for k in range(SIDE)]
    steps = [(a, b, c) for a in range(SIDE) for b in range(SIDE) for c in range(SIDE)][1:]
    steps.sort(key=lambda s: -sum(min(v, SIDE - v) for v in s))
    peers = [at_y[a] + at_z[b] + at_x[c] for a, b, c in steps]

    get_up = pltpu.make_async_copy(up_hbm, up, up_sem)
    get_up.start()
    barrier = pltpu.get_barrier_semaphore()
    for target in [partner] + peers + [other_side]:
        pl.semaphore_signal(barrier, inc=1, device_id=(target,), device_id_type=MESH)

    wpos_ref[pl.ds(leaves, leaves)] = pos_ref[...]
    wden_ref[pl.ds(leaves, leaves)] = den_ref[...]
    rounded = jnp.concatenate([den_ref[:, c, :] for c in range(3)], axis=1)
    row = lax.broadcasted_iota(jnp.int32, rounded.shape, 0)

    def spread(pair, _):
        for sub in range(2):
            leaf = pair * 2 + sub
            rows = jnp.concatenate([pos_ref[leaf], den_ref[leaf], jnp.zeros((2, 128), F32)], axis=0)
            turned = jnp.transpose(rows, (1, 0))
            for k in range(6):
                cols[leaf, k] = jnp.broadcast_to(turned[:, k : k + 1], (128, 128))
        return 0

    get_up.wait()
    get_table = pltpu.make_async_copy(table_hbm, table, table_sem)
    get_table.start()
    total = jnp.zeros((leaves, width), F32)
    for leaf in range(leaves):
        only = jnp.where(row == leaf, rounded, 0.0).astype(BF16)
        total = total + lax.dot_general(
            only, up[leaf], (((1,), (1,)), ((), ())), preferred_element_type=F32
        )
    main = total[:, :128]
    tail = jnp.concatenate([total[:, 128:]] * (128 // (width - 128)), axis=1)
    lane = lax.broadcasted_iota(jnp.int32, tail.shape, 1)
    leaf_of = lax.broadcasted_iota(jnp.int32, tail.shape, 0)
    per_row = 128 // (width - 128)
    tail = jnp.where(lane // (width - 128) == leaf_of % per_row, tail, 0.0)
    ends = [
        jnp.sum(tail[i * per_row : (i + 1) * per_row], axis=0, keepdims=True)
        for i in range(leaves // per_row)
    ]
    fill = jnp.zeros((8 - len(ends), 128), F32)
    own[...] = jnp.concatenate([main] + ends + [fill], axis=0).astype(BF16)
    pl.semaphore_wait(barrier, chips + 1)
    to_partner = pltpu.make_async_remote_copy(
        src_ref=own,
        dst_ref=theirs,
        send_sem=pair_send,
        recv_sem=pair_recv,
        device_id=(partner,),
        device_id_type=MESH,
    )
    to_partner.start()
    halos = []
    for i, (src, dst) in enumerate(((pos_ref, wpos_ref), (den_ref, wden_ref))):
        for j, (target, at) in enumerate(((before, 2 * leaves), (after, 0))):
            halos.append(
                pltpu.make_async_remote_copy(
                    src_ref=src,
                    dst_ref=dst.at[pl.ds(at, leaves)],
                    send_sem=halo_send.at[2 * i + j],
                    recv_sem=halo_recv.at[2 * i + j],
                    device_id=(target,),
                    device_id_type=MESH,
                )
            )
    for copy in halos:
        copy.start()
    to_partner.wait_recv()
    mine, his = own[...].astype(F32), theirs[...].astype(F32)
    first = jnp.where(core == 0, mine, his)
    second = jnp.where(core == 0, his, mine)
    main_rows = leaves
    mom_ref[chip] = jnp.concatenate(
        [
            first[:main_rows],
            second[:main_rows],
            first[main_rows : main_rows + 2],
            second[main_rows : main_rows + 2],
            jnp.zeros((4, 128), F32),
        ],
        axis=0,
    ).astype(BF16)
    block = mom_ref.at[chip]
    for target in peers:
        pltpu.make_async_remote_copy(
            src_ref=block,
            dst_ref=block,
            send_sem=send_sem,
            recv_sem=recv_sem,
            device_id=(target,),
            device_id_type=MESH,
        ).start()
    lax.fori_loop(0, leaves // 2, spread, 0)
    racc[...] = jnp.zeros_like(racc)
    get_table.wait()
    widen_table(table, wide)
    for copy in halos:
        copy.wait()

    shift = (me - 1) * leaves

    def early(leaf, _):
        for slot in range(EARLY):
            source = jnp.clip(near_ref[slot, leaf] - shift, 0, 3 * leaves - 1)
            live = jnp.where(slot < cnt_ref[leaf], 1.0, 0.0)
            down = pair_block(leaf, wpos_ref[source], wden_ref[source] * live, cols, racc)
            early_ref[leaf, slot] = jnp.concatenate(
                [jnp.sum(d, axis=0, keepdims=True) for d in down], axis=0
            )
        return 0

    lax.fori_loop(0, leaves, early, 0)
    to_partner.wait_send()
    moved = mom_ref.at[pl.ds(0, chips - 1)]
    pltpu.make_async_copy(moved, moved, send_sem).wait()
    pltpu.make_async_copy(moved, moved, recv_sem).wait()


def exchange_call(count, near, cnt, pos, den, up, table):
    leaves, rows, lanes = pos.shape
    height = table.shape[0] * class_pitch(table.shape[1] // 128) + 8
    window = jax.ShapeDtypeStruct((3 * leaves, rows, lanes), F32)
    return pl.pallas_call(
        functools.partial(exchange_kernel, count),
        name="exchange",
        out_shape=(
            window,
            window,
            jax.ShapeDtypeStruct((count // 2, 40, 128), BF16),
            jax.ShapeDtypeStruct((leaves, 6, 128, 128), F32),
            jax.ShapeDtypeStruct((leaves, 3, 128, 128), F32),
            jax.ShapeDtypeStruct((leaves, EARLY, 3, 128), F32),
            jax.ShapeDtypeStruct((height + -height % 8, 128), F32),
        ),
        in_specs=[SMEM, SMEM, VMEM, VMEM, HBM, HBM],
        out_specs=(VMEM,) * 7,
        scratch_shapes=[
            pltpu.VMEM(table.shape, BF16),
            pltpu.VMEM(up.shape, BF16),
            pltpu.VMEM((24, 128), BF16),
            pltpu.VMEM((24, 128), BF16),
            pltpu.SemaphoreType.DMA,
            pltpu.SemaphoreType.DMA,
            pltpu.SemaphoreType.DMA,
            pltpu.SemaphoreType.DMA,
            pltpu.SemaphoreType.DMA((4,)),
            pltpu.SemaphoreType.DMA((4,)),
            pltpu.SemaphoreType.DMA,
            pltpu.SemaphoreType.DMA,
        ],
        compiler_params=pltpu.CompilerParams(
            collective_id=0, has_side_effects=True, vmem_limit_bytes=12 * MIB
        ),
    )(*in_hbm(near, cnt, pos, den, up, table))


def near_kernel(near_ref, cnt_ref, wpos_ref, wden_ref, cols, early_ref, bef_ref, aft_ref, racc, own_ref, sacc):
    leaves = bef_ref.shape[0]
    shift = (lax.axis_index("patch") - 1) * leaves
    sacc[...] = jnp.zeros_like(sacc)

    def leaf_step(leaf, _):
        racc[leaf] = jnp.zeros_like(racc[leaf])
        for slot in range(EARLY):
            other = near_ref[slot, leaf] - shift
            sacc[other, :, 0, :] += early_ref[leaf, slot]

        def slot_step(slot, _):
            other = near_ref[slot, leaf] - shift
            down = pair_block(leaf, wpos_ref[other], wden_ref[other], cols, racc)
            for k in range(3):
                sacc[other, k] += down[k]
            return 0

        lax.fori_loop(EARLY, cnt_ref[leaf], slot_step, 0)
        return 0

    lax.fori_loop(0, leaves, leaf_step, 0)

    for k in range(3):
        own_ref[:, k] = sacc[leaves : 2 * leaves, k]

    def gather(leaf, _):
        for k in range(3):
            row = pl.ds(k, 1)
            bef_ref[leaf, row] = jnp.sum(sacc[leaf, k], axis=0, keepdims=True) * -KERNEL
            aft_ref[leaf, row] = jnp.sum(sacc[2 * leaves + leaf, k], axis=0, keepdims=True) * -KERNEL
        return 0

    lax.fori_loop(0, leaves, gather, 0, unroll=4)


def near_call(near, cnt, wpos, wden, cols, early):
    leaves = cnt.shape[0]
    grad = jax.ShapeDtypeStruct((leaves, 3, 128), F32)
    return pl.pallas_call(
        near_kernel,
        name="near",
        out_shape=(
            grad,
            grad,
            jax.ShapeDtypeStruct((leaves, 3, 128, 128), F32),
            jax.ShapeDtypeStruct((leaves, 3, 8, 128), F32),
        ),
        in_specs=[SMEM] * 2 + [VMEM] * 4,
        out_specs=(VMEM,) * 4,
        scratch_shapes=[
            pltpu.VMEM((3 * leaves, 3, 8, 128), F32),
        ],
        compiler_params=pltpu.CompilerParams(vmem_limit_bytes=LIMIT),
        cost_estimate=pl.CostEstimate(flops=10**8, bytes_accessed=10**7, transcendentals=10**6),
    )(*in_hbm(near, cnt), wpos, wden, cols, early)


def back_kernel(
    count, bef_ref, aft_ref, mom_ref, sel_ref, first_acc, racc, own_ref, got, pattern, tgt_ref, send_sem, recv_sem
):
    me = lax.axis_index("patch")
    before = (me + count - 1) % count
    after = (me + 1) % count
    barrier = pltpu.get_barrier_semaphore()
    for target in (before, after):
        pl.semaphore_signal(barrier, inc=1, device_id=(target,), device_id_type=MESH)
    pl.semaphore_wait(barrier, 2)
    copies = []
    for i, (src, target) in enumerate(((bef_ref, before), (aft_ref, after))):
        copies.append(
            pltpu.make_async_remote_copy(
                src_ref=src,
                dst_ref=got.at[i],
                send_sem=send_sem.at[i],
                recv_sem=recv_sem.at[i],
                device_id=(target,),
                device_id_type=MESH,
            )
        )
        copies[-1].start()
    lane = lax.broadcasted_iota(jnp.int32, (8, 128), 1)
    mine = lane // 16 == lax.broadcasted_iota(jnp.int32, (8, 128), 0)

    def spread(step, _):
        lefts, rights = [], []
        for sub in range(8):
            block = mom_ref[step * 8 + sub]
            lefts.append(block[:32])
            ends = block[32:40].astype(F32)
            for i in range(4):
                rights.append(jnp.where(mine, jnp.broadcast_to(ends[i : i + 1], (8, 128)), 0.0))
        lhs = jnp.concatenate(
            [jnp.concatenate(lefts, axis=0), jnp.concatenate(rights, axis=0).astype(BF16)], axis=1
        )
        rows = pl.ds(pl.multiple_of(step * 256, 256), 256)
        for v in range(0, 9, 2):
            some = min(2, 9 - v)
            out = jnp.dot(lhs, sel_ref[:, 128 * v : 128 * (v + some)], preferred_element_type=F32)
            for i in range(some):
                pattern[v + i, rows] = out[:, 128 * i : 128 * i + 128]
        return 0

    lax.fori_loop(0, mom_ref.shape[0] // 8, spread, 0)

    pattern[:, mom_ref.shape[0] * 32 :] = jnp.zeros((9, 8, 128), F32)

    def gather(pair, _):
        for sub in range(2):
            leaf = pair * 2 + sub
            for k in range(3):
                turned = jnp.transpose(racc[leaf, k] + first_acc[leaf, k], (1, 0))
                folded = turned[0:8]
                for tile in range(1, 16):
                    folded = folded + turned[8 * tile : 8 * tile + 8]
                folded = folded - own_ref[leaf, k]
                tgt_ref[leaf, pl.ds(k, 1)] = jnp.sum(folded, axis=0, keepdims=True) * KERNEL
        return 0

    lax.fori_loop(0, racc.shape[0] // 2, gather, 0)
    for copy in copies:
        copy.wait()


def back_call(count, bef, aft, mom, first, racc, own, width):
    leaves = bef.shape[0]
    sel, _ = constants(width)
    return pl.pallas_call(
        functools.partial(back_kernel, count),
        name="back",
        out_shape=(
            jax.ShapeDtypeStruct((2,) + bef.shape, F32),
            jax.ShapeDtypeStruct((9, count * leaves + 8, 128), F32),
            jax.ShapeDtypeStruct(bef.shape, F32),
        ),
        in_specs=[VMEM] * 7,
        out_specs=(VMEM,) * 3,
        scratch_shapes=[
            pltpu.SemaphoreType.DMA((2,)),
            pltpu.SemaphoreType.DMA((2,)),
        ],
        compiler_params=pltpu.CompilerParams(
            collective_id=1, has_side_effects=True, vmem_limit_bytes=LIMIT
        ),
    )(bef, aft, mom, sel, first, racc, own)


def far_kernel(
    slot_ref, class_ref, fcnt_ref, req_ref, wide, pattern, seg_ref, rep_ref, basis, den_ref, tgt_ref, got, out_ref, sums, weight, down
):
    leaves, parts = basis.shape[0], basis.shape[1]
    width = basis.shape[2]
    pitch = class_pitch(width * width // 128)
    tall = width // 8
    nothing = pattern.shape[1] - 8
    slots = slot_ref.shape[1]

    def leaf_step(leaf, _):
        live = fcnt_ref[leaf]

        def fetch(slot):
            at = jnp.minimum(slot, slots - 1)
            v = slot_ref[leaf, at]
            who = v >> 2
            place = who * leaves + req_ref[v & 3, who]
            return jnp.where(slot < live, place, nothing), class_ref[leaf, at] * pitch

        def slot_step(step, carry):
            now, acc = carry
            following = tuple(fetch(UNROLL * (step + 1) + i) for i in range(UNROLL))
            new = []
            for v in range(9):
                p = [jnp.broadcast_to(pattern[v, pl.ds(a[0], 1), :], (8, 128)) for a in now]
                for g in range(3):
                    t = [wide[pl.ds(a[1] + tall * v + 8 * g, 8), :] for a in now]
                    total = acc[3 * v + g]
                    for x, y in zip(p, t):
                        total = total + x * y
                    new.append(total)
            return following, tuple(new)

        zero = jnp.zeros((8, 128), F32)
        first = tuple(fetch(i) for i in range(UNROLL))
        _, acc = lax.fori_loop(0, (live + UNROLL - 1) // UNROLL, slot_step, (first, (zero,) * 27))
        for v in range(9):
            for g in range(3):
                rows = pl.ds(pl.multiple_of(leaf * 24 + 8 * g, 8), 8)
                sums[v, rows] = acc[3 * v + g]
        return 0

    lax.fori_loop(0, leaves, leaf_step, 0)
    result = jnp.zeros((leaves * 24, seg_ref.shape[1]), F32)
    for v in range(9):
        total = sums[v]
        high = total.astype(BF16)
        low = (total - high.astype(F32)).astype(BF16)
        both = jnp.concatenate([high, low], axis=1)
        part = seg_ref[256 * v : 256 * v + 256]
        result = result + jnp.dot(both, part, preferred_element_type=F32)
    expansion = result.astype(BF16)
    for w in range(8):
        spread = jnp.dot(expansion, rep_ref[:, 128 * w : 128 * w + 128], preferred_element_type=F32)
        weight[pl.ds(w, leaves * 24, stride=8), :] = spread

    def down_step(leaf, _):
        for q in range(parts):
            part = [jnp.zeros((8, 128), F32) for _ in range(2)]
            for r in range(width // 16):
                d = basis[leaf, q, 16 * r : 16 * r + 16].astype(F32)
                for i in range(2):
                    part[i] = part[i] + d[8 * i : 8 * i + 8] * weight[pl.ds(pl.multiple_of(leaf * 192, 8) + 16 * r + 8 * i, 8), :]
            down[q, pl.ds(leaf, 1)] = jnp.sum(part[0] + part[1], axis=0, keepdims=True)
        return 0

    lax.fori_loop(0, leaves, down_step, 0)
    field = [down[q] for q in range(parts)]
    for k in range(3):
        far = den_ref[:, 0, :] * field[k]
        for c in range(1, 3):
            far = far + den_ref[:, c, :] * field[3 * c + k]
        out_ref[:, k, :] = far + (tgt_ref[:, k, :] + (got[0, :, k, :] + got[1, :, k, :]))


def constants(width):
    flat = np.arange(9 * 128)
    sel = np.zeros((256, 9 * 128), np.float32)
    place = flat % width
    sel[:128] = place[None, :] == np.arange(128)[:, None]
    sel[128:] = (place[None, :] >= 128) & ((place[None, :] - 128) == np.arange(128)[:, None] % (width - 128))
    seg = (flat[:, None] // width == np.arange(128)[None, :]).astype(np.float32)
    seg = np.repeat(seg.reshape(9, 1, 128, 128), 2, axis=1).reshape(-1, 128)
    return [jnp.asarray(m, BF16) for m in (sel, seg)]


def far_call(slots, kinds, fcnt, requests, wide, pattern, basis, den, tgt, got):
    leaves = den.shape[0]
    _, seg = constants(basis.shape[2])
    rep = (np.arange(1024)[None, :] // 128 == np.arange(128)[:, None]).astype(np.float32)
    return pl.pallas_call(
        far_kernel,
        name="far",
        out_shape=jax.ShapeDtypeStruct(den.shape, F32),
        in_specs=[SMEM] * 4 + [VMEM] * 8,
        out_specs=VMEM,
        scratch_shapes=[
            pltpu.VMEM((9, leaves * 24, 128), F32),
            pltpu.VMEM((leaves * 192, 128), F32),
            pltpu.VMEM((basis.shape[1], leaves, 128), F32),
        ],
        compiler_params=pltpu.CompilerParams(vmem_limit_bytes=LIMIT),
        cost_estimate=pl.CostEstimate(flops=10**8, bytes_accessed=10**7, transcendentals=0),
    )(slots, kinds, fcnt, requests, wide, pattern, seg, jnp.asarray(rep, BF16), basis, den, tgt, got)


def per_device(
    count,
    positions,
    densities,
    near_src,
    near_count,
    far_slot,
    far_class,
    far_count,
    requests,
    up_basis,
    transfer_table,
    down_basis,
):
    leaves = near_count.shape[0]
    width = up_basis.shape[1]

    def by_leaf(a):
        return a.reshape(3, leaves, -1).transpose(1, 0, 2)

    pos, den = by_leaf(positions), by_leaf(densities)
    near = near_src.T
    wpos, wden, mom, cols, first, early, wide = exchange_call(
        count, near, near_count, pos, den, up_basis, transfer_table
    )
    bef, aft, racc, own = near_call(near, near_count, wpos, wden, cols, early)
    got, pattern, tgt = back_call(count, bef, aft, mom, first, racc, own, width)
    out = far_call(
        far_slot,
        far_class,
        far_count,
        requests[0].T,
        wide,
        pattern,
        down_basis.transpose(0, 2, 1, 3),
        den,
        tgt,
        got,
    )
    return out.transpose(1, 0, 2).reshape(3, -1)


def solution(mesh):
    placed = (
        P(None, "patch"),
        P(None, "patch"),
        P("patch", None),
        P("patch"),
        P("patch", None),
        P("patch", None),
        P("patch"),
        P("patch", None, None),
        P("patch", None, None),
        P(),
        P("patch", None, None, None),
    )
    return jax.shard_map(
        functools.partial(per_device, mesh.shape["patch"]),
        mesh=mesh,
        in_specs=placed,
        out_specs=P(None, "patch"),
        check_vma=False,
    )
```

```python
import functools
import math

import jax
import jax.numpy as jnp
import numpy as np
from jax import lax
from jax.experimental import pallas as pl
from jax.experimental.pallas import tpu as pltpu
from jax.sharding import PartitionSpec as P

KERNEL = 1.0 / (8.0 * math.pi)
BLOB = 0.25
SIDE = 4
F32 = jnp.float32
BF16 = jnp.bfloat16
MESH = pl.DeviceIdType.MESH
SMEM = pl.BlockSpec(memory_space=pltpu.SMEM)
VMEM = pl.BlockSpec(memory_space=pltpu.VMEM)
HBM = pl.BlockSpec(memory_space=pltpu.HBM)
MIB = 1 << 20
MIDDLE_LIMIT = 14 * MIB
LIMIT = 6 * MIB


def in_hbm(*arrays):
    return [pltpu.with_memory_space_constraint(a, pltpu.HBM) for a in arrays]

UNROLL = 3
EARLY = 3


def class_pitch(chunks):
    return chunks + 1 + chunks % 2


def widen_table(table, wide):
    classes = table.shape[0]
    chunks = table.shape[1] // 128
    pitch = class_pitch(chunks)

    def widen(block, _):
        rows = pl.ds(pl.multiple_of(block * 8, 8), 8)
        at = block * (8 * pitch)
        for chunk in range(chunks):
            to = chunk % 9 * (chunks // 9) + chunk // 9
            wide[pl.ds(at + to, 8, stride=pitch), :] = table[rows, 128 * chunk : 128 * chunk + 128].astype(F32)
        return 0

    full = classes // 8
    rest = classes - 8 * full
    lax.fori_loop(0, full, widen, 0)
    if rest:
        at = full * 8 * pitch
        for chunk in range(chunks):
            to = chunk % 9 * (chunks // 9) + chunk // 9
            wide[pl.ds(at + to, rest, stride=pitch), :] = table[
                8 * full :, 128 * chunk : 128 * chunk + 128
            ].astype(F32)


def pair_block(leaf, source_x, source_f, cols, racc):
    xs = [jnp.broadcast_to(source_x[k : k + 1], (8, 128)) for k in range(3)]
    fs = [jnp.broadcast_to(source_f[k : k + 1], (8, 128)) for k in range(3)]
    down = [jnp.zeros((8, 128), F32) for _ in range(3)]
    for tile in range(16):
        part = pl.ds(8 * tile, 8)
        fa = [cols[leaf, 3 + k, part] for k in range(3)]
        sep = [cols[leaf, k, part] - xs[k] for k in range(3)]
        rho = (sep[0] * sep[0] + sep[1] * sep[1]) + (sep[2] * sep[2] + BLOB)
        inv = lax.rsqrt(rho)
        inv_two = inv * inv
        inv_three = inv_two * inv
        ab = fa[0] * fs[0] + fa[1] * fs[1] + fa[2] * fs[2]
        ar = fa[0] * sep[0] + fa[1] * sep[1] + fa[2] * sep[2]
        br = fs[0] * sep[0] + fs[1] * sep[1] + fs[2] * sep[2]
        on_b = ar * inv_three
        on_a = br * inv_three
        on_r = ab * inv_three + (on_b * br) * (inv_two * 3.0)
        for k in range(3):
            term = fa[k] * on_a + fs[k] * on_b - on_r * sep[k]
            racc[leaf, k, part] += term
            down[k] = down[k] + term
    return down


def exchange_kernel(
    count, near_ref, cnt_ref, pos_ref, den_ref, up_hbm, table_hbm, sum_ref, wpos_ref, wden_ref, mom_ref, cols, racc, early_ref, wide,
    table, left, up, own, theirs, up_sem, table_sem, pair_send, pair_recv, halo_send, halo_recv, send_sem, recv_sem
):
    leaves, width = up.shape[0], up.shape[1]
    plane = SIDE * SIDE
    chips = plane * SIDE
    me = lax.axis_index("patch")
    core = me % 2
    chip = me // 2
    y, z, x = chip // plane, (chip // SIDE) % SIDE, chip % SIDE
    partner = me + 1 - 2 * core
    other_side = (me + 2 * core - 1 + count) % count
    before = (me + count - 1) % count
    after = (me + 1) % count
    at_y = [((y + k) % SIDE) * (2 * plane) + core for k in range(SIDE)]
    at_z = [((z + k) % SIDE) * (2 * SIDE) for k in range(SIDE)]
    at_x = [((x + k) % SIDE) * 2 for k in range(SIDE)]
    steps = [(a, b, c) for a in range(SIDE) for b in range(SIDE) for c in range(SIDE)][1:]
    steps.sort(key=lambda s: -sum(min(v, SIDE - v) for v in s))
    peers = [at_y[a] + at_z[b] + at_x[c] for a, b, c in steps]

    get_ups = []
    for i in range(4):
        part = pl.ds(i * (leaves // 4), leaves // 4)
        get_ups.append(pltpu.make_async_copy(up_hbm.at[part], up.at[part], up_sem.at[i]))
        get_ups[-1].start()
    barrier = pltpu.get_barrier_semaphore()
    for target in [partner] + peers + [other_side]:
        pl.semaphore_signal(barrier, inc=1, device_id=(target,), device_id_type=MESH)

    wpos_ref[pl.ds(leaves, leaves)] = pos_ref[...]
    wden_ref[pl.ds(leaves, leaves)] = den_ref[...]
    rounded = jnp.concatenate([den_ref[:, c, :] for c in range(3)], axis=1)
    row = lax.broadcasted_iota(jnp.int32, rounded.shape, 0)

    def spread(step, _):
        for sub in range(4):
            leaf = step * 4 + sub
            turned = jnp.transpose(left[pl.ds(leaf * 25, 24), :], (1, 0)).astype(BF16)
            wide_rows = jnp.dot(turned, sum_ref[...], preferred_element_type=F32)
            for k in range(6):
                cols[leaf, k] = wide_rows[:, 128 * k : 128 * k + 128]
        return 0

    def columns():
        for k in range(6):
            rest = (pos_ref, den_ref)[k // 3][:, k % 3, :]
            for p in range(3):
                part = rest.astype(BF16).astype(F32)
                left[pl.ds(3 * k + p, leaves, stride=25), :] = part
                rest = rest - part
        for row_at in range(18, 24):
            left[pl.ds(row_at, leaves, stride=25), :] = jnp.zeros((leaves, 128), F32)
        lax.fori_loop(0, leaves // 4, spread, 0)

    get_table = pltpu.make_async_copy(table_hbm, table, table_sem)
    total = jnp.zeros((leaves, width), F32)
    for leaf in range(leaves):
        if leaf % (leaves // 4) == 0:
            get_ups[leaf // (leaves // 4)].wait()
        only = jnp.where(row == leaf, rounded, 0.0).astype(BF16)
        total = total + lax.dot_general(
            only, up[leaf], (((1,), (1,)), ((), ())), preferred_element_type=F32
        )
    get_table.start()
    main = total[:, :128]
    tail = jnp.concatenate([total[:, 128:]] * (128 // (width - 128)), axis=1)
    lane = lax.broadcasted_iota(jnp.int32, tail.shape, 1)
    leaf_of = lax.broadcasted_iota(jnp.int32, tail.shape, 0)
    per_row = 128 // (width - 128)
    tail = jnp.where(lane // (width - 128) == leaf_of % per_row, tail, 0.0)
    ends = [
        jnp.sum(tail[i * per_row : (i + 1) * per_row], axis=0, keepdims=True)
        for i in range(leaves // per_row)
    ]
    fill = jnp.zeros((8 - len(ends), 128), F32)
    own[...] = jnp.concatenate([main] + ends + [fill], axis=0).astype(BF16)
    pl.semaphore_wait(barrier, chips + 1)
    to_partner = pltpu.make_async_remote_copy(
        src_ref=own,
        dst_ref=theirs,
        send_sem=pair_send,
        recv_sem=pair_recv,
        device_id=(partner,),
        device_id_type=MESH,
    )
    to_partner.start()
    halos = []
    for i, (src, dst) in enumerate(((pos_ref, wpos_ref), (den_ref, wden_ref))):
        for j, (target, at) in enumerate(((before, 2 * leaves), (after, 0))):
            halos.append(
                pltpu.make_async_remote_copy(
                    src_ref=src,
                    dst_ref=dst.at[pl.ds(at, leaves)],
                    send_sem=halo_send.at[2 * i + j],
                    recv_sem=halo_recv.at[2 * i + j],
                    device_id=(target,),
                    device_id_type=MESH,
                )
            )
    for copy in halos:
        copy.start()
    to_partner.wait_recv()
    mine, his = own[...].astype(F32), theirs[...].astype(F32)
    first = jnp.where(core == 0, mine, his)
    second = jnp.where(core == 0, his, mine)
    main_rows = leaves
    mom_ref[chip] = jnp.concatenate(
        [
            first[:main_rows],
            second[:main_rows],
            first[main_rows : main_rows + 2],
            second[main_rows : main_rows + 2],
            jnp.zeros((4, 128), F32),
        ],
        axis=0,
    ).astype(BF16)
    block = mom_ref.at[chip]
    for target in peers:
        pltpu.make_async_remote_copy(
            src_ref=block,
            dst_ref=block,
            send_sem=send_sem,
            recv_sem=recv_sem,
            device_id=(target,),
            device_id_type=MESH,
        ).start()
    columns()
    racc[...] = jnp.zeros_like(racc)
    get_table.wait()
    widen_table(table, wide)
    for copy in halos:
        copy.wait()

    shift = (me - 1) * leaves

    def early(leaf, _):
        for slot in range(EARLY):
            source = jnp.clip(near_ref[slot, leaf] - shift, 0, 3 * leaves - 1)
            live = jnp.where(slot < cnt_ref[leaf], 1.0, 0.0)
            down = pair_block(leaf, wpos_ref[source], wden_ref[source] * live, cols, racc)
            early_ref[leaf, slot] = jnp.concatenate(
                [jnp.sum(d, axis=0, keepdims=True) for d in down], axis=0
            )
        return 0

    lax.fori_loop(0, leaves, early, 0)
    to_partner.wait_send()
    moved = mom_ref.at[pl.ds(0, chips - 1)]
    pltpu.make_async_copy(moved, moved, send_sem).wait()
    pltpu.make_async_copy(moved, moved, recv_sem).wait()


def exchange_call(count, near, cnt, pos, den, up, table):
    leaves, rows, lanes = pos.shape
    sums = np.zeros((24, 6 * 128), np.float32)
    for k in range(6):
        sums[3 * k : 3 * k + 3, 128 * k : 128 * k + 128] = 1.0
    sums = jnp.asarray(sums, BF16)
    height = table.shape[0] * class_pitch(table.shape[1] // 128) + 8
    window = jax.ShapeDtypeStruct((3 * leaves, rows, lanes), F32)
    return pl.pallas_call(
        functools.partial(exchange_kernel, count),
        name="exchange",
        out_shape=(
            window,
            window,
            jax.ShapeDtypeStruct((count // 2, 40, 128), BF16),
            jax.ShapeDtypeStruct((leaves, 6, 128, 128), F32),
            jax.ShapeDtypeStruct((leaves, 3, 128, 128), F32),
            jax.ShapeDtypeStruct((leaves, EARLY, 3, 128), F32),
            jax.ShapeDtypeStruct((height + -height % 8, 128), F32),
        ),
        in_specs=[SMEM, SMEM, VMEM, VMEM, HBM, HBM, VMEM],
        out_specs=(VMEM,) * 7,
        scratch_shapes=[
            pltpu.VMEM(table.shape, BF16),
            pltpu.VMEM((leaves * 25, 128), F32),
            pltpu.VMEM(up.shape, BF16),
            pltpu.VMEM((24, 128), BF16),
            pltpu.VMEM((24, 128), BF16),
            pltpu.SemaphoreType.DMA((4,)),
            pltpu.SemaphoreType.DMA,
            pltpu.SemaphoreType.DMA,
            pltpu.SemaphoreType.DMA,
            pltpu.SemaphoreType.DMA((4,)),
            pltpu.SemaphoreType.DMA((4,)),
            pltpu.SemaphoreType.DMA,
            pltpu.SemaphoreType.DMA,
        ],
        compiler_params=pltpu.CompilerParams(
            collective_id=0, has_side_effects=True, vmem_limit_bytes=12 * MIB
        ),
    )(*in_hbm(near, cnt, pos, den, up, table, sums))


def middle_kernel(
    width, near_ref, cnt_ref, slot_ref, class_ref, fcnt_ref, req_ref, wpos_ref, wden_ref, cols, early_ref, mom_ref, sel_ref, wide,
    bef_ref, aft_ref, racc, own_ref, sums, sacc, pattern
):
    leaves = bef_ref.shape[0]
    shift = (lax.axis_index("patch") - 1) * leaves
    sacc[...] = jnp.zeros_like(sacc)

    def leaf_step(leaf, _):
        racc[leaf] = jnp.zeros_like(racc[leaf])
        for slot in range(EARLY):
            other = near_ref[slot, leaf] - shift
            sacc[other, :, 0, :] += early_ref[leaf, slot]

        def slot_step(slot, _):
            other = near_ref[slot, leaf] - shift
            down = pair_block(leaf, wpos_ref[other], wden_ref[other], cols, racc)
            for k in range(3):
                sacc[other, k] += down[k]
            return 0

        lax.fori_loop(EARLY, cnt_ref[leaf], slot_step, 0)
        return 0

    lax.fori_loop(0, leaves, leaf_step, 0)

    for k in range(3):
        own_ref[:, k] = sacc[leaves : 2 * leaves, k]

    def gather(leaf, _):
        for k in range(3):
            row = pl.ds(k, 1)
            bef_ref[leaf, row] = jnp.sum(sacc[leaf, k], axis=0, keepdims=True) * -KERNEL
            aft_ref[leaf, row] = jnp.sum(sacc[2 * leaves + leaf, k], axis=0, keepdims=True) * -KERNEL
        return 0

    lax.fori_loop(0, leaves, gather, 0, unroll=4)

    lane = lax.broadcasted_iota(jnp.int32, (8, 128), 1)
    mine = lane // 16 == lax.broadcasted_iota(jnp.int32, (8, 128), 0)

    def spread(step, _):
        lefts, rights = [], []
        for sub in range(8):
            block = mom_ref[step * 8 + sub]
            lefts.append(block[:32])
            ends = block[32:40].astype(F32)
            for i in range(4):
                rights.append(jnp.where(mine, jnp.broadcast_to(ends[i : i + 1], (8, 128)), 0.0))
        lhs = jnp.concatenate(
            [jnp.concatenate(lefts, axis=0), jnp.concatenate(rights, axis=0).astype(BF16)], axis=1
        )
        rows = pl.ds(pl.multiple_of(step * 256, 256), 256)
        for v in range(0, 9, 2):
            some = min(2, 9 - v)
            out = jnp.dot(lhs, sel_ref[:, 128 * v : 128 * (v + some)], preferred_element_type=F32)
            for i in range(some):
                pattern[v + i, rows] = out[:, 128 * i : 128 * i + 128]
        return 0

    lax.fori_loop(0, mom_ref.shape[0] // 8, spread, 0)

    pattern[:, mom_ref.shape[0] * 32 :] = jnp.zeros((9, 8, 128), F32)

    pitch = class_pitch(width * width // 128)
    tall = width // 8
    nothing = pattern.shape[1] - 8
    slots = slot_ref.shape[1]

    def leaf_step(leaf, _):
        live = fcnt_ref[leaf]

        def fetch(slot):
            at = jnp.minimum(slot, slots - 1)
            v = slot_ref[leaf, at]
            who = v >> 2
            place = who * leaves + req_ref[v & 3, who]
            return jnp.where(slot < live, place, nothing), class_ref[leaf, at] * pitch

        def slot_step(step, carry):
            now, acc = carry
            following = tuple(fetch(UNROLL * (step + 1) + i) for i in range(UNROLL))
            new = []
            for v in range(9):
                p = [jnp.broadcast_to(pattern[v, pl.ds(a[0], 1), :], (8, 128)) for a in now]
                for g in range(3):
                    t = [wide[pl.ds(a[1] + tall * v + 8 * g, 8), :] for a in now]
                    total = acc[3 * v + g]
                    for x, y in zip(p, t):
                        total = total + x * y
                    new.append(total)
            return following, tuple(new)

        zero = jnp.zeros((8, 128), F32)
        first = tuple(fetch(i) for i in range(UNROLL))
        _, acc = lax.fori_loop(0, (live + UNROLL - 1) // UNROLL, slot_step, (first, (zero,) * 27))
        for v in range(9):
            for g in range(3):
                rows = pl.ds(pl.multiple_of(leaf * 24 + 8 * g, 8), 8)
                sums[v, rows] = acc[3 * v + g]
        return 0

    lax.fori_loop(0, leaves, leaf_step, 0)


def middle_call(near, cnt, slots, kinds, fcnt, requests, wpos, wden, cols, early, mom, wide, count, width):
    leaves = cnt.shape[0]
    grad = jax.ShapeDtypeStruct((leaves, 3, 128), F32)
    sel, _ = constants(width)
    return pl.pallas_call(
        functools.partial(middle_kernel, width),
        name="middle",
        out_shape=(
            grad,
            grad,
            jax.ShapeDtypeStruct((leaves, 3, 128, 128), F32),
            jax.ShapeDtypeStruct((leaves, 3, 8, 128), F32),
            jax.ShapeDtypeStruct((9, leaves * 24, 128), F32),
        ),
        in_specs=[SMEM] * 6 + [VMEM] * 7,
        out_specs=(VMEM,) * 5,
        scratch_shapes=[
            pltpu.VMEM((3 * leaves, 3, 8, 128), F32),
            pltpu.VMEM((9, count * leaves + 8, 128), F32),
        ],
        compiler_params=pltpu.CompilerParams(vmem_limit_bytes=MIDDLE_LIMIT),
        cost_estimate=pl.CostEstimate(flops=10**8, bytes_accessed=10**7, transcendentals=10**6),
    )(near, cnt, slots, kinds, fcnt, requests, wpos, wden, cols, early, mom, sel, wide)


def back_kernel(
    count, bef_ref, aft_ref, first_acc, racc, own_ref, sums, seg_ref, rep_ref, basis, den_ref, out_ref, got, tgt_ref, weight,
    down, send_sem, recv_sem
):
    leaves, parts = basis.shape[0], basis.shape[1]
    width = basis.shape[2]
    me = lax.axis_index("patch")
    before = (me + count - 1) % count
    after = (me + 1) % count
    barrier = pltpu.get_barrier_semaphore()
    for target in (before, after):
        pl.semaphore_signal(barrier, inc=1, device_id=(target,), device_id_type=MESH)
    pl.semaphore_wait(barrier, 2)
    copies = []
    for i, (src, target) in enumerate(((bef_ref, before), (aft_ref, after))):
        copies.append(
            pltpu.make_async_remote_copy(
                src_ref=src,
                dst_ref=got.at[i],
                send_sem=send_sem.at[i],
                recv_sem=recv_sem.at[i],
                device_id=(target,),
                device_id_type=MESH,
            )
        )
        copies[-1].start()
    result = jnp.zeros((leaves * 24, seg_ref.shape[1]), F32)
    for v in range(9):
        total = sums[v]
        high = total.astype(BF16)
        low = (total - high.astype(F32)).astype(BF16)
        both = jnp.concatenate([high, low], axis=1)
        part = seg_ref[256 * v : 256 * v + 256]
        result = result + jnp.dot(both, part, preferred_element_type=F32)
    expansion = result.astype(BF16)
    for w in range(8):
        spread = jnp.dot(expansion, rep_ref[:, 128 * w : 128 * w + 128], preferred_element_type=F32)
        weight[pl.ds(w, leaves * 24, stride=8), :] = spread

    def down_step(leaf, _):
        for q in range(parts):
            part = [jnp.zeros((8, 128), F32) for _ in range(2)]
            for r in range(width // 16):
                d = basis[leaf, q, 16 * r : 16 * r + 16].astype(F32)
                for i in range(2):
                    part[i] = part[i] + d[8 * i : 8 * i + 8] * weight[pl.ds(pl.multiple_of(leaf * 192, 8) + 16 * r + 8 * i, 8), :]
            down[q, pl.ds(leaf, 1)] = jnp.sum(part[0] + part[1], axis=0, keepdims=True)
        return 0

    lax.fori_loop(0, leaves, down_step, 0)
    field = [down[q] for q in range(parts)]
    def gather(pair, _):
        for sub in range(2):
            leaf = pair * 2 + sub
            for k in range(3):
                turned = jnp.transpose(racc[leaf, k] + first_acc[leaf, k], (1, 0))
                folded = turned[0:8]
                for tile in range(1, 16):
                    folded = folded + turned[8 * tile : 8 * tile + 8]
                folded = folded - own_ref[leaf, k]
                tgt_ref[leaf, pl.ds(k, 1)] = jnp.sum(folded, axis=0, keepdims=True) * KERNEL
        return 0

    lax.fori_loop(0, racc.shape[0] // 2, gather, 0)
    for copy in copies:
        copy.wait()
    for k in range(3):
        far = den_ref[:, 0, :] * field[k]
        for c in range(1, 3):
            far = far + den_ref[:, c, :] * field[3 * c + k]
        out_ref[:, k, :] = far + (tgt_ref[:, k, :] + (got[0, :, k, :] + got[1, :, k, :]))


def back_call(count, bef, aft, first, racc, own, sums, basis, den):
    leaves = den.shape[0]
    _, seg = constants(basis.shape[2])
    rep = (np.arange(1024)[None, :] // 128 == np.arange(128)[:, None]).astype(np.float32)
    return pl.pallas_call(
        functools.partial(back_kernel, count),
        name="back",
        out_shape=jax.ShapeDtypeStruct(den.shape, F32),
        in_specs=[VMEM] * 10,
        out_specs=VMEM,
        scratch_shapes=[
            pltpu.VMEM((2,) + den.shape, F32),
            pltpu.VMEM(den.shape, F32),
            pltpu.VMEM((leaves * 192, 128), F32),
            pltpu.VMEM((basis.shape[1], leaves, 128), F32),
            pltpu.SemaphoreType.DMA((2,)),
            pltpu.SemaphoreType.DMA((2,)),
        ],
        compiler_params=pltpu.CompilerParams(
            collective_id=1, has_side_effects=True, vmem_limit_bytes=LIMIT
        ),
    )(bef, aft, first, racc, own, sums, seg, jnp.asarray(rep, BF16), basis, den)


def constants(width):
    flat = np.arange(9 * 128)
    sel = np.zeros((256, 9 * 128), np.float32)
    place = flat % width
    sel[:128] = place[None, :] == np.arange(128)[:, None]
    sel[128:] = (place[None, :] >= 128) & ((place[None, :] - 128) == np.arange(128)[:, None] % (width - 128))
    seg = (flat[:, None] // width == np.arange(128)[None, :]).astype(np.float32)
    seg = np.repeat(seg.reshape(9, 1, 128, 128), 2, axis=1).reshape(-1, 128)
    return [jnp.asarray(m, BF16) for m in (sel, seg)]


def per_device(
    count,
    positions,
    densities,
    near_src,
    near_count,
    far_slot,
    far_class,
    far_count,
    requests,
    up_basis,
    transfer_table,
    down_basis,
):
    leaves = near_count.shape[0]
    width = up_basis.shape[1]

    def by_leaf(a):
        return a.reshape(3, leaves, -1).transpose(1, 0, 2)

    pos, den = by_leaf(positions), by_leaf(densities)
    near = near_src.T
    wpos, wden, mom, cols, first, early, wide = exchange_call(
        count, near, near_count, pos, den, up_basis, transfer_table
    )
    bef, aft, racc, own, sums = middle_call(
        near,
        near_count,
        far_slot,
        far_class,
        far_count,
        requests[0].T,
        wpos,
        wden,
        cols,
        early,
        mom,
        wide,
        count,
        width,
    )
    out = back_call(count, bef, aft, first, racc, own, sums, down_basis.transpose(0, 2, 1, 3), den)
    return out.transpose(1, 0, 2).reshape(3, -1)


def solution(mesh):
    placed = (
        P(None, "patch"),
        P(None, "patch"),
        P("patch", None),
        P("patch"),
        P("patch", None),
        P("patch", None),
        P("patch"),
        P("patch", None, None),
        P("patch", None, None),
        P(),
        P("patch", None, None, None),
    )
    return jax.shard_map(
        functools.partial(per_device, mesh.shape["patch"]),
        mesh=mesh,
        in_specs=placed,
        out_specs=P(None, "patch"),
        check_vma=False,
    )
```

```python
import functools
import math

import jax
import jax.numpy as jnp
import numpy as np
from jax import lax
from jax.experimental import pallas as pl
from jax.experimental.pallas import tpu as pltpu
from jax.sharding import PartitionSpec as P

KERNEL = 1.0 / (8.0 * math.pi)
BLOB = 0.25
SIDE = 4
F32 = jnp.float32
BF16 = jnp.bfloat16
MESH = pl.DeviceIdType.MESH
SMEM = pl.BlockSpec(memory_space=pltpu.SMEM)
VMEM = pl.BlockSpec(memory_space=pltpu.VMEM)
HBM = pl.BlockSpec(memory_space=pltpu.HBM)
MIB = 1 << 20
MIDDLE_LIMIT = 14 * MIB
LIMIT = 6 * MIB


def in_hbm(*arrays):
    return [pltpu.with_memory_space_constraint(a, pltpu.HBM) for a in arrays]

UNROLL = 3
EARLY = 3


def class_pitch(chunks):
    return chunks + 1 + chunks % 2


def widen_table(table, wide):
    classes = table.shape[0]
    chunks = table.shape[1] // 128
    pitch = class_pitch(chunks)

    def widen(block, _):
        rows = pl.ds(pl.multiple_of(block * 8, 8), 8)
        at = block * (8 * pitch)
        for chunk in range(chunks):
            to = chunk % 9 * (chunks // 9) + chunk // 9
            wide[pl.ds(at + to, 8, stride=pitch), :] = table[rows, 128 * chunk : 128 * chunk + 128].astype(F32)
        return 0

    full = classes // 8
    rest = classes - 8 * full
    lax.fori_loop(0, full, widen, 0)
    if rest:
        at = full * 8 * pitch
        for chunk in range(chunks):
            to = chunk % 9 * (chunks // 9) + chunk // 9
            wide[pl.ds(at + to, rest, stride=pitch), :] = table[
                8 * full :, 128 * chunk : 128 * chunk + 128
            ].astype(F32)


def pair_block(leaf, source_x, source_f, cols, racc):
    xs = [jnp.broadcast_to(source_x[k : k + 1], (8, 128)) for k in range(3)]
    fs = [jnp.broadcast_to(source_f[k : k + 1], (8, 128)) for k in range(3)]
    down = [jnp.zeros((8, 128), F32) for _ in range(3)]
    for tile in range(16):
        part = pl.ds(8 * tile, 8)
        fa = [cols[leaf, 3 + k, part] for k in range(3)]
        sep = [cols[leaf, k, part] - xs[k] for k in range(3)]
        rho = (sep[0] * sep[0] + sep[1] * sep[1]) + (sep[2] * sep[2] + BLOB)
        inv = lax.rsqrt(rho)
        inv_two = inv * inv
        inv_three = inv_two * inv
        ab = fa[0] * fs[0] + fa[1] * fs[1] + fa[2] * fs[2]
        ar = fa[0] * sep[0] + fa[1] * sep[1] + fa[2] * sep[2]
        br = fs[0] * sep[0] + fs[1] * sep[1] + fs[2] * sep[2]
        on_b = ar * inv_three
        on_a = br * inv_three
        on_r = ab * inv_three + (on_b * br) * (inv_two * 3.0)
        for k in range(3):
            term = fa[k] * on_a + fs[k] * on_b - on_r * sep[k]
            racc[leaf, k, part] += term
            down[k] = down[k] + term
    return down


def exchange_kernel(
    count, near_ref, cnt_ref, pos_ref, den_ref, up_hbm, table_hbm, sum_ref, wpos_ref, wden_ref, mom_ref, cols, racc, early_ref, wide,
    table, left, up, own, theirs, up_sem, table_sem, pair_send, pair_recv, halo_send, halo_recv, send_sem, recv_sem
):
    leaves, width = up.shape[0], up.shape[1]
    plane = SIDE * SIDE
    chips = plane * SIDE
    me = lax.axis_index("patch")
    core = me % 2
    chip = me // 2
    y, z, x = chip // plane, (chip // SIDE) % SIDE, chip % SIDE
    partner = me + 1 - 2 * core
    other_side = (me + 2 * core - 1 + count) % count
    before = (me + count - 1) % count
    after = (me + 1) % count
    at_y = [((y + k) % SIDE) * (2 * plane) + core for k in range(SIDE)]
    at_z = [((z + k) % SIDE) * (2 * SIDE) for k in range(SIDE)]
    at_x = [((x + k) % SIDE) * 2 for k in range(SIDE)]
    steps = [(a, b, c) for a in range(SIDE) for b in range(SIDE) for c in range(SIDE)][1:]
    steps.sort(key=lambda s: -sum(min(v, SIDE - v) for v in s))
    peers = [at_y[a] + at_z[b] + at_x[c] for a, b, c in steps]

    get_ups = []
    for i in range(4):
        part = pl.ds(i * (leaves // 4), leaves // 4)
        get_ups.append(pltpu.make_async_copy(up_hbm.at[part], up.at[part], up_sem.at[i]))
        get_ups[-1].start()
    barrier = pltpu.get_barrier_semaphore()
    for target in [partner] + peers + [other_side]:
        pl.semaphore_signal(barrier, inc=1, device_id=(target,), device_id_type=MESH)

    wpos_ref[pl.ds(leaves, leaves)] = pos_ref[...]
    wden_ref[pl.ds(leaves, leaves)] = den_ref[...]
    rounded = jnp.concatenate([den_ref[:, c, :] for c in range(3)], axis=1)
    row = lax.broadcasted_iota(jnp.int32, rounded.shape, 0)

    def spread(step, _):
        for sub in range(4):
            leaf = step * 4 + sub
            turned = jnp.transpose(left[pl.ds(leaf * 25, 24), :], (1, 0)).astype(BF16)
            wide_rows = jnp.dot(turned, sum_ref[...], preferred_element_type=F32)
            for k in range(6):
                cols[leaf, k] = wide_rows[:, 128 * k : 128 * k + 128]
        return 0

    def columns():
        for k in range(6):
            rest = (pos_ref, den_ref)[k // 3][:, k % 3, :]
            for p in range(3):
                part = rest.astype(BF16).astype(F32)
                left[pl.ds(3 * k + p, leaves, stride=25), :] = part
                rest = rest - part
        for row_at in range(18, 24):
            left[pl.ds(row_at, leaves, stride=25), :] = jnp.zeros((leaves, 128), F32)
        lax.fori_loop(0, leaves // 4, spread, 0)

    get_table = pltpu.make_async_copy(table_hbm, table, table_sem)
    total = jnp.zeros((leaves, width), F32)
    for leaf in range(leaves):
        if leaf % (leaves // 4) == 0:
            get_ups[leaf // (leaves // 4)].wait()
        only = jnp.where(row == leaf, rounded, 0.0).astype(BF16)
        total = total + lax.dot_general(
            only, up[leaf], (((1,), (1,)), ((), ())), preferred_element_type=F32
        )
    get_table.start()
    main = total[:, :128]
    tail = jnp.concatenate([total[:, 128:]] * (128 // (width - 128)), axis=1)
    lane = lax.broadcasted_iota(jnp.int32, tail.shape, 1)
    leaf_of = lax.broadcasted_iota(jnp.int32, tail.shape, 0)
    per_row = 128 // (width - 128)
    tail = jnp.where(lane // (width - 128) == leaf_of % per_row, tail, 0.0)
    ends = [
        jnp.sum(tail[i * per_row : (i + 1) * per_row], axis=0, keepdims=True)
        for i in range(leaves // per_row)
    ]
    fill = jnp.zeros((8 - len(ends), 128), F32)
    own[...] = jnp.concatenate([main] + ends + [fill], axis=0).astype(BF16)
    pl.semaphore_wait(barrier, chips + 1)
    to_partner = pltpu.make_async_remote_copy(
        src_ref=own,
        dst_ref=theirs,
        send_sem=pair_send,
        recv_sem=pair_recv,
        device_id=(partner,),
        device_id_type=MESH,
    )
    to_partner.start()
    halos = []
    for i, (src, dst) in enumerate(((pos_ref, wpos_ref), (den_ref, wden_ref))):
        for j, (target, at) in enumerate(((before, 2 * leaves), (after, 0))):
            halos.append(
                pltpu.make_async_remote_copy(
                    src_ref=src,
                    dst_ref=dst.at[pl.ds(at, leaves)],
                    send_sem=halo_send.at[2 * i + j],
                    recv_sem=halo_recv.at[2 * i + j],
                    device_id=(target,),
                    device_id_type=MESH,
                )
            )
    for copy in halos:
        copy.start()
    to_partner.wait_recv()
    mine, his = own[...].astype(F32), theirs[...].astype(F32)
    first = jnp.where(core == 0, mine, his)
    second = jnp.where(core == 0, his, mine)
    main_rows = leaves
    mom_ref[chip] = jnp.concatenate(
        [
            first[:main_rows],
            second[:main_rows],
            first[main_rows : main_rows + 2],
            second[main_rows : main_rows + 2],
            jnp.zeros((4, 128), F32),
        ],
        axis=0,
    ).astype(BF16)
    block = mom_ref.at[chip]
    for target in peers:
        pltpu.make_async_remote_copy(
            src_ref=block,
            dst_ref=block,
            send_sem=send_sem,
            recv_sem=recv_sem,
            device_id=(target,),
            device_id_type=MESH,
        ).start()
    columns()
    racc[...] = jnp.zeros_like(racc)
    get_table.wait()
    widen_table(table, wide)
    for copy in halos:
        copy.wait()

    shift = (me - 1) * leaves

    def early(leaf, _):
        for slot in range(EARLY):
            source = jnp.clip(near_ref[slot, leaf] - shift, 0, 3 * leaves - 1)
            live = jnp.where(slot < cnt_ref[leaf], 1.0, 0.0)
            down = pair_block(leaf, wpos_ref[source], wden_ref[source] * live, cols, racc)
            early_ref[leaf, slot] = jnp.concatenate(
                [jnp.sum(d, axis=0, keepdims=True) for d in down], axis=0
            )
        return 0

    lax.fori_loop(0, leaves, early, 0)
    to_partner.wait_send()
    moved = mom_ref.at[pl.ds(0, chips - 1)]
    pltpu.make_async_copy(moved, moved, send_sem).wait()
    pltpu.make_async_copy(moved, moved, recv_sem).wait()


def exchange_call(count, near, cnt, pos, den, up, table):
    leaves, rows, lanes = pos.shape
    sums = np.zeros((24, 6 * 128), np.float32)
    for k in range(6):
        sums[3 * k : 3 * k + 3, 128 * k : 128 * k + 128] = 1.0
    sums = jnp.asarray(sums, BF16)
    height = table.shape[0] * class_pitch(table.shape[1] // 128) + 8
    window = jax.ShapeDtypeStruct((3 * leaves, rows, lanes), F32)
    return pl.pallas_call(
        functools.partial(exchange_kernel, count),
        name="exchange",
        out_shape=(
            window,
            window,
            jax.ShapeDtypeStruct((count // 2, 40, 128), BF16),
            jax.ShapeDtypeStruct((leaves, 6, 128, 128), F32),
            jax.ShapeDtypeStruct((leaves, 3, 128, 128), F32),
            jax.ShapeDtypeStruct((leaves, EARLY, 3, 128), F32),
            jax.ShapeDtypeStruct((height + -height % 8, 128), F32),
        ),
        in_specs=[SMEM, SMEM, VMEM, VMEM, HBM, HBM, VMEM],
        out_specs=(VMEM,) * 7,
        scratch_shapes=[
            pltpu.VMEM(table.shape, BF16),
            pltpu.VMEM((leaves * 25, 128), F32),
            pltpu.VMEM(up.shape, BF16),
            pltpu.VMEM((24, 128), BF16),
            pltpu.VMEM((24, 128), BF16),
            pltpu.SemaphoreType.DMA((4,)),
            pltpu.SemaphoreType.DMA,
            pltpu.SemaphoreType.DMA,
            pltpu.SemaphoreType.DMA,
            pltpu.SemaphoreType.DMA((4,)),
            pltpu.SemaphoreType.DMA((4,)),
            pltpu.SemaphoreType.DMA,
            pltpu.SemaphoreType.DMA,
        ],
        compiler_params=pltpu.CompilerParams(
            collective_id=0, has_side_effects=True, vmem_limit_bytes=12 * MIB
        ),
    )(*in_hbm(near, cnt, pos, den, up, table, sums))


def middle_kernel(
    width, near_ref, cnt_ref, slot_ref, class_ref, fcnt_ref, req_ref, wpos_ref, wden_ref, cols, early_ref, mom_ref, sel_ref, wide,
    bef_ref, aft_ref, racc, own_ref, sums, sacc, pattern
):
    leaves = bef_ref.shape[0]
    shift = (lax.axis_index("patch") - 1) * leaves
    sacc[...] = jnp.zeros_like(sacc)

    def leaf_step(leaf, _):
        racc[leaf] = jnp.zeros_like(racc[leaf])
        for slot in range(EARLY):
            other = near_ref[slot, leaf] - shift
            sacc[other, :, 0, :] += early_ref[leaf, slot]

        def slot_step(slot, _):
            other = near_ref[slot, leaf] - shift
            down = pair_block(leaf, wpos_ref[other], wden_ref[other], cols, racc)
            for k in range(3):
                sacc[other, k] += down[k]
            return 0

        lax.fori_loop(EARLY, cnt_ref[leaf], slot_step, 0)
        return 0

    lax.fori_loop(0, leaves, leaf_step, 0)

    for k in range(3):
        own_ref[:, k] = sacc[leaves : 2 * leaves, k]

    def gather(leaf, _):
        for k in range(3):
            row = pl.ds(k, 1)
            bef_ref[leaf, row] = jnp.sum(sacc[leaf, k], axis=0, keepdims=True) * -KERNEL
            aft_ref[leaf, row] = jnp.sum(sacc[2 * leaves + leaf, k], axis=0, keepdims=True) * -KERNEL
        return 0

    lax.fori_loop(0, leaves, gather, 0, unroll=4)

    lane = lax.broadcasted_iota(jnp.int32, (8, 128), 1)
    mine = lane // 16 == lax.broadcasted_iota(jnp.int32, (8, 128), 0)

    def spread(step, _):
        lefts, rights = [], []
        for sub in range(8):
            block = mom_ref[step * 8 + sub]
            lefts.append(block[:32])
            ends = block[32:40].astype(F32)
            for i in range(4):
                rights.append(jnp.where(mine, jnp.broadcast_to(ends[i : i + 1], (8, 128)), 0.0))
        lhs = jnp.concatenate(
            [jnp.concatenate(lefts, axis=0), jnp.concatenate(rights, axis=0).astype(BF16)], axis=1
        )
        rows = pl.ds(pl.multiple_of(step * 256, 256), 256)
        for v in range(0, 9, 2):
            some = min(2, 9 - v)
            out = jnp.dot(lhs, sel_ref[:, 128 * v : 128 * (v + some)], preferred_element_type=F32)
            for i in range(some):
                pattern[v + i, rows] = out[:, 128 * i : 128 * i + 128]
        return 0

    lax.fori_loop(0, mom_ref.shape[0] // 8, spread, 0)

    pattern[:, mom_ref.shape[0] * 32 :] = jnp.zeros((9, 8, 128), F32)

    pitch = class_pitch(width * width // 128)
    tall = width // 8
    nothing = pattern.shape[1] - 8
    slots = slot_ref.shape[1]

    def leaf_step(leaf, _):
        live = fcnt_ref[leaf]

        def fetch(slot):
            at = jnp.minimum(slot, slots - 1)
            v = slot_ref[leaf, at]
            who = v >> 2
            place = who * leaves + req_ref[v & 3, who]
            return jnp.where(slot < live, place, nothing), class_ref[leaf, at] * pitch

        def slot_step(step, carry):
            now, acc = carry
            following = tuple(fetch(UNROLL * (step + 1) + i) for i in range(UNROLL))
            new = []
            for v in range(9):
                p = [jnp.broadcast_to(pattern[v, pl.ds(a[0], 1), :], (8, 128)) for a in now]
                for g in range(3):
                    t = [wide[pl.ds(a[1] + tall * v + 8 * g, 8), :] for a in now]
                    total = acc[3 * v + g]
                    for x, y in zip(p, t):
                        total = total + x * y
                    new.append(total)
            return following, tuple(new)

        zero = jnp.zeros((8, 128), F32)
        first = tuple(fetch(i) for i in range(UNROLL))
        _, acc = lax.fori_loop(0, (live + UNROLL - 1) // UNROLL, slot_step, (first, (zero,) * 27))
        for v in range(9):
            for g in range(3):
                rows = pl.ds(pl.multiple_of(leaf * 24 + 8 * g, 8), 8)
                sums[v, rows] = acc[3 * v + g]
        return 0

    lax.fori_loop(0, leaves, leaf_step, 0)


def middle_call(near, cnt, slots, kinds, fcnt, requests, wpos, wden, cols, early, mom, wide, count, width):
    leaves = cnt.shape[0]
    grad = jax.ShapeDtypeStruct((leaves, 3, 128), F32)
    sel, _ = constants(width)
    return pl.pallas_call(
        functools.partial(middle_kernel, width),
        name="middle",
        out_shape=(
            grad,
            grad,
            jax.ShapeDtypeStruct((leaves, 3, 128, 128), F32),
            jax.ShapeDtypeStruct((leaves, 3, 8, 128), F32),
            jax.ShapeDtypeStruct((9, leaves * 24, 128), F32),
        ),
        in_specs=[SMEM] * 6 + [VMEM] * 7,
        out_specs=(VMEM,) * 5,
        scratch_shapes=[
            pltpu.VMEM((3 * leaves, 3, 8, 128), F32),
            pltpu.VMEM((9, count * leaves + 8, 128), F32),
        ],
        compiler_params=pltpu.CompilerParams(vmem_limit_bytes=MIDDLE_LIMIT),
        cost_estimate=pl.CostEstimate(flops=10**8, bytes_accessed=10**7, transcendentals=10**6),
    )(near, cnt, slots, kinds, fcnt, requests, wpos, wden, cols, early, mom, sel, wide)


def back_kernel(
    count, bef_ref, aft_ref, first_acc, racc, own_ref, sums, seg_ref, rep_ref, basis, den_ref, out_ref, got, tgt_ref, weight,
    down, send_sem, recv_sem
):
    leaves, parts = basis.shape[0], basis.shape[1]
    width = basis.shape[2]
    me = lax.axis_index("patch")
    before = (me + count - 1) % count
    after = (me + 1) % count
    sides = ((me > 0, before), (me < count - 1, after))
    barrier = pltpu.get_barrier_semaphore()
    for there, target in sides:

        @pl.when(there)
        def _(target=target):
            pl.semaphore_signal(barrier, inc=1, device_id=(target,), device_id_type=MESH)

    result = jnp.zeros((leaves * 24, seg_ref.shape[1]), F32)
    for v in range(9):
        total = sums[v]
        high = total.astype(BF16)
        low = (total - high.astype(F32)).astype(BF16)
        both = jnp.concatenate([high, low], axis=1)
        part = seg_ref[256 * v : 256 * v + 256]
        result = result + jnp.dot(both, part, preferred_element_type=F32)
    expansion = result.astype(BF16)
    for w in range(0, 8, 2):
        spread = jnp.dot(expansion, rep_ref[:, 128 * w : 128 * w + 256], preferred_element_type=F32)
        for i in range(2):
            weight[pl.ds(w + i, leaves * 24, stride=8), :] = spread[:, 128 * i : 128 * i + 128]

    pl.semaphore_wait(barrier, jnp.minimum(me, 1) + jnp.minimum(count - 1 - me, 1))
    copies = []
    for i, (src, target) in enumerate(((bef_ref, before), (aft_ref, after))):
        copies.append(
            pltpu.make_async_remote_copy(
                src_ref=src,
                dst_ref=got.at[i],
                send_sem=send_sem.at[i],
                recv_sem=recv_sem.at[i],
                device_id=(target,),
                device_id_type=MESH,
            )
        )

        @pl.when(sides[i][0])
        def _(copy=copies[i]):
            copy.start()

        @pl.when(jnp.logical_not(sides[1 - i][0]))
        def _(i=i):
            got[i] = jnp.zeros(got.shape[1:], F32)

    def down_step(leaf, _):
        for q in range(parts):
            part = [jnp.zeros((8, 128), F32) for _ in range(2)]
            for r in range(width // 16):
                d = basis[leaf, q, 16 * r : 16 * r + 16].astype(F32)
                for i in range(2):
                    part[i] = part[i] + d[8 * i : 8 * i + 8] * weight[pl.ds(pl.multiple_of(leaf * 192, 8) + 16 * r + 8 * i, 8), :]
            down[q, pl.ds(leaf, 1)] = jnp.sum(part[0] + part[1], axis=0, keepdims=True)
        return 0

    lax.fori_loop(0, leaves, down_step, 0)
    field = [down[q] for q in range(parts)]
    def gather(pair, _):
        for sub in range(2):
            leaf = pair * 2 + sub
            for k in range(3):
                turned = jnp.transpose(racc[leaf, k] + first_acc[leaf, k], (1, 0))
                folded = turned[0:8]
                for tile in range(1, 16):
                    folded = folded + turned[8 * tile : 8 * tile + 8]
                folded = folded - own_ref[leaf, k]
                tgt_ref[leaf, pl.ds(k, 1)] = jnp.sum(folded, axis=0, keepdims=True) * KERNEL
        return 0

    lax.fori_loop(0, racc.shape[0] // 2, gather, 0)
    for i in range(2):

        @pl.when(sides[i][0])
        def _(i=i):
            copies[i].wait_send()
            copies[1 - i].wait_recv()

    for k in range(3):
        far = den_ref[:, 0, :] * field[k]
        for c in range(1, 3):
            far = far + den_ref[:, c, :] * field[3 * c + k]
        out_ref[:, k, :] = far + (tgt_ref[:, k, :] + (got[0, :, k, :] + got[1, :, k, :]))


def back_call(count, bef, aft, first, racc, own, sums, basis, den):
    leaves = den.shape[0]
    _, seg = constants(basis.shape[2])
    rep = (np.arange(1024)[None, :] // 128 == np.arange(128)[:, None]).astype(np.float32)
    return pl.pallas_call(
        functools.partial(back_kernel, count),
        name="back",
        out_shape=jax.ShapeDtypeStruct(den.shape, F32),
        in_specs=[VMEM] * 10,
        out_specs=VMEM,
        scratch_shapes=[
            pltpu.VMEM((2,) + den.shape, F32),
            pltpu.VMEM(den.shape, F32),
            pltpu.VMEM((leaves * 192, 128), F32),
            pltpu.VMEM((basis.shape[1], leaves, 128), F32),
            pltpu.SemaphoreType.DMA((2,)),
            pltpu.SemaphoreType.DMA((2,)),
        ],
        compiler_params=pltpu.CompilerParams(
            collective_id=1, has_side_effects=True, vmem_limit_bytes=LIMIT
        ),
    )(bef, aft, first, racc, own, sums, seg, jnp.asarray(rep, BF16), basis, den)


def constants(width):
    flat = np.arange(9 * 128)
    sel = np.zeros((256, 9 * 128), np.float32)
    place = flat % width
    sel[:128] = place[None, :] == np.arange(128)[:, None]
    sel[128:] = (place[None, :] >= 128) & ((place[None, :] - 128) == np.arange(128)[:, None] % (width - 128))
    seg = (flat[:, None] // width == np.arange(128)[None, :]).astype(np.float32)
    seg = np.repeat(seg.reshape(9, 1, 128, 128), 2, axis=1).reshape(-1, 128)
    return [jnp.asarray(m, BF16) for m in (sel, seg)]


def per_device(
    count,
    positions,
    densities,
    near_src,
    near_count,
    far_slot,
    far_class,
    far_count,
    requests,
    up_basis,
    transfer_table,
    down_basis,
):
    leaves = near_count.shape[0]
    width = up_basis.shape[1]

    def by_leaf(a):
        return a.reshape(3, leaves, -1).transpose(1, 0, 2)

    pos, den = by_leaf(positions), by_leaf(densities)
    near = near_src.T
    wpos, wden, mom, cols, first, early, wide = exchange_call(
        count, near, near_count, pos, den, up_basis, transfer_table
    )
    bef, aft, racc, own, sums = middle_call(
        near,
        near_count,
        far_slot,
        far_class,
        far_count,
        requests[0].T,
        wpos,
        wden,
        cols,
        early,
        mom,
        wide,
        count,
        width,
    )
    out = back_call(count, bef, aft, first, racc, own, sums, down_basis.transpose(0, 2, 1, 3), den)
    return out.transpose(1, 0, 2).reshape(3, -1)


def solution(mesh):
    placed = (
        P(None, "patch"),
        P(None, "patch"),
        P("patch", None),
        P("patch"),
        P("patch", None),
        P("patch", None),
        P("patch"),
        P("patch", None, None),
        P("patch", None, None),
        P(),
        P("patch", None, None, None),
    )
    return jax.shard_map(
        functools.partial(per_device, mesh.shape["patch"]),
        mesh=mesh,
        in_specs=placed,
        out_specs=P(None, "patch"),
        check_vma=False,
    )
```

```python
import functools
import math

import jax
import jax.numpy as jnp
import numpy as np
from jax import lax
from jax.experimental import pallas as pl
from jax.experimental.pallas import tpu as pltpu
from jax.sharding import PartitionSpec as P

KERNEL = 1.0 / (8.0 * math.pi)
BLOB = 0.25
SIDE = 4
F32 = jnp.float32
BF16 = jnp.bfloat16
MESH = pl.DeviceIdType.MESH
SMEM = pl.BlockSpec(memory_space=pltpu.SMEM)
VMEM = pl.BlockSpec(memory_space=pltpu.VMEM)
HBM = pl.BlockSpec(memory_space=pltpu.HBM)
MIB = 1 << 20
MIDDLE_LIMIT = 14 * MIB
LIMIT = 6 * MIB


def in_hbm(*arrays):
    return [pltpu.with_memory_space_constraint(a, pltpu.HBM) for a in arrays]

UNROLL = 3
EARLY = 3


def class_pitch(chunks):
    return chunks + 1 + chunks % 2


def widen_table(table, wide):
    classes = table.shape[0]
    chunks = table.shape[1] // 128
    pitch = class_pitch(chunks)

    def widen(block, _):
        rows = pl.ds(pl.multiple_of(block * 8, 8), 8)
        at = block * (8 * pitch)
        for chunk in range(chunks):
            to = chunk % 9 * (chunks // 9) + chunk // 9
            wide[pl.ds(at + to, 8, stride=pitch), :] = table[rows, 128 * chunk : 128 * chunk + 128].astype(F32)
        return 0

    full = classes // 8
    rest = classes - 8 * full
    lax.fori_loop(0, full, widen, 0)
    if rest:
        at = full * 8 * pitch
        for chunk in range(chunks):
            to = chunk % 9 * (chunks // 9) + chunk // 9
            wide[pl.ds(at + to, rest, stride=pitch), :] = table[
                8 * full :, 128 * chunk : 128 * chunk + 128
            ].astype(F32)


def pair_block(leaf, source_x, source_f, cols, racc):
    xs = [jnp.broadcast_to(source_x[k : k + 1], (8, 128)) for k in range(3)]
    fs = [jnp.broadcast_to(source_f[k : k + 1], (8, 128)) for k in range(3)]
    down = [jnp.zeros((8, 128), F32) for _ in range(3)]
    for tile in range(16):
        part = pl.ds(8 * tile, 8)
        fa = [cols[leaf, 3 + k, part] for k in range(3)]
        sep = [cols[leaf, k, part] - xs[k] for k in range(3)]
        rho = (sep[0] * sep[0] + sep[1] * sep[1]) + (sep[2] * sep[2] + BLOB)
        inv = lax.rsqrt(rho)
        inv_two = inv * inv
        inv_three = inv_two * inv
        ab = fa[0] * fs[0] + fa[1] * fs[1] + fa[2] * fs[2]
        ar = fa[0] * sep[0] + fa[1] * sep[1] + fa[2] * sep[2]
        br = fs[0] * sep[0] + fs[1] * sep[1] + fs[2] * sep[2]
        on_b = ar * inv_three
        on_a = br * inv_three
        on_r = ab * inv_three + (on_b * br) * (inv_two * 3.0)
        for k in range(3):
            term = fa[k] * on_a + fs[k] * on_b - on_r * sep[k]
            racc[leaf, k, part] += term
            down[k] = down[k] + term
    return down


def exchange_kernel(
    count, near_ref, cnt_ref, pos_ref, den_ref, up_hbm, table_hbm, sum_ref, wpos_ref, wden_ref, mom_ref, cols, racc, early_ref, wide,
    table, left, up, own, theirs, up_sem, table_sem, pair_send, pair_recv, halo_send, halo_recv, send_sem, recv_sem
):
    leaves, width = up.shape[0], up.shape[1]
    plane = SIDE * SIDE
    chips = plane * SIDE
    me = lax.axis_index("patch")
    core = me % 2
    chip = me // 2
    y, z, x = chip // plane, (chip // SIDE) % SIDE, chip % SIDE
    partner = me + 1 - 2 * core
    other_side = (me + 2 * core - 1 + count) % count
    before = (me + count - 1) % count
    after = (me + 1) % count
    at_y = [((y + k) % SIDE) * (2 * plane) + core for k in range(SIDE)]
    at_z = [((z + k) % SIDE) * (2 * SIDE) for k in range(SIDE)]
    at_x = [((x + k) % SIDE) * 2 for k in range(SIDE)]
    steps = [(a, b, c) for a in range(SIDE) for b in range(SIDE) for c in range(SIDE)][1:]
    steps.sort(key=lambda s: -sum(min(v, SIDE - v) for v in s))
    peers = [at_y[a] + at_z[b] + at_x[c] for a, b, c in steps]

    get_ups = []
    for i in range(4):
        part = pl.ds(i * (leaves // 4), leaves // 4)
        get_ups.append(pltpu.make_async_copy(up_hbm.at[part], up.at[part], up_sem.at[i]))
        get_ups[-1].start()
    barrier = pltpu.get_barrier_semaphore()
    for target in [partner] + peers + [other_side]:
        pl.semaphore_signal(barrier, inc=1, device_id=(target,), device_id_type=MESH)

    wpos_ref[pl.ds(leaves, leaves)] = pos_ref[...]
    wden_ref[pl.ds(leaves, leaves)] = den_ref[...]
    rounded = jnp.concatenate([den_ref[:, c, :] for c in range(3)], axis=1)
    row = lax.broadcasted_iota(jnp.int32, rounded.shape, 0)

    def spread(step, _):
        for sub in range(4):
            leaf = step * 4 + sub
            turned = jnp.transpose(left[pl.ds(leaf * 25, 24), :], (1, 0)).astype(BF16)
            wide_rows = jnp.dot(turned, sum_ref[...], preferred_element_type=F32)
            for k in range(6):
                cols[leaf, k] = wide_rows[:, 128 * k : 128 * k + 128]
        return 0

    def columns():
        for k in range(6):
            rest = (pos_ref, den_ref)[k // 3][:, k % 3, :]
            for p in range(3):
                part = rest.astype(BF16).astype(F32)
                left[pl.ds(3 * k + p, leaves, stride=25), :] = part
                rest = rest - part
        for row_at in range(18, 24):
            left[pl.ds(row_at, leaves, stride=25), :] = jnp.zeros((leaves, 128), F32)
        lax.fori_loop(0, leaves // 4, spread, 0)

    get_table = pltpu.make_async_copy(table_hbm, table, table_sem)
    total = jnp.zeros((leaves, width), F32)
    for leaf in range(leaves):
        if leaf % (leaves // 4) == 0:
            get_ups[leaf // (leaves // 4)].wait()
        only = jnp.where(row == leaf, rounded, 0.0).astype(BF16)
        total = total + lax.dot_general(
            only, up[leaf], (((1,), (1,)), ((), ())), preferred_element_type=F32
        )
    get_table.start()
    main = total[:, :128]
    tail = jnp.concatenate([total[:, 128:]] * (128 // (width - 128)), axis=1)
    lane = lax.broadcasted_iota(jnp.int32, tail.shape, 1)
    leaf_of = lax.broadcasted_iota(jnp.int32, tail.shape, 0)
    per_row = 128 // (width - 128)
    tail = jnp.where(lane // (width - 128) == leaf_of % per_row, tail, 0.0)
    ends = [
        jnp.sum(tail[i * per_row : (i + 1) * per_row], axis=0, keepdims=True)
        for i in range(leaves // per_row)
    ]
    fill = jnp.zeros((8 - len(ends), 128), F32)
    own[...] = jnp.concatenate([main] + ends + [fill], axis=0).astype(BF16)
    pl.semaphore_wait(barrier, chips + 1)
    to_partner = pltpu.make_async_remote_copy(
        src_ref=own,
        dst_ref=theirs,
        send_sem=pair_send,
        recv_sem=pair_recv,
        device_id=(partner,),
        device_id_type=MESH,
    )
    to_partner.start()
    halos = []
    for i, (src, dst) in enumerate(((pos_ref, wpos_ref), (den_ref, wden_ref))):
        for j, (target, at) in enumerate(((before, 2 * leaves), (after, 0))):
            halos.append(
                pltpu.make_async_remote_copy(
                    src_ref=src,
                    dst_ref=dst.at[pl.ds(at, leaves)],
                    send_sem=halo_send.at[2 * i + j],
                    recv_sem=halo_recv.at[2 * i + j],
                    device_id=(target,),
                    device_id_type=MESH,
                )
            )
    for copy in halos:
        copy.start()
    to_partner.wait_recv()
    mine, his = own[...].astype(F32), theirs[...].astype(F32)
    first = jnp.where(core == 0, mine, his)
    second = jnp.where(core == 0, his, mine)
    main_rows = leaves
    mom_ref[chip] = jnp.concatenate(
        [
            first[:main_rows],
            second[:main_rows],
            first[main_rows : main_rows + 2],
            second[main_rows : main_rows + 2],
            jnp.zeros((4, 128), F32),
        ],
        axis=0,
    ).astype(BF16)
    block = mom_ref.at[chip]
    for target in peers:
        pltpu.make_async_remote_copy(
            src_ref=block,
            dst_ref=block,
            send_sem=send_sem,
            recv_sem=recv_sem,
            device_id=(target,),
            device_id_type=MESH,
        ).start()
    columns()
    racc[...] = jnp.zeros_like(racc)
    get_table.wait()
    widen_table(table, wide)
    for copy in halos:
        copy.wait()

    shift = (me - 1) * leaves

    def early(leaf, _):
        for slot in range(EARLY):
            source = jnp.clip(near_ref[slot, leaf] - shift, 0, 3 * leaves - 1)
            live = jnp.where(slot < cnt_ref[leaf], 1.0, 0.0)
            down = pair_block(leaf, wpos_ref[source], wden_ref[source] * live, cols, racc)
            early_ref[leaf, slot] = jnp.concatenate(
                [jnp.sum(d, axis=0, keepdims=True) for d in down], axis=0
            )
        return 0

    lax.fori_loop(0, leaves, early, 0)
    to_partner.wait_send()
    moved = mom_ref.at[pl.ds(0, chips - 1)]
    pltpu.make_async_copy(moved, moved, send_sem).wait()
    pltpu.make_async_copy(moved, moved, recv_sem).wait()


def exchange_call(count, near, cnt, pos, den, up, table):
    leaves, rows, lanes = pos.shape
    sums = np.zeros((24, 6 * 128), np.float32)
    for k in range(6):
        sums[3 * k : 3 * k + 3, 128 * k : 128 * k + 128] = 1.0
    sums = jnp.asarray(sums, BF16)
    height = table.shape[0] * class_pitch(table.shape[1] // 128) + 8
    window = jax.ShapeDtypeStruct((3 * leaves, rows, lanes), F32)
    return pl.pallas_call(
        functools.partial(exchange_kernel, count),
        name="exchange",
        out_shape=(
            window,
            window,
            jax.ShapeDtypeStruct((count // 2, 40, 128), BF16),
            jax.ShapeDtypeStruct((leaves, 6, 128, 128), F32),
            jax.ShapeDtypeStruct((leaves, 3, 128, 128), F32),
            jax.ShapeDtypeStruct((leaves, EARLY, 3, 128), F32),
            jax.ShapeDtypeStruct((height + -height % 8, 128), F32),
        ),
        in_specs=[SMEM, SMEM, VMEM, VMEM, HBM, HBM, VMEM],
        out_specs=(VMEM,) * 7,
        scratch_shapes=[
            pltpu.VMEM(table.shape, BF16),
            pltpu.VMEM((leaves * 25, 128), F32),
            pltpu.VMEM(up.shape, BF16),
            pltpu.VMEM((24, 128), BF16),
            pltpu.VMEM((24, 128), BF16),
            pltpu.SemaphoreType.DMA((4,)),
            pltpu.SemaphoreType.DMA,
            pltpu.SemaphoreType.DMA,
            pltpu.SemaphoreType.DMA,
            pltpu.SemaphoreType.DMA((4,)),
            pltpu.SemaphoreType.DMA((4,)),
            pltpu.SemaphoreType.DMA,
            pltpu.SemaphoreType.DMA,
        ],
        compiler_params=pltpu.CompilerParams(
            collective_id=0, has_side_effects=True, vmem_limit_bytes=12 * MIB
        ),
    )(*in_hbm(near, cnt, pos, den, up, table, sums))


def middle_kernel(
    width, near_ref, cnt_ref, slot_ref, class_ref, fcnt_ref, req_ref, wpos_ref, wden_ref, cols, early_ref, mom_ref, sel_ref, wide,
    bef_ref, aft_ref, racc, own_ref, sums, sacc, pattern
):
    leaves = bef_ref.shape[0]
    shift = (lax.axis_index("patch") - 1) * leaves
    sacc[...] = jnp.zeros_like(sacc)

    def leaf_step(leaf, _):
        racc[leaf] = jnp.zeros_like(racc[leaf])
        for slot in range(EARLY):
            other = near_ref[slot, leaf] - shift
            sacc[other, :, 0, :] += early_ref[leaf, slot]

        def slot_step(slot, _):
            other = near_ref[slot, leaf] - shift
            down = pair_block(leaf, wpos_ref[other], wden_ref[other], cols, racc)
            for k in range(3):
                sacc[other, k] += down[k]
            return 0

        lax.fori_loop(EARLY, cnt_ref[leaf], slot_step, 0)
        return 0

    lax.fori_loop(0, leaves, leaf_step, 0)

    for k in range(3):
        own_ref[:, k] = sacc[leaves : 2 * leaves, k]

    def gather(leaf, _):
        for k in range(3):
            row = pl.ds(k, 1)
            bef_ref[leaf, row] = jnp.sum(sacc[leaf, k], axis=0, keepdims=True) * -KERNEL
            aft_ref[leaf, row] = jnp.sum(sacc[2 * leaves + leaf, k], axis=0, keepdims=True) * -KERNEL
        return 0

    lax.fori_loop(0, leaves, gather, 0, unroll=4)

    lane = lax.broadcasted_iota(jnp.int32, (8, 128), 1)
    mine = lane // 16 == lax.broadcasted_iota(jnp.int32, (8, 128), 0)

    def spread(step, _):
        lefts, rights = [], []
        for sub in range(8):
            block = mom_ref[step * 8 + sub]
            lefts.append(block[:32])
            ends = block[32:40].astype(F32)
            for i in range(4):
                rights.append(jnp.where(mine, jnp.broadcast_to(ends[i : i + 1], (8, 128)), 0.0))
        lhs = jnp.concatenate(
            [jnp.concatenate(lefts, axis=0), jnp.concatenate(rights, axis=0).astype(BF16)], axis=1
        )
        rows = pl.ds(pl.multiple_of(step * 256, 256), 256)
        for v in range(0, 9, 2):
            some = min(2, 9 - v)
            out = jnp.dot(lhs, sel_ref[:, 128 * v : 128 * (v + some)], preferred_element_type=F32)
            for i in range(some):
                pattern[v + i, rows] = out[:, 128 * i : 128 * i + 128]
        return 0

    lax.fori_loop(0, mom_ref.shape[0] // 8, spread, 0, unroll=4)

    pattern[:, mom_ref.shape[0] * 32 :] = jnp.zeros((9, 8, 128), F32)

    pitch = class_pitch(width * width // 128)
    tall = width // 8
    nothing = pattern.shape[1] - 8
    slots = slot_ref.shape[1]

    def leaf_step(leaf, _):
        live = fcnt_ref[leaf]

        def fetch(slot):
            at = jnp.minimum(slot, slots - 1)
            v = slot_ref[leaf, at]
            who = v >> 2
            place = who * leaves + req_ref[v & 3, who]
            return jnp.where(slot < live, place, nothing), class_ref[leaf, at] * pitch

        def slot_step(step, carry):
            now, acc = carry
            following = tuple(fetch(UNROLL * (step + 1) + i) for i in range(UNROLL))
            new = []
            for v in range(9):
                p = [jnp.broadcast_to(pattern[v, pl.ds(a[0], 1), :], (8, 128)) for a in now]
                for g in range(3):
                    t = [wide[pl.ds(a[1] + tall * v + 8 * g, 8), :] for a in now]
                    total = acc[3 * v + g]
                    for x, y in zip(p, t):
                        total = total + x * y
                    new.append(total)
            return following, tuple(new)

        zero = jnp.zeros((8, 128), F32)
        first = tuple(fetch(i) for i in range(UNROLL))
        _, acc = lax.fori_loop(0, (live + UNROLL - 1) // UNROLL, slot_step, (first, (zero,) * 27))
        for v in range(9):
            for g in range(3):
                rows = pl.ds(pl.multiple_of(leaf * 24 + 8 * g, 8), 8)
                sums[v, rows] = acc[3 * v + g]
        return 0

    lax.fori_loop(0, leaves, leaf_step, 0)


def middle_call(near, cnt, slots, kinds, fcnt, requests, wpos, wden, cols, early, mom, wide, count, width):
    leaves = cnt.shape[0]
    grad = jax.ShapeDtypeStruct((leaves, 3, 128), F32)
    sel, _ = constants(width)
    return pl.pallas_call(
        functools.partial(middle_kernel, width),
        name="middle",
        out_shape=(
            grad,
            grad,
            jax.ShapeDtypeStruct((leaves, 3, 128, 128), F32),
            jax.ShapeDtypeStruct((leaves, 3, 8, 128), F32),
            jax.ShapeDtypeStruct((9, leaves * 24, 128), F32),
        ),
        in_specs=[SMEM] * 6 + [VMEM] * 7,
        out_specs=(VMEM,) * 5,
        scratch_shapes=[
            pltpu.VMEM((3 * leaves, 3, 8, 128), F32),
            pltpu.VMEM((9, count * leaves + 8, 128), F32),
        ],
        compiler_params=pltpu.CompilerParams(vmem_limit_bytes=MIDDLE_LIMIT),
        cost_estimate=pl.CostEstimate(flops=10**8, bytes_accessed=10**7, transcendentals=10**6),
    )(near, cnt, slots, kinds, fcnt, requests, wpos, wden, cols, early, mom, sel, wide)


def back_kernel(
    count, bef_ref, aft_ref, first_acc, racc, own_ref, sums, seg_ref, rep_ref, basis, den_ref, out_ref, got, tgt_ref, weight,
    down, send_sem, recv_sem
):
    leaves, parts = basis.shape[0], basis.shape[1]
    width = basis.shape[2]
    me = lax.axis_index("patch")
    before = (me + count - 1) % count
    after = (me + 1) % count
    sides = ((me > 0, before), (me < count - 1, after))
    barrier = pltpu.get_barrier_semaphore()
    for there, target in sides:

        @pl.when(there)
        def _(target=target):
            pl.semaphore_signal(barrier, inc=1, device_id=(target,), device_id_type=MESH)

    result = jnp.zeros((leaves * 24, seg_ref.shape[1]), F32)
    for v in range(9):
        total = sums[v]
        high = total.astype(BF16)
        low = (total - high.astype(F32)).astype(BF16)
        both = jnp.concatenate([high, low], axis=1)
        part = seg_ref[256 * v : 256 * v + 256]
        result = result + jnp.dot(both, part, preferred_element_type=F32)
    expansion = result.astype(BF16)
    for w in range(0, 8, 2):
        spread = jnp.dot(expansion, rep_ref[:, 128 * w : 128 * w + 256], preferred_element_type=F32)
        for i in range(2):
            weight[pl.ds(w + i, leaves * 24, stride=8), :] = spread[:, 128 * i : 128 * i + 128]

    pl.semaphore_wait(barrier, jnp.minimum(me, 1) + jnp.minimum(count - 1 - me, 1))
    copies = []
    for i, (src, target) in enumerate(((bef_ref, before), (aft_ref, after))):
        copies.append(
            pltpu.make_async_remote_copy(
                src_ref=src,
                dst_ref=got.at[i],
                send_sem=send_sem.at[i],
                recv_sem=recv_sem.at[i],
                device_id=(target,),
                device_id_type=MESH,
            )
        )

        @pl.when(sides[i][0])
        def _(copy=copies[i]):
            copy.start()

        @pl.when(jnp.logical_not(sides[1 - i][0]))
        def _(i=i):
            got[i] = jnp.zeros(got.shape[1:], F32)

    def down_step(leaf, _):
        for q in range(parts):
            part = [jnp.zeros((8, 128), F32) for _ in range(2)]
            for r in range(width // 16):
                d = basis[leaf, q, 16 * r : 16 * r + 16].astype(F32)
                for i in range(2):
                    part[i] = part[i] + d[8 * i : 8 * i + 8] * weight[pl.ds(pl.multiple_of(leaf * 192, 8) + 16 * r + 8 * i, 8), :]
            down[q, pl.ds(leaf, 1)] = jnp.sum(part[0] + part[1], axis=0, keepdims=True)
        return 0

    lax.fori_loop(0, leaves, down_step, 0, unroll=4)
    field = [down[q] for q in range(parts)]
    def gather(pair, _):
        for sub in range(2):
            leaf = pair * 2 + sub
            for k in range(3):
                turned = jnp.transpose(racc[leaf, k] + first_acc[leaf, k], (1, 0))
                folded = turned[0:8]
                for tile in range(1, 16):
                    folded = folded + turned[8 * tile : 8 * tile + 8]
                folded = folded - own_ref[leaf, k]
                tgt_ref[leaf, pl.ds(k, 1)] = jnp.sum(folded, axis=0, keepdims=True) * KERNEL
        return 0

    lax.fori_loop(0, racc.shape[0] // 2, gather, 0, unroll=4)
    for i in range(2):

        @pl.when(sides[i][0])
        def _(i=i):
            copies[i].wait_send()
            copies[1 - i].wait_recv()

    for k in range(3):
        far = den_ref[:, 0, :] * field[k]
        for c in range(1, 3):
            far = far + den_ref[:, c, :] * field[3 * c + k]
        out_ref[:, k, :] = far + (tgt_ref[:, k, :] + (got[0, :, k, :] + got[1, :, k, :]))


def back_call(count, bef, aft, first, racc, own, sums, basis, den):
    leaves = den.shape[0]
    _, seg = constants(basis.shape[2])
    rep = (np.arange(1024)[None, :] // 128 == np.arange(128)[:, None]).astype(np.float32)
    return pl.pallas_call(
        functools.partial(back_kernel, count),
        name="back",
        out_shape=jax.ShapeDtypeStruct(den.shape, F32),
        in_specs=[VMEM] * 10,
        out_specs=VMEM,
        scratch_shapes=[
            pltpu.VMEM((2,) + den.shape, F32),
            pltpu.VMEM(den.shape, F32),
            pltpu.VMEM((leaves * 192, 128), F32),
            pltpu.VMEM((basis.shape[1], leaves, 128), F32),
            pltpu.SemaphoreType.DMA((2,)),
            pltpu.SemaphoreType.DMA((2,)),
        ],
        compiler_params=pltpu.CompilerParams(
            collective_id=1, has_side_effects=True, vmem_limit_bytes=LIMIT
        ),
    )(bef, aft, first, racc, own, sums, seg, jnp.asarray(rep, BF16), basis, den)


def constants(width):
    flat = np.arange(9 * 128)
    sel = np.zeros((256, 9 * 128), np.float32)
    place = flat % width
    sel[:128] = place[None, :] == np.arange(128)[:, None]
    sel[128:] = (place[None, :] >= 128) & ((place[None, :] - 128) == np.arange(128)[:, None] % (width - 128))
    seg = (flat[:, None] // width == np.arange(128)[None, :]).astype(np.float32)
    seg = np.repeat(seg.reshape(9, 1, 128, 128), 2, axis=1).reshape(-1, 128)
    return [jnp.asarray(m, BF16) for m in (sel, seg)]


def per_device(
    count,
    positions,
    densities,
    near_src,
    near_count,
    far_slot,
    far_class,
    far_count,
    requests,
    up_basis,
    transfer_table,
    down_basis,
):
    leaves = near_count.shape[0]
    width = up_basis.shape[1]

    def by_leaf(a):
        return a.reshape(3, leaves, -1).transpose(1, 0, 2)

    pos, den = by_leaf(positions), by_leaf(densities)
    near = near_src.T
    wpos, wden, mom, cols, first, early, wide = exchange_call(
        count, near, near_count, pos, den, up_basis, transfer_table
    )
    bef, aft, racc, own, sums = middle_call(
        near,
        near_count,
        far_slot,
        far_class,
        far_count,
        requests[0].T,
        wpos,
        wden,
        cols,
        early,
        mom,
        wide,
        count,
        width,
    )
    out = back_call(count, bef, aft, first, racc, own, sums, down_basis.transpose(0, 2, 1, 3), den)
    return out.transpose(1, 0, 2).reshape(3, -1)


def solution(mesh):
    placed = (
        P(None, "patch"),
        P(None, "patch"),
        P("patch", None),
        P("patch"),
        P("patch", None),
        P("patch", None),
        P("patch"),
        P("patch", None, None),
        P("patch", None, None),
        P(),
        P("patch", None, None, None),
    )
    return jax.shard_map(
        functools.partial(per_device, mesh.shape["patch"]),
        mesh=mesh,
        in_specs=placed,
        out_specs=P(None, "patch"),
        check_vma=False,
    )
```
